512 devices in a mesh: band: 2 (over core), tmpl: 32 (over z, x), tm: 8 (over y).
Axes of the slice: x: 4, y: 8, z: 8, core: 2. Of those that a mesh axis runs over, the one named last changes fastest.
Arguments:
- strain_high: float32 [65536], P('tm'), may hold values from -6 to 6
- strain_mid: float32 [8192], P('tm'), may hold values from -6 to 6
- strain_low: float32 [1024], P('tm'), may hold values from -6 to 6
- filters_high: float32 [320, 1024], P('tmpl'), may hold values from -0.1875 to 0.1875
- filters_mid: float32 [320, 1024], P('tmpl'), may hold values from -0.1875 to 0.1875
- filters_low: float32 [320, 128], P('tmpl'), may hold values from -0.5 to 0.5
- recon_high: float32 [320, 2, 2048], P(None, None, 'tmpl'), may hold values from -0.3125 to 0.3125
- recon_mid: float32 [320, 2, 2048], P(None, None, 'tmpl'), may hold values from -0.3125 to 0.3125
- recon_low: float32 [320, 2, 2048], P(None, None, 'tmpl'), may hold values from -0.3125 to 0.3125
- basis_count: int32 [3], replicated, may hold values from 160 to 320
Outputs:
- snr: float32 [2, 2048, 65536], P('band', 'tmpl', 'tm')
The draws below stay inside these ranges and needn't reach their ends.
Inputs may be any that keep to these rules, and one draw needn't show every extreme that they name: basis_count[b] says how many of the first 320 basis vectors band b uses.
All inputs are finite; a program needn't handle non-finite values.
Results may differ from the reference program's by a relative error of at most 0.000082.
Values sent between devices are 32-bit elements; how exact they have to be, the bound alone decides.
No kernel may reach another device: no remote copies, remote signals or barrier semaphores. Data moves between devices by JAX's collectives and lax.ppermute only.
A program may use at most 128 MiB of HBM per device.

```python
import jax
import jax.numpy as jnp
from jax import lax

TEMPLATES = 2048
BASIS = 320
TAPS_HIGH = 1024
TAPS_MID = 1024
TAPS_LOW = 128
RATIO = 8
HALF_TAPS = 8
TIME = 65536
N_TMPL = 32


def block_scale(key, dims, cuts, smallest, largest):
    loudness = 1.0
    for dim, blocks in cuts:
        heights = jax.random.uniform(jax.random.fold_in(jax.random.fold_in(key, 6), dim), (blocks,), jnp.float32, smallest / len(cuts), largest / len(cuts))
        loudness = loudness * jnp.repeat(jnp.exp(heights), dims[dim] // blocks).reshape((-1,) + (1,) * (len(dims) - 1 - dim))
    return loudness


def centred(own_key, extent, deviation, limit, split=(), held_as=jnp.bfloat16):
    values = jax.random.normal(own_key, extent, jnp.float32) * deviation
    if len(split) > 0:
        values = block_scale(own_key, extent, split, -0.22, 0.18) * values
    return jnp.clip(values, min=-limit, max=limit).astype(held_as)


def setup_inputs(seed: int = 0) -> dict:
    keys = jax.random.split(jax.random.key(seed), 11)
    return {
        "strain_high": centred(keys[0], (TIME,), 1.0, 6.0, ((0, 8),), jnp.float32),
        "strain_mid": centred(keys[1], (TIME // RATIO,), 1.0, 6.0, ((0, 8),), jnp.float32),
        "strain_low": centred(keys[2], (TIME // (RATIO * RATIO),), 1.0, 6.0, ((0, 8),), jnp.float32),
        "filters_high": centred(keys[3], (BASIS, TAPS_HIGH), TAPS_HIGH ** -0.5, 0.1875, ((0, 32),), jnp.float32),
        "filters_mid": centred(keys[4], (BASIS, TAPS_MID), TAPS_MID ** -0.5, 0.1875, ((0, 32),), jnp.float32),
        "filters_low": centred(keys[5], (BASIS, TAPS_LOW), TAPS_LOW ** -0.5, 0.5, ((0, 32),), jnp.float32),
        "recon_high": centred(keys[6], (BASIS, 2, TEMPLATES), BASIS ** -0.5, 0.3125, ((2, 32),), jnp.float32),
        "recon_mid": centred(keys[7], (BASIS, 2, TEMPLATES), BASIS ** -0.5, 0.3125, ((2, 32),), jnp.float32),
        "recon_low": centred(keys[8], (BASIS, 2, TEMPLATES), BASIS ** -0.5, 0.3125, ((2, 32),), jnp.float32),
        "basis_count": jax.random.randint(keys[9], (3,), BASIS // 2, BASIS + 1).astype(jnp.int32),
    }


highest = lax.Precision.HIGHEST


def interp_value(offset, half_taps):
    return jnp.sinc(offset) * (0.5 + 0.5 * jnp.cos(jnp.pi * offset / (half_taps + 1)))


def interp_table(half_taps):
    phase_frac = jnp.arange(RATIO, dtype=jnp.float32)[:, None] / RATIO
    lag_index = jnp.arange(2 * half_taps, dtype=jnp.float32)[None, :]
    return interp_value(phase_frac - (lag_index - half_taps), half_taps)


def causal(series, filter_rows):
    tap_count = filter_rows.shape[1]
    padded = jnp.concatenate([jnp.zeros((tap_count - 1,), jnp.float32), series])
    result = lax.conv_general_dilated(padded[None, None, :], filter_rows[:, None, ::-1], (1,), "VALID", precision=highest)
    return result[0]


def masked(series, row_limit):
    row_index = jnp.arange(series.shape[0], dtype=jnp.int32)[:, None]
    return jnp.where(row_index < row_limit, series, 0.0)


def contract(weights, series):
    return lax.dot_general(weights, series, (((0,), (0,)), ((), ())), precision=highest, preferred_element_type=jnp.float32)


def upsample(signal, kernel_table):
    half_taps = kernel_table.shape[1] // 2
    channels, sample_count = signal.shape
    padded = jnp.pad(signal, ((0, 0), (half_taps, half_taps)))
    accumulated = jnp.zeros((channels, sample_count, RATIO), jnp.float32)
    for lag_index in range(2 * half_taps):
        accumulated = accumulated + padded[:, lag_index: lag_index + sample_count, None] * kernel_table[None, None, :, lag_index]
    return accumulated.reshape(channels, sample_count * RATIO)


def reference(strain_high, strain_mid, strain_low, filters_high, filters_mid, filters_low, recon_high, recon_mid, recon_low, basis_count):
    series_high = masked(causal(strain_high, filters_high), basis_count[0])
    series_mid = masked(causal(strain_mid, filters_mid), basis_count[1])
    series_low = masked(causal(strain_low, filters_low), basis_count[2])
    kernel_table = interp_table(HALF_TAPS)
    block_tmpl = TEMPLATES // N_TMPL
    starts = (jnp.arange(N_TMPL, dtype=jnp.int32) * block_tmpl).astype(jnp.int32)

    def one_block(start):
        def take_block(weights):
            return lax.dynamic_slice_in_dim(weights, start, block_tmpl, 2).reshape(BASIS, 2 * block_tmpl)

        low_snr = contract(take_block(recon_low), series_low)
        mid_snr = contract(take_block(recon_mid), series_mid) + upsample(low_snr, kernel_table)
        full_snr = contract(take_block(recon_high), series_high) + upsample(mid_snr, kernel_table)
        return full_snr.reshape(2, block_tmpl, TIME)

    blocks = lax.map(one_block, starts)
    return jnp.transpose(blocks, (1, 0, 2, 3)).reshape(2, TEMPLATES, TIME)
```

```python
import functools

import jax
import jax.numpy as jnp
import numpy as np
from jax import lax
from jax.experimental import pallas as pl
from jax.experimental.pallas import tpu as pltpu
from jax.sharding import PartitionSpec as P

RATIO = 8
HALF_TAPS = 8
LANES = 128
ROWS = 8
BF16 = jnp.bfloat16
F32 = jnp.float32


def interp_blocks():
    phase = np.arange(RATIO)[:, None] / RATIO
    lag = np.arange(2 * HALF_TAPS)[None, :]
    v = phase - (lag - HALF_TAPS)
    g = np.sinc(v) * (0.5 + 0.5 * np.cos(np.pi * v / (HALF_TAPS + 1)))
    blocks = np.zeros((4, 256, 256), np.float64)
    for r in range(4):
        for n in range(256):
            for q in range(2 * HALF_TAPS):
                blocks[r, 32 * r + n // RATIO + q, n] = g[n % RATIO, q]
    return blocks


def split(x):
    hi = x.astype(BF16)
    lo = (x - hi.astype(F32)).astype(BF16)
    return hi, lo


def dot(a, b):
    return lax.dot_general(a, b, (((1,), (0,)), ((), ())), preferred_element_type=F32)


def dot3(a_hi, a_lo, b_hi, b_lo):
    left = jnp.concatenate([a_hi, a_lo, a_hi], axis=1)
    right = jnp.concatenate([b_hi, b_hi, b_lo], axis=0)
    return dot(left, right)


def lane_iota(rows):
    return lax.broadcasted_iota(jnp.int32, (rows, LANES), 1)


def pack_filters(idx_ref, high_ref, mid_ref, low_ref, out_ref):
    band, slot = idx_ref[0], idx_ref[1]
    rows = high_ref.shape[0]
    start = pl.multiple_of(slot * LANES, LANES)
    high = high_ref[:, pl.ds(start, LANES)]
    mid = mid_ref[:, pl.ds(start, LANES)]
    main = jnp.where(band == 0, high, mid)
    low = pltpu.roll(low_ref[...], (LANES - 16 * slot) % LANES, 1)
    lane = lane_iota(1)
    line = [jnp.zeros((1, LANES), F32) for _ in range(2)]
    for q in range(rows):
        at = 16 * (q % 8)
        moved = low[q : q + 1, :]
        if at:
            moved = pltpu.roll(moved, at, 1)
        line[q // 8] = jnp.where((lane >= at) & (lane < at + 16), moved, line[q // 8])
    for p in range(out_ref.shape[0]):
        out_ref[p, 0:rows, :] = main
        out_ref[p, rows : rows + 1, :] = line[0]
        out_ref[p, rows + 1 : rows + 2, :] = line[1]
        out_ref[p, rows + 2 :, :] = jnp.zeros((out_ref.shape[1] - rows - 2, LANES), F32)


def combine(idx_ref, got_ref, high_ref, mid_ref, low_ref, tail_ref, smid_ref, slow_ref, out_ref, f_ref, fl_ref):
    band = idx_ref[0]
    limit = jnp.where(band == 0, idx_ref[2], idx_ref[3])
    limit_low = idx_ref[4]
    parts = got_ref.shape[0]
    basis = high_ref.shape[1]
    rows = basis // parts
    for q in range(rows):
        f_ref[pl.ds(q, parts, stride=rows), :] = got_ref[:, q, :]
        low = got_ref[:, rows + q // 8, :]
        at = 16 * (q % 8)
        if at:
            low = pltpu.roll(low, LANES - at, 1)
        fl_ref[pl.ds(q, parts, stride=rows), :] = low
    column = lax.broadcasted_iota(jnp.int32, high_ref.shape, 1)
    weights = jnp.where(column < limit, jnp.where(band == 0, high_ref[...], mid_ref[...]), 0.0)
    weights_low = jnp.where(column < limit_low, low_ref[...], 0.0)
    h = dot3(*split(weights), *split(f_ref[...]))
    h_low = jnp.transpose(dot3(*split(weights_low), *split(fl_ref[...])))[0:16, :]
    half = h.shape[0] // 2
    lane = lane_iota(ROWS)
    mid = smid_ref[...]
    mid_turned = pltpu.roll(mid, 64, 1)
    for part in range(2):
        turned = h_low if part == 0 else pltpu.roll(h_low, 64, 1)
        one_a = jnp.where(lane < 64, turned[0:8, :], mid_turned)
        one_b = jnp.where(lane < 64, turned[8:16, :], mid)
        last_a = jnp.where(band == 0, tail_ref[...], one_a)
        last_b = jnp.where(band == 0, jnp.broadcast_to(slow_ref[...], (ROWS, LANES)), one_b)
        for slot in range(out_ref.shape[0] // 2):
            at = part * (out_ref.shape[0] // 2) + slot
            out_ref[at, 0:half, :] = h[part * half : (part + 1) * half, :]
            out_ref[at, half : half + 8, :] = last_a
            out_ref[at, half + 8 : half + 16, :] = last_b


class Toeplitz:
    def __init__(self, source, shift, hi_ref, lo_ref):
        self.source, self.shift, self.hi_ref, self.lo_ref = source, shift, hi_ref, lo_ref
        self.turned = {}
        self.lane = lane_iota(ROWS)
        self.sub = lax.broadcasted_iota(jnp.int32, (ROWS, LANES), 0)

    def turn(self, group, n):
        key = (group, n)
        if key not in self.turned:
            by = (ROWS * group + self.shift) % LANES
            self.turned[key] = pltpu.roll(self.source(n), by, 1, stride=1, stride_axis=0)
        return self.turned[key]

    def eight(self, group, n):
        by = ROWS * group + self.shift
        amount = self.sub + by
        value = jnp.where(self.lane >= amount, self.turn(group, n), self.turn(group, n - 1))
        if by + ROWS - 1 > LANES:
            value = jnp.where(self.lane >= amount - LANES, value, self.turn(group, n - 2))
        return value

    def build(self, n, column):
        for pair in range(LANES // 16):
            value = jnp.concatenate([self.eight(2 * pair, n), self.eight(2 * pair + 1, n)], axis=0)
            hi, lo = split(value)
            at = (pl.ds(16 * pair, 16), pl.ds(LANES * column, LANES))
            self.hi_ref[at] = hi
            self.lo_ref[at] = lo


def wide(hi_ref, lo_ref, start, width):
    def pair(ref):
        return [ref[:, start : start + width], ref[:, start - LANES : start - LANES + width]]

    return jnp.concatenate(pair(hi_ref) + pair(hi_ref) + pair(lo_ref), axis=0)


def filter_and_rebuild(
    idx_ref, got_ref, strain_ref, up_hi_ref, up_lo_ref, out_ref,
    xh_ref, ym_ref, yl_ref, th_hi, th_lo, tm_hi, tm_lo, tl_hi, tl_lo, hh_ref, hm_ref, sm_ref,
):
    slot = idx_ref[1]
    slots = got_ref.shape[0] // 2
    tmpl = out_ref.shape[0]
    lane = lane_iota(ROWS)

    def fetch(by):
        index = jnp.clip(slot + by, 0, slots - 1)
        keep = (slot + by >= 0) & (slot + by < slots)
        zero = jnp.zeros((ROWS, LANES), F32)
        tail = jnp.where(keep, got_ref[index, 64:72, :], zero)
        low = jnp.where(keep, got_ref[index, 72:80, :], zero)[0:1, :]
        first = got_ref[slots + index, 64:72, :]
        second = got_ref[slots + index, 72:80, :]
        mid = jnp.where(lane < 64, pltpu.roll(first, 64, 1), second)
        return tail, jnp.where(keep, mid, zero), low

    tail_1, mid_1, low_1 = fetch(-1)
    _, mid_2, low_2 = fetch(-2)
    _, mid_0, low_0 = fetch(0)
    _, mid_r, low_r = fetch(1)
    xh_ref[0:8, :] = tail_1
    xh_ref[8:72, :] = strain_ref[...]
    ym_ref[0:8, :] = mid_2
    ym_ref[8:16, :] = mid_1
    ym_ref[16:24, :] = mid_0
    ym_ref[24:32, :] = mid_r
    yl_ref[0:1, :] = low_2
    yl_ref[1:2, :] = low_1
    yl_ref[2:3, :] = low_0
    yl_ref[3:4, :] = low_r

    for ref, first in ((hh_ref, 0), (hm_ref, slots)):
        for i in range(slots):
            hi, lo = split(got_ref[first + i, 0:tmpl, :])
            c, at = i // 2, LANES * (i % 2)
            rows = slice(c * tmpl, (c + 1) * tmpl)
            ref[rows, at : at + LANES] = hi
            ref[rows, 256 + at : 256 + at + LANES] = lo
            ref[rows, 512 + at : 512 + at + LANES] = hi
    h_low = jnp.transpose(jnp.concatenate([got_ref[slots + i, 64:80, :] for i in range(slots)], axis=0))[0:tmpl, :]

    def rows_of(ref):
        return lambda n: jnp.broadcast_to(ref[n : n + 1, :], (ROWS, LANES))

    low_t = Toeplitz(rows_of(yl_ref), 9, tl_hi, tl_lo)
    low_t.build(2, 0)
    low_t.build(3, 1)
    part_low = dot3(*split(h_low), tl_hi[...], tl_lo[...])
    low_count = LANES
    z = lax.broadcasted_iota(jnp.int32, part_low.shape, 1) - 9 + slot * low_count
    part_low = jnp.where((z >= 0) & (z < slots * low_count), part_low, 0.0)
    low_hi, low_lo = split(part_low)

    mid_t = Toeplitz(rows_of(ym_ref), 8, tm_hi, tm_lo)
    for n in range(1, 17):
        mid_t.build(n + 7 + 1, n)
    for r in range(4):
        sm_ref[:, 256 * r : 256 * r + 256] = dot3(low_hi, low_lo, up_hi_ref[r], up_lo_ref[r])
    edge = dot3(low_hi[:, LANES:], low_lo[:, LANES:], up_hi_ref[0, 0:LANES, 0:LANES], up_lo_ref[0, 0:LANES, 0:LANES])
    for c in range(4):
        edge = edge + dot(hm_ref[c * tmpl : (c + 1) * tmpl, :], wide(tm_hi, tm_lo, 2048 - 256 * c, LANES))
    for m in range(-3, 4):
        first, last = max(0, -m), min(3, 3 - m)
        got = dot(hm_ref[first * tmpl : (last + 1) * tmpl, :], wide(tm_hi, tm_lo, 256 * m + 1024, 256))
        for c in range(first, last + 1):
            at = 256 * (m + c)
            sm_ref[:, at : at + 256] += got[(c - first) * tmpl : (c - first + 1) * tmpl, :]
    sm_ref[:, 1024:1152] = edge
    mid_count = 1024
    v = lax.broadcasted_iota(jnp.int32, sm_ref.shape, 1) - 8 + slot * mid_count
    part_mid = jnp.where((v >= 0) & (v < slots * mid_count), sm_ref[...], 0.0)
    mid_hi, mid_lo = split(part_mid)

    def stacked(x):
        return jnp.concatenate([x[:, LANES * g : LANES * g + 256] for g in range(8)], axis=0)

    stack_hi, stack_lo = stacked(mid_hi), stacked(mid_lo)
    for r in range(4):
        got = dot3(stack_hi, stack_lo, up_hi_ref[r], up_lo_ref[r])
        for g in range(8):
            at = 1024 * g + 256 * r
            out_ref[:, at : at + 256] = got[g * tmpl : (g + 1) * tmpl, :]
    high_t = Toeplitz(rows_of(xh_ref), 0, th_hi, th_lo)
    blocks = out_ref.shape[1] // 256
    for n in (1, 2, 3):
        high_t.build(n, n)
    for m in range(-3, blocks):
        high_t.build(2 * m + 8, 2 * m + 8) if 2 * m + 8 > 3 else None
        high_t.build(2 * m + 9, 2 * m + 9) if 2 * m + 9 > 3 else None
        first, last = max(0, -m), min(3, blocks - 1 - m)
        got = dot(hh_ref[first * tmpl : (last + 1) * tmpl, :], wide(th_hi, th_lo, 256 * m + 1024, 256))
        for c in range(first, last + 1):
            at = 256 * (m + c)
            out_ref[:, at : at + 256] += got[(c - first) * tmpl : (c - first + 1) * tmpl, :]


VMEM = pl.BlockSpec(memory_space=pltpu.VMEM)
SMEM = pl.BlockSpec(memory_space=pltpu.SMEM)


def call_pack(idx, high, mid, low, parts, **kw):
    return pl.pallas_call(
        pack_filters,
        out_shape=jax.ShapeDtypeStruct((parts, 16, LANES), F32),
        in_specs=[SMEM] + [VMEM] * 3,
        out_specs=VMEM,
        name="pack_filters",
        **kw,
    )(idx, high, mid, low)


def call_combine(idx, got, high, mid, low, tail, smid, slow, peers, **kw):
    basis = high.shape[1]
    return pl.pallas_call(
        combine,
        out_shape=jax.ShapeDtypeStruct((peers, 80, LANES), F32),
        in_specs=[SMEM] + [VMEM] * 7,
        out_specs=VMEM,
        scratch_shapes=[pltpu.VMEM((basis, LANES), F32)] * 2,
        name="combine",
        **kw,
    )(idx, got, high, mid, low, tail, smid, slow)


def call_filter(idx, got, strain, up_hi, up_lo, tmpl, count, **kw):
    return pl.pallas_call(
        filter_and_rebuild,
        out_shape=jax.ShapeDtypeStruct((tmpl, count), F32),
        in_specs=[SMEM] + [VMEM] * 4,
        out_specs=VMEM,
        scratch_shapes=[
            pltpu.VMEM((72, LANES), F32),
            pltpu.VMEM((32, LANES), F32),
            pltpu.VMEM((8, LANES), F32),
            pltpu.VMEM((LANES, 9216), BF16),
            pltpu.VMEM((LANES, 9216), BF16),
            pltpu.VMEM((LANES, 2304), BF16),
            pltpu.VMEM((LANES, 2304), BF16),
            pltpu.VMEM((LANES, 256), BF16),
            pltpu.VMEM((LANES, 256), BF16),
            pltpu.VMEM((4 * tmpl, 768), BF16),
            pltpu.VMEM((4 * tmpl, 768), BF16),
            pltpu.VMEM((tmpl, 1152), F32),
        ],
        name="filter_and_rebuild",
        **kw,
    )(idx, got, strain, up_hi, up_lo)


def interp_halves():
    exact = jnp.asarray(interp_blocks().astype(np.float32))
    return split(exact)


def local(
    strain_high, strain_mid, strain_low,
    filters_high, filters_mid, filters_low,
    recon_high, recon_mid, recon_low, basis_count,
):
    band = lax.axis_index("band").astype(jnp.int32)
    slot = lax.axis_index("tm").astype(jnp.int32)
    tmpl_count = lax.axis_size("tmpl")
    peers = lax.axis_size("band") * lax.axis_size("tm")
    idx = jnp.concatenate([jnp.stack([band, slot]), basis_count, jnp.zeros((3,), jnp.int32)])
    packed = call_pack(idx, filters_high, filters_mid, filters_low, tmpl_count)
    got = lax.all_to_all(packed, "tmpl", 0, 0, tiled=True)

    def turned(recon):
        basis, parts, count = recon.shape
        return jnp.transpose(recon, (1, 2, 0)).reshape(parts * count, basis)

    rows = strain_high.reshape(-1, LANES)
    sent = call_combine(
        idx, got, turned(recon_high), turned(recon_mid), turned(recon_low),
        rows[-8:], strain_mid.reshape(-1, LANES), strain_low.reshape(1, LANES), peers,
    )
    here = lax.all_to_all(sent, ("band", "tm"), 0, 0, tiled=True)
    up_hi, up_lo = interp_halves()
    out = call_filter(idx, here, rows, up_hi, up_lo, recon_high.shape[2], strain_high.shape[0])
    return out[None]


def solution(mesh):
    in_specs = (
        P("tm"), P("tm"), P("tm"),
        P("tmpl", None), P("tmpl", None), P("tmpl", None),
        P(None, None, "tmpl"), P(None, None, "tmpl"), P(None, None, "tmpl"),
        P(),
    )
    out_specs = P("band", "tmpl", "tm")
    return jax.shard_map(local, mesh=mesh, in_specs=in_specs, out_specs=out_specs, check_vma=False)
```

```python
import functools

import jax
import jax.numpy as jnp
import numpy as np
from jax import lax
from jax.experimental import pallas as pl
from jax.experimental.pallas import tpu as pltpu
from jax.sharding import PartitionSpec as P

RATIO = 8
HALF_TAPS = 8
LANES = 128
ROWS = 8
BF16 = jnp.bfloat16
F32 = jnp.float32


def interp_blocks():
    phase = np.arange(RATIO)[:, None] / RATIO
    lag = np.arange(2 * HALF_TAPS)[None, :]
    v = phase - (lag - HALF_TAPS)
    g = np.sinc(v) * (0.5 + 0.5 * np.cos(np.pi * v / (HALF_TAPS + 1)))
    blocks = np.zeros((4, 256, 256), np.float64)
    for r in range(4):
        for n in range(256):
            for q in range(2 * HALF_TAPS):
                blocks[r, 32 * r + n // RATIO + q, n] = g[n % RATIO, q]
    return blocks


def split(x):
    hi = x.astype(BF16)
    lo = (x - hi.astype(F32)).astype(BF16)
    return hi, lo


def dot(a, b):
    return lax.dot_general(a, b, (((1,), (0,)), ((), ())), preferred_element_type=F32)


def dot3(a_hi, a_lo, b_hi, b_lo):
    left = jnp.concatenate([a_hi, a_lo, a_hi], axis=1)
    right = jnp.concatenate([b_hi, b_hi, b_lo], axis=0)
    return dot(left, right)


def rebuild(hi, lo, up_hi_ref, up_lo_ref, r):
    if r == 3:
        return dot3(hi, lo, up_hi_ref[r], up_lo_ref[r])
    first_hi, first_lo = hi[:, :LANES], lo[:, :LANES]
    return dot3(first_hi, first_lo, up_hi_ref[r, :LANES, :], up_lo_ref[r, :LANES, :])


def lane_iota(rows):
    return lax.broadcasted_iota(jnp.int32, (rows, LANES), 1)


def pack_filters(
    place, count_ref, high_ref, mid_ref, low_ref, rhigh_ref, rmid_ref, rlow_ref, shigh_ref, smid_ref, slow_ref,
    out_ref, w_hi_ref, w_lo_ref, l_hi_ref, l_lo_ref, strain_ref,
):
    band, slot = place()
    strain_ref[0:64, :] = shigh_ref[...]
    strain_ref[64:72, :] = smid_ref[...]
    strain_ref[72:80, :] = jnp.broadcast_to(slow_ref[...], (ROWS, LANES))
    column = lax.broadcasted_iota(jnp.int32, rhigh_ref.shape, 1)
    limit = jnp.where(band == 0, count_ref[0], count_ref[1])
    weights = jnp.where(column < limit, jnp.where(band == 0, rhigh_ref[...], rmid_ref[...]), 0.0)
    w_hi_ref[...], w_lo_ref[...] = split(weights)
    l_hi_ref[...], l_lo_ref[...] = split(jnp.where(column < count_ref[2], rlow_ref[...], 0.0))
    rows = high_ref.shape[0]
    start = pl.multiple_of(slot * LANES, LANES)
    high = high_ref[:, pl.ds(start, LANES)]
    mid = mid_ref[:, pl.ds(start, LANES)]
    main = jnp.where(band == 0, high, mid)
    low = pltpu.roll(low_ref[...], (LANES - 16 * slot) % LANES, 1)
    lane = lane_iota(1)
    line = [jnp.zeros((1, LANES), F32) for _ in range(2)]
    for q in range(rows):
        at = 16 * (q % 8)
        moved = low[q : q + 1, :]
        if at:
            moved = pltpu.roll(moved, at, 1)
        line[q // 8] = jnp.where((lane >= at) & (lane < at + 16), moved, line[q // 8])
    for p in range(out_ref.shape[0]):
        out_ref[p, 0:rows, :] = main
        out_ref[p, rows : rows + 1, :] = line[0]
        out_ref[p, rows + 1 : rows + 2, :] = line[1]
        out_ref[p, rows + 2 :, :] = jnp.zeros((out_ref.shape[1] - rows - 2, LANES), F32)


def combine(place, got_ref, w_hi_ref, w_lo_ref, l_hi_ref, l_lo_ref, strain_ref, out_ref, f_ref, fl_ref):
    band, _ = place()
    parts = got_ref.shape[0]
    basis = w_hi_ref.shape[1]
    rows = basis // parts
    for q in range(rows):
        f_ref[pl.ds(q, parts, stride=rows), :] = got_ref[:, q, :]
        low = got_ref[:, rows + q // 8, :]
        at = 16 * (q % 8)
        if at:
            low = pltpu.roll(low, LANES - at, 1)
        fl_ref[pl.ds(q, parts, stride=rows), :] = low
    h = dot3(w_hi_ref[...], w_lo_ref[...], *split(f_ref[...]))
    h_low = jnp.transpose(dot3(l_hi_ref[...], l_lo_ref[...], *split(fl_ref[...])))[0:16, :]
    half = h.shape[0] // 2
    lane = lane_iota(ROWS)
    mid = strain_ref[64:72, :]
    mid_turned = pltpu.roll(mid, 64, 1)
    for part in range(2):
        turned = h_low if part == 0 else pltpu.roll(h_low, 64, 1)
        one_a = jnp.where(lane < 64, turned[0:8, :], mid_turned)
        one_b = jnp.where(lane < 64, turned[8:16, :], mid)
        last_a = jnp.where(band == 0, strain_ref[56:64, :], one_a)
        last_b = jnp.where(band == 0, strain_ref[72:80, :], one_b)
        for slot in range(out_ref.shape[0] // 2):
            at = part * (out_ref.shape[0] // 2) + slot
            out_ref[at, 0:half, :] = h[part * half : (part + 1) * half, :]
            out_ref[at, half : half + 8, :] = last_a
            out_ref[at, half + 8 : half + 16, :] = last_b


class Toeplitz:
    def __init__(self, source, shift, hi_ref, lo_ref):
        self.source, self.shift, self.hi_ref, self.lo_ref = source, shift, hi_ref, lo_ref
        self.turned = {}
        self.lane = lane_iota(ROWS)
        self.sub = lax.broadcasted_iota(jnp.int32, (ROWS, LANES), 0)

    def turn(self, group, n):
        key = (group, n)
        if key not in self.turned:
            by = (ROWS * group + self.shift) % LANES
            self.turned[key] = pltpu.roll(self.source(n), by, 1, stride=1, stride_axis=0)
        return self.turned[key]

    def eight(self, group, n):
        by = ROWS * group + self.shift
        amount = self.sub + by
        value = jnp.where(self.lane >= amount, self.turn(group, n), self.turn(group, n - 1))
        if by + ROWS - 1 > LANES:
            value = jnp.where(self.lane >= amount - LANES, value, self.turn(group, n - 2))
        return value

    def build(self, n, column):
        for pair in range(LANES // 16):
            value = jnp.concatenate([self.eight(2 * pair, n), self.eight(2 * pair + 1, n)], axis=0)
            hi, lo = split(value)
            at = (pl.ds(16 * pair, 16), pl.ds(LANES * column, LANES))
            self.hi_ref[at] = hi
            self.lo_ref[at] = lo


def wide(hi_ref, lo_ref, start, width):
    def pair(ref):
        return [ref[:, start : start + width], ref[:, start - LANES : start - LANES + width]]

    return jnp.concatenate(pair(hi_ref) + pair(hi_ref) + pair(lo_ref), axis=0)


def filter_and_rebuild(
    place, got_ref, strain_ref, up_hi_ref, up_lo_ref, result_ref,
    out_ref, sem_ref, xh_ref, ym_ref, yl_ref, th_hi, th_lo, tm_hi, tm_lo, tl_hi, tl_lo, hh_ref, hm_ref, sm_ref,
):
    _, slot = place()
    slots = got_ref.shape[0] // 2
    tmpl = out_ref.shape[0]
    lane = lane_iota(ROWS)

    def fetch(by):
        index = jnp.clip(slot + by, 0, slots - 1)
        keep = (slot + by >= 0) & (slot + by < slots)
        zero = jnp.zeros((ROWS, LANES), F32)
        tail = jnp.where(keep, got_ref[index, 64:72, :], zero)
        low = jnp.where(keep, got_ref[index, 72:80, :], zero)[0:1, :]
        first = got_ref[slots + index, 64:72, :]
        second = got_ref[slots + index, 72:80, :]
        mid = jnp.where(lane < 64, pltpu.roll(first, 64, 1), second)
        return tail, jnp.where(keep, mid, zero), low

    tail_1, mid_1, low_1 = fetch(-1)
    _, mid_2, low_2 = fetch(-2)
    _, mid_0, low_0 = fetch(0)
    _, mid_r, low_r = fetch(1)
    xh_ref[0:8, :] = tail_1
    xh_ref[8:72, :] = strain_ref[0:64, :]
    ym_ref[0:8, :] = mid_2
    ym_ref[8:16, :] = mid_1
    ym_ref[16:24, :] = mid_0
    ym_ref[24:32, :] = mid_r
    yl_ref[0:1, :] = low_2
    yl_ref[1:2, :] = low_1
    yl_ref[2:3, :] = low_0
    yl_ref[3:4, :] = low_r

    for ref, first in ((hh_ref, 0), (hm_ref, slots)):
        for i in range(slots):
            hi, lo = split(got_ref[first + i, 0:tmpl, :])
            c, at = i // 2, LANES * (i % 2)
            rows = slice(c * tmpl, (c + 1) * tmpl)
            ref[rows, at : at + LANES] = hi
            ref[rows, 256 + at : 256 + at + LANES] = lo
            ref[rows, 512 + at : 512 + at + LANES] = hi
    h_low = jnp.transpose(jnp.concatenate([got_ref[slots + i, 64:80, :] for i in range(slots)], axis=0))[0:tmpl, :]

    def rows_of(ref):
        return lambda n: jnp.broadcast_to(ref[n : n + 1, :], (ROWS, LANES))

    low_t = Toeplitz(rows_of(yl_ref), 9, tl_hi, tl_lo)
    low_t.build(2, 0)
    low_t.build(3, 1)
    part_low = dot3(*split(h_low), tl_hi[...], tl_lo[...])
    low_count = LANES
    z = lax.broadcasted_iota(jnp.int32, part_low.shape, 1) - 9 + slot * low_count
    part_low = jnp.where((z >= 0) & (z < slots * low_count), part_low, 0.0)
    low_hi, low_lo = split(part_low)

    mid_t = Toeplitz(rows_of(ym_ref), 8, tm_hi, tm_lo)
    for n in range(1, 17):
        mid_t.build(n + 7 + 1, n)
    for r in range(4):
        sm_ref[:, 256 * r : 256 * r + 256] = rebuild(low_hi, low_lo, up_hi_ref, up_lo_ref, r)
    edge = dot3(low_hi[:, LANES:], low_lo[:, LANES:], up_hi_ref[0, 0:LANES, 0:LANES], up_lo_ref[0, 0:LANES, 0:LANES])
    for c in range(4):
        edge = edge + dot(hm_ref[c * tmpl : (c + 1) * tmpl, :], wide(tm_hi, tm_lo, 2048 - 256 * c, LANES))
    for m in range(-3, 4):
        first, last = max(0, -m), min(3, 3 - m)
        got = dot(hm_ref[first * tmpl : (last + 1) * tmpl, :], wide(tm_hi, tm_lo, 256 * m + 1024, 256))
        for c in range(first, last + 1):
            at = 256 * (m + c)
            sm_ref[:, at : at + 256] += got[(c - first) * tmpl : (c - first + 1) * tmpl, :]
    sm_ref[:, 1024:1152] = edge
    mid_count = 1024
    v = lax.broadcasted_iota(jnp.int32, sm_ref.shape, 1) - 8 + slot * mid_count
    part_mid = jnp.where((v >= 0) & (v < slots * mid_count), sm_ref[...], 0.0)
    mid_hi, mid_lo = split(part_mid)

    def stacked(x):
        return jnp.concatenate([x[:, LANES * g : LANES * g + 256] for g in range(8)], axis=0)

    stack_hi, stack_lo = stacked(mid_hi), stacked(mid_lo)
    for r in range(4):
        got = rebuild(stack_hi, stack_lo, up_hi_ref, up_lo_ref, r)
        for g in range(8):
            at = 1024 * g + 256 * r
            out_ref[:, at : at + 256] = got[g * tmpl : (g + 1) * tmpl, :]
    high_t = Toeplitz(rows_of(xh_ref), 0, th_hi, th_lo)
    blocks = out_ref.shape[1] // 256
    copies = []

    def chunk(k):
        where = (slice(None), pl.ds(1024 * k, 1024))
        return pltpu.make_async_copy(out_ref.at[where], result_ref.at[where], sem_ref.at[k])

    for n in (1, 2, 3):
        high_t.build(n, n)
    for m in range(-3, blocks):
        high_t.build(2 * m + 8, 2 * m + 8) if 2 * m + 8 > 3 else None
        high_t.build(2 * m + 9, 2 * m + 9) if 2 * m + 9 > 3 else None
        first, last = max(0, -m), min(3, blocks - 1 - m)
        got = dot(hh_ref[first * tmpl : (last + 1) * tmpl, :], wide(th_hi, th_lo, 256 * m + 1024, 256))
        for c in range(first, last + 1):
            at = 256 * (m + c)
            out_ref[:, at : at + 256] += got[(c - first) * tmpl : (c - first + 1) * tmpl, :]
        if m % 4 == 3 and m >= 0:
            done = chunk(m // 4)
            done.start()
            copies.append(done)
    for done in copies:
        done.wait()


VMEM = pl.BlockSpec(memory_space=pltpu.VMEM)
SMEM = pl.BlockSpec(memory_space=pltpu.SMEM)
ANY = pl.BlockSpec(memory_space=pl.ANY)


def near(x):
    return pltpu.with_memory_space_constraint(x, pltpu.VMEM)


def place():
    return lax.axis_index("band").astype(jnp.int32), lax.axis_index("tm").astype(jnp.int32)


def call_pack(count, filters, recons, strains, parts, place=place):
    wide, basis = recons[0].shape
    half = pltpu.VMEM((wide, basis), BF16)
    return pl.pallas_call(
        functools.partial(pack_filters, place),
        out_shape=(pltpu.VMEM((parts, 16, LANES), F32), half, half, half, half, pltpu.VMEM((80, LANES), F32)),
        in_specs=[SMEM] + [VMEM] * 9,
        out_specs=(VMEM,) * 6,
        name="pack_filters",
    )(count, *filters, *recons, *strains)


def call_combine(got, weights, strain, peers, place=place):
    basis = weights[0].shape[1]
    return pl.pallas_call(
        functools.partial(combine, place),
        out_shape=pltpu.VMEM((peers, 80, LANES), F32),
        in_specs=[VMEM] * 6,
        out_specs=VMEM,
        scratch_shapes=[pltpu.VMEM((basis, LANES), F32)] * 2,
        name="combine",
    )(*[near(x) for x in (got, *weights, strain)])


def call_filter(got, strain, up_hi, up_lo, tmpl, count, place=place):
    return pl.pallas_call(
        functools.partial(filter_and_rebuild, place),
        out_shape=jax.ShapeDtypeStruct((tmpl, count), F32),
        in_specs=[VMEM] * 4,
        out_specs=ANY,
        scratch_shapes=[
            pltpu.VMEM((tmpl, count), F32),
            pltpu.SemaphoreType.DMA((count // 1024,)),
            pltpu.VMEM((72, LANES), F32),
            pltpu.VMEM((32, LANES), F32),
            pltpu.VMEM((8, LANES), F32),
            pltpu.VMEM((LANES, 9216), BF16),
            pltpu.VMEM((LANES, 9216), BF16),
            pltpu.VMEM((LANES, 2304), BF16),
            pltpu.VMEM((LANES, 2304), BF16),
            pltpu.VMEM((LANES, 256), BF16),
            pltpu.VMEM((LANES, 256), BF16),
            pltpu.VMEM((4 * tmpl, 768), BF16),
            pltpu.VMEM((4 * tmpl, 768), BF16),
            pltpu.VMEM((tmpl, 1152), F32),
        ],
        name="filter_and_rebuild",
    )(*[near(x) for x in (got, strain, up_hi, up_lo)])


def interp_halves():
    exact = jnp.asarray(interp_blocks().astype(np.float32))
    return split(exact)


def local(
    strain_high, strain_mid, strain_low,
    filters_high, filters_mid, filters_low,
    recon_high, recon_mid, recon_low, basis_count,
):
    tmpl_count = lax.axis_size("tmpl")
    peers = lax.axis_size("band") * lax.axis_size("tm")

    def turned(recon):
        basis, parts, count = recon.shape
        return jnp.transpose(recon, (1, 2, 0)).reshape(parts * count, basis)

    packed, *weights, strain = call_pack(
        basis_count,
        (filters_high, filters_mid, filters_low),
        (turned(recon_high), turned(recon_mid), turned(recon_low)),
        (strain_high.reshape(-1, LANES), strain_mid.reshape(-1, LANES), strain_low.reshape(1, LANES)),
        tmpl_count,
    )
    got = lax.all_to_all(packed, "tmpl", 0, 0, tiled=True)
    sent = call_combine(got, weights, strain, peers)
    here = lax.all_to_all(sent, ("band", "tm"), 0, 0, tiled=True)
    up_hi, up_lo = interp_halves()
    out = call_filter(here, strain, up_hi, up_lo, recon_high.shape[2], strain_high.shape[0])
    return out[None]


def solution(mesh):
    in_specs = (
        P("tm"), P("tm"), P("tm"),
        P("tmpl", None), P("tmpl", None), P("tmpl", None),
        P(None, None, "tmpl"), P(None, None, "tmpl"), P(None, None, "tmpl"),
        P(),
    )
    out_specs = P("band", "tmpl", "tm")
    return jax.shard_map(local, mesh=mesh, in_specs=in_specs, out_specs=out_specs, check_vma=False)
```

```python
import functools

import jax
import jax.numpy as jnp
import numpy as np
from jax import lax
from jax.experimental import pallas as pl
from jax.experimental.pallas import tpu as pltpu
from jax.sharding import PartitionSpec as P

RATIO = 8
HALF_TAPS = 8
LANES = 128
ROWS = 8
BF16 = jnp.bfloat16
F32 = jnp.float32


def interp_blocks():
    phase = np.arange(RATIO)[:, None] / RATIO
    lag = np.arange(2 * HALF_TAPS)[None, :]
    v = phase - (lag - HALF_TAPS)
    g = np.sinc(v) * (0.5 + 0.5 * np.cos(np.pi * v / (HALF_TAPS + 1)))
    blocks = np.zeros((4, 256, 256), np.float64)
    for r in range(4):
        for n in range(256):
            for q in range(2 * HALF_TAPS):
                blocks[r, 32 * r + n // RATIO + q, n] = g[n % RATIO, q]
    return blocks


def split(x):
    hi = x.astype(BF16)
    lo = (x - hi.astype(F32)).astype(BF16)
    return hi, lo


def dot(a, b):
    return lax.dot_general(a, b, (((1,), (0,)), ((), ())), preferred_element_type=F32)


def dot3(a_hi, a_lo, b_hi, b_lo):
    left = jnp.concatenate([a_hi, a_lo, a_hi], axis=1)
    right = jnp.concatenate([b_hi, b_hi, b_lo], axis=0)
    return dot(left, right)


def rebuild(hi, lo, up_hi_ref, up_lo_ref, r):
    if r == 3:
        return dot3(hi, lo, up_hi_ref[r], up_lo_ref[r])
    first_hi, first_lo = hi[:, :LANES], lo[:, :LANES]
    return dot3(first_hi, first_lo, up_hi_ref[r, :LANES, :], up_lo_ref[r, :LANES, :])


def lane_iota(rows):
    return lax.broadcasted_iota(jnp.int32, (rows, LANES), 1)


def pack_filters(
    place, count_ref, high_ref, mid_ref, low_ref, rhigh_ref, rmid_ref, rlow_ref, shigh_ref, smid_ref, slow_ref,
    out_ref, w_hi_ref, w_lo_ref, l_hi_ref, l_lo_ref, strain_ref, edge_ref, line_ref,
):
    band, slot = place()
    half = slot % 2
    rows = high_ref.shape[0]
    for t in range(4):
        start = pl.multiple_of(half * 512 + t * LANES, LANES)
        high = high_ref[:, pl.ds(start, LANES)]
        mid = mid_ref[:, pl.ds(start, LANES)]
        line_ref[rows * t : rows * (t + 1), :] = jnp.where(band == 0, high, mid)
    low = low_ref[...]
    low = jnp.where(half == 0, low, pltpu.roll(low, 64, 1))
    shifted = pltpu.roll(low, 64, 1)
    lane = lane_iota(1)
    line_ref[40:48, :] = jnp.zeros((ROWS, LANES), F32)
    for q in range(0, rows, 2):
        line_ref[40 + q // 2 : 41 + q // 2, :] = jnp.where(lane < 64, low[q : q + 1, :], shifted[q + 1 : q + 2, :])
    line = line_ref[...]
    for p in range(out_ref.shape[0]):
        out_ref[p] = line
    strain_ref[0:64, :] = shigh_ref[...]
    edge_ref[0:8, :] = shigh_ref[56:64, :]
    edge_ref[8:16, :] = smid_ref[...]
    edge_ref[16:24, :] = jnp.broadcast_to(slow_ref[...], (ROWS, LANES))
    column = lax.broadcasted_iota(jnp.int32, rhigh_ref.shape, 1)
    limit = jnp.where(band == 0, count_ref[0], count_ref[1])
    weights = jnp.where(column < limit, jnp.where(band == 0, rhigh_ref[...], rmid_ref[...]), 0.0)
    w_hi_ref[...], w_lo_ref[...] = split(weights)
    l_hi_ref[...], l_lo_ref[...] = split(jnp.where(column < count_ref[2], rlow_ref[...], 0.0))


def combine(place, got_ref, w_hi_ref, w_lo_ref, l_hi_ref, l_lo_ref, edge_ref, out_ref, f_ref):
    band, _ = place()
    parts = got_ref.shape[0]
    basis = w_hi_ref.shape[1]
    rows = basis // parts
    for q in range(rows):
        at = pl.ds(q, parts, stride=rows)
        for t in range(4):
            f_ref[t, at, :] = got_ref[:, rows * t + q, :]
        low = got_ref[:, 40 + q // 2, :]
        f_ref[4, at, :] = pltpu.roll(low, 64, 1) if q % 2 else low
    taps = jnp.concatenate([f_ref[t] for t in range(4)], axis=1)
    out_ref[:, 0:512] = dot3(w_hi_ref[...], w_lo_ref[...], *split(taps))
    low = dot3(l_hi_ref[...], l_lo_ref[...], *split(f_ref[4]))
    edge = jnp.concatenate([edge_ref[...], jnp.zeros((40, LANES), F32)] * 2, axis=0)
    out_ref[:, 512:640] = jnp.where(band == 0, edge, low)


class Toeplitz:
    def __init__(self, source, shift, hi_ref, lo_ref):
        self.source, self.shift, self.hi_ref, self.lo_ref = source, shift, hi_ref, lo_ref
        self.turned = {}
        self.lane = lane_iota(ROWS)
        self.sub = lax.broadcasted_iota(jnp.int32, (ROWS, LANES), 0)

    def turn(self, group, n):
        key = (group, n)
        if key not in self.turned:
            by = (ROWS * group + self.shift) % LANES
            self.turned[key] = pltpu.roll(self.source(n), by, 1, stride=1, stride_axis=0)
        return self.turned[key]

    def eight(self, group, n):
        by = ROWS * group + self.shift
        amount = self.sub + by
        value = jnp.where(self.lane >= amount, self.turn(group, n), self.turn(group, n - 1))
        if by + ROWS - 1 > LANES:
            value = jnp.where(self.lane >= amount - LANES, value, self.turn(group, n - 2))
        return value

    def build(self, n, column):
        for pair in range(LANES // 16):
            value = jnp.concatenate([self.eight(2 * pair, n), self.eight(2 * pair + 1, n)], axis=0)
            hi, lo = split(value)
            at = (pl.ds(16 * pair, 16), pl.ds(LANES * column, LANES))
            self.hi_ref[at] = hi
            self.lo_ref[at] = lo


def wide(hi_ref, lo_ref, start, width):
    def pair(ref):
        return [ref[:, start : start + width], ref[:, start - LANES : start - LANES + width]]

    return jnp.concatenate(pair(hi_ref) + pair(hi_ref) + pair(lo_ref), axis=0)


def filter_and_rebuild(
    place, own_ref, pair_ref, other_ref, second_ref, strain_ref, up_hi_ref, up_lo_ref, result_ref,
    out_ref, sem_ref, xh_ref, ym_ref, yl_ref, th_hi, th_lo, tm_hi, tm_lo, tl_hi, tl_lo, hh_ref, hm_ref, sm_ref,
):
    band, slot, slots = place()
    half = slot % 2
    tmpl = out_ref.shape[0]
    mine = pl.multiple_of(band * tmpl, tmpl)
    lane = lane_iota(ROWS)

    def edges(ref, first, lanes):
        return [ref[first + 8 * k : first + 8 * k + 8, lanes] for k in range(3)]

    last = slice(512, 640)
    here = edges(own_ref, 0, last)
    partner = edges(pair_ref, 0, last)
    other = edges(other_ref, 0, slice(None))
    second = edges(second_ref, 0, slice(None))
    left = [jnp.where(half == 0, o, p) for o, p in zip(other, partner)]
    right = [jnp.where(half == 0, p, o) for o, p in zip(other, partner)]
    xh_ref[0:8, :] = left[0]
    xh_ref[8:72, :] = strain_ref[...]
    for k, block in enumerate((second, left, here, right)):
        ym_ref[8 * k : 8 * k + 8, :] = block[1]
        yl_ref[k : k + 1, :] = block[2][0:1, :]

    def low_of(ref):
        return ref[pl.ds(2 * tmpl + mine, tmpl), last]

    for ref, first in ((hh_ref, 0), (hm_ref, 2 * tmpl)):
        for source, part in ((own_ref, half), (pair_ref, 1 - half)):
            for t in range(4):
                hi, lo = split(source[pl.ds(first + mine, tmpl), LANES * t : LANES * (t + 1)])
                at = LANES * (t % 2)
                rows = pl.ds(pl.multiple_of((2 * part + t // 2) * tmpl, tmpl), tmpl)
                ref[rows, at : at + LANES] = hi
                ref[rows, 256 + at : 256 + at + LANES] = lo
                ref[rows, 512 + at : 512 + at + LANES] = hi
    own_low, pair_low = low_of(own_ref), low_of(pair_ref)
    first_low = jnp.where(half == 0, own_low, pair_low)
    second_low = jnp.where(half == 0, pair_low, own_low)
    h_low = jnp.where(lane_iota(tmpl) < 64, first_low, pltpu.roll(second_low, 64, 1))

    def rows_of(ref):
        return lambda n: jnp.broadcast_to(ref[n : n + 1, :], (ROWS, LANES))

    low_t = Toeplitz(rows_of(yl_ref), 9, tl_hi, tl_lo)
    low_t.build(2, 0)
    low_t.build(3, 1)
    part_low = dot3(*split(h_low), tl_hi[...], tl_lo[...])
    low_count = LANES
    z = lax.broadcasted_iota(jnp.int32, part_low.shape, 1) - 9 + slot * low_count
    part_low = jnp.where((z >= 0) & (z < slots * low_count), part_low, 0.0)
    low_hi, low_lo = split(part_low)

    mid_t = Toeplitz(rows_of(ym_ref), 8, tm_hi, tm_lo)
    for n in range(1, 17):
        mid_t.build(n + 7 + 1, n)
    for r in range(4):
        sm_ref[:, 256 * r : 256 * r + 256] = rebuild(low_hi, low_lo, up_hi_ref, up_lo_ref, r)
    edge = dot3(low_hi[:, LANES:], low_lo[:, LANES:], up_hi_ref[0, 0:LANES, 0:LANES], up_lo_ref[0, 0:LANES, 0:LANES])
    for c in range(4):
        edge = edge + dot(hm_ref[c * tmpl : (c + 1) * tmpl, :], wide(tm_hi, tm_lo, 2048 - 256 * c, LANES))
    for m in range(-3, 4):
        first, last = max(0, -m), min(3, 3 - m)
        got = dot(hm_ref[first * tmpl : (last + 1) * tmpl, :], wide(tm_hi, tm_lo, 256 * m + 1024, 256))
        for c in range(first, last + 1):
            at = 256 * (m + c)
            sm_ref[:, at : at + 256] += got[(c - first) * tmpl : (c - first + 1) * tmpl, :]
    sm_ref[:, 1024:1152] = edge
    mid_count = 1024
    v = lax.broadcasted_iota(jnp.int32, sm_ref.shape, 1) - 8 + slot * mid_count
    part_mid = jnp.where((v >= 0) & (v < slots * mid_count), sm_ref[...], 0.0)
    mid_hi, mid_lo = split(part_mid)

    def stacked(x):
        return jnp.concatenate([x[:, LANES * g : LANES * g + 256] for g in range(8)], axis=0)

    stack_hi, stack_lo = stacked(mid_hi), stacked(mid_lo)
    for r in range(4):
        got = rebuild(stack_hi, stack_lo, up_hi_ref, up_lo_ref, r)
        for g in range(8):
            at = 1024 * g + 256 * r
            out_ref[:, at : at + 256] = got[g * tmpl : (g + 1) * tmpl, :]
    high_t = Toeplitz(rows_of(xh_ref), 0, th_hi, th_lo)
    blocks = out_ref.shape[1] // 256
    copies = []

    def chunk(k):
        where = (slice(None), pl.ds(1024 * k, 1024))
        return pltpu.make_async_copy(out_ref.at[where], result_ref.at[where], sem_ref.at[k])

    for n in (1, 2, 3):
        high_t.build(n, n)
    for m in range(-3, blocks):
        high_t.build(2 * m + 8, 2 * m + 8) if 2 * m + 8 > 3 else None
        high_t.build(2 * m + 9, 2 * m + 9) if 2 * m + 9 > 3 else None
        first, last = max(0, -m), min(3, blocks - 1 - m)
        got = dot(hh_ref[first * tmpl : (last + 1) * tmpl, :], wide(th_hi, th_lo, 256 * m + 1024, 256))
        for c in range(first, last + 1):
            at = 256 * (m + c)
            out_ref[:, at : at + 256] += got[(c - first) * tmpl : (c - first + 1) * tmpl, :]
        if m % 4 == 3 and m >= 0:
            done = chunk(m // 4)
            done.start()
            copies.append(done)
    for done in copies:
        done.wait()


VMEM = pl.BlockSpec(memory_space=pltpu.VMEM)
SMEM = pl.BlockSpec(memory_space=pltpu.SMEM)
ANY = pl.BlockSpec(memory_space=pl.ANY)


def near(x):
    return pltpu.with_memory_space_constraint(x, pltpu.VMEM)


def place():
    return lax.axis_index("band").astype(jnp.int32), lax.axis_index("tm").astype(jnp.int32)


def call_pack(count, filters, recons, strains, parts, place=place):
    wide, basis = recons[0].shape
    half = pltpu.VMEM((wide, basis), BF16)
    return pl.pallas_call(
        functools.partial(pack_filters, place),
        out_shape=(
            pltpu.VMEM((parts, 48, LANES), F32), half, half, half, half,
            pltpu.VMEM(strains[0].shape, F32), pltpu.VMEM((24, LANES), F32),
        ),
        in_specs=[SMEM] + [VMEM] * 9,
        out_specs=(VMEM,) * 7,
        scratch_shapes=[pltpu.VMEM((48, LANES), F32)],
        name="pack_filters",
    )(count, *filters, *recons, *strains)


def call_combine(got, weights, edge, place=place):
    wide, basis = weights[0].shape
    return pl.pallas_call(
        functools.partial(combine, place),
        out_shape=pltpu.VMEM((wide, 640), F32),
        in_specs=[VMEM] * 6,
        out_specs=VMEM,
        scratch_shapes=[pltpu.VMEM((5, basis, LANES), F32)],
        name="combine",
    )(*[near(x) for x in (got, *weights, edge)])


def call_filter(own, pair, other, second, strain, up_hi, up_lo, tmpl, count, slots, place=place):
    return pl.pallas_call(
        functools.partial(filter_and_rebuild, lambda: (*place(), slots)),
        out_shape=jax.ShapeDtypeStruct((tmpl, count), F32),
        in_specs=[VMEM] * 7,
        out_specs=ANY,
        scratch_shapes=[
            pltpu.VMEM((tmpl, count), F32),
            pltpu.SemaphoreType.DMA((count // 1024,)),
            pltpu.VMEM((72, LANES), F32),
            pltpu.VMEM((32, LANES), F32),
            pltpu.VMEM((8, LANES), F32),
            pltpu.VMEM((LANES, 9216), BF16),
            pltpu.VMEM((LANES, 9216), BF16),
            pltpu.VMEM((LANES, 2304), BF16),
            pltpu.VMEM((LANES, 2304), BF16),
            pltpu.VMEM((LANES, 256), BF16),
            pltpu.VMEM((LANES, 256), BF16),
            pltpu.VMEM((4 * tmpl, 768), BF16),
            pltpu.VMEM((4 * tmpl, 768), BF16),
            pltpu.VMEM((tmpl, 1152), F32),
        ],
        name="filter_and_rebuild",
    )(*[near(x) for x in (own, pair, other, second, strain, up_hi, up_lo)])


def interp_halves():
    exact = jnp.asarray(interp_blocks().astype(np.float32))
    return split(exact)


def other_side(slots):
    pairs = [(i, i + 1) for i in range(1, slots - 1, 2)]
    return pairs + [(b, a) for a, b in pairs]


def local(
    strain_high, strain_mid, strain_low,
    filters_high, filters_mid, filters_low,
    recon_high, recon_mid, recon_low, basis_count,
):
    tmpl_count = lax.axis_size("tmpl")
    def turned(recon):
        basis, parts, count = recon.shape
        return jnp.transpose(recon, (1, 2, 0)).reshape(parts * count, basis)

    packed, *weights, strain, edge = call_pack(
        basis_count,
        (filters_high, filters_mid, filters_low),
        (turned(recon_high), turned(recon_mid), turned(recon_low)),
        (strain_high.reshape(-1, LANES), strain_mid.reshape(-1, LANES), strain_low.reshape(1, LANES)),
        tmpl_count,
    )
    slots = lax.axis_size("tm")
    got = lax.all_to_all(packed, "tmpl", 0, 0, tiled=True)
    other = lax.ppermute(edge, "tm", other_side(slots))
    second = lax.ppermute(edge, "tm", [(i, i + 2) for i in range(slots - 2)])
    mine = call_combine(got, weights, edge)
    theirs = lax.ppermute(mine, "tm", [(i, i ^ 1) for i in range(slots)])
    own = lax.all_gather(mine, "band", axis=0, tiled=True)
    pair = lax.all_gather(theirs, "band", axis=0, tiled=True)
    up_hi, up_lo = interp_halves()
    out = call_filter(own, pair, other, second, strain, up_hi, up_lo, recon_high.shape[2], strain_high.shape[0], slots)
    return out[None]


def solution(mesh):
    in_specs = (
        P("tm"), P("tm"), P("tm"),
        P("tmpl", None), P("tmpl", None), P("tmpl", None),
        P(None, None, "tmpl"), P(None, None, "tmpl"), P(None, None, "tmpl"),
        P(),
    )
    out_specs = P("band", "tmpl", "tm")
    return jax.shard_map(local, mesh=mesh, in_specs=in_specs, out_specs=out_specs, check_vma=False)
```

```python
import functools

import jax
import jax.numpy as jnp
import numpy as np
from jax import lax
from jax.experimental import pallas as pl
from jax.experimental.pallas import tpu as pltpu
from jax.sharding import PartitionSpec as P

RATIO = 8
HALF_TAPS = 8
LANES = 128
ROWS = 8
SHARES = 4
BF16 = jnp.bfloat16
F32 = jnp.float32


def interp_blocks():
    phase = np.arange(RATIO)[:, None] / RATIO
    lag = np.arange(2 * HALF_TAPS)[None, :]
    v = phase - (lag - HALF_TAPS)
    g = np.sinc(v) * (0.5 + 0.5 * np.cos(np.pi * v / (HALF_TAPS + 1)))
    blocks = np.zeros((4, 256, 256), np.float64)
    for r in range(4):
        for n in range(256):
            for q in range(2 * HALF_TAPS):
                blocks[r, 32 * r + n // RATIO + q, n] = g[n % RATIO, q]
    return blocks


def split(x):
    hi = x.astype(BF16)
    lo = (x - hi.astype(F32)).astype(BF16)
    return hi, lo


def dot(a, b):
    return lax.dot_general(a, b, (((1,), (0,)), ((), ())), preferred_element_type=F32)


def dot3(a_hi, a_lo, b_hi, b_lo):
    left = jnp.concatenate([a_hi, a_lo, a_hi], axis=1)
    right = jnp.concatenate([b_hi, b_hi, b_lo], axis=0)
    return dot(left, right)


def rebuild(hi, lo, up_hi_ref, up_lo_ref, r):
    if r == 3:
        return dot3(hi, lo, up_hi_ref[r], up_lo_ref[r])
    first_hi, first_lo = hi[:, :LANES], lo[:, :LANES]
    return dot3(first_hi, first_lo, up_hi_ref[r, :LANES, :], up_lo_ref[r, :LANES, :])


def lane_iota(rows):
    return lax.broadcasted_iota(jnp.int32, (rows, LANES), 1)


def pack_filters(
    place, count_ref, high_ref, mid_ref, low_ref, rhigh_ref, rmid_ref, rlow_ref, shigh_ref, smid_ref, slow_ref,
    out_ref, w_hi_ref, w_lo_ref, l_hi_ref, l_lo_ref, strain_ref, edge_ref, line_ref,
):
    band, slot = place()
    share = slot % SHARES
    rows = high_ref.shape[0]
    for t in range(2):
        start = pl.multiple_of(share * 256 + t * LANES, LANES)
        high = high_ref[:, pl.ds(start, LANES)]
        mid = mid_ref[:, pl.ds(start, LANES)]
        line_ref[rows * t : rows * (t + 1), :] = jnp.where(band == 0, high, mid)
    low = pltpu.roll(low_ref[...], (LANES - 32 * share) % LANES, 1)
    turned = [low] + [pltpu.roll(low, 32 * k, 1) for k in (1, 2, 3)]
    lane = lane_iota(1)
    for first in range(0, 12, 4):
        value = jnp.zeros((1, LANES), F32)
        for q in range(first, min(first + 4, rows)):
            at = 32 * (q - first)
            value = jnp.where((lane >= at) & (lane < at + 32), turned[q - first][q : q + 1, :], value)
        line_ref[2 * rows + first // 4 : 2 * rows + first // 4 + 1, :] = value
    line_ref[2 * rows + 3 : 24, :] = jnp.zeros((24 - 2 * rows - 3, LANES), F32)
    line = line_ref[...]
    for p in range(out_ref.shape[0]):
        out_ref[p] = line
    strain_ref[0:64, :] = shigh_ref[...]
    edge_ref[0:8, :] = shigh_ref[56:64, :]
    edge_ref[8:16, :] = smid_ref[...]
    edge_ref[16:24, :] = jnp.broadcast_to(slow_ref[...], (ROWS, LANES))
    column = lax.broadcasted_iota(jnp.int32, rhigh_ref.shape, 1)
    limit = jnp.where(band == 0, count_ref[0], count_ref[1])
    weights = jnp.where(column < limit, jnp.where(band == 0, rhigh_ref[...], rmid_ref[...]), 0.0)
    w_hi_ref[...], w_lo_ref[...] = split(weights)
    l_hi_ref[...], l_lo_ref[...] = split(jnp.where(column < count_ref[2], rlow_ref[...], 0.0))


def combine(place, got_ref, w_hi_ref, w_lo_ref, l_hi_ref, l_lo_ref, edge_ref, out_ref, f_ref):
    band, _ = place()
    parts = got_ref.shape[0]
    basis = w_hi_ref.shape[1]
    rows = basis // parts
    for q in range(rows):
        at = pl.ds(q, parts, stride=rows)
        for t in range(2):
            f_ref[t, at, :] = got_ref[:, rows * t + q, :]
        low = got_ref[:, 2 * rows + q // 4, :]
        f_ref[2, at, :] = pltpu.roll(low, LANES - 32 * (q % 4), 1) if q % 4 else low
    taps = jnp.concatenate([f_ref[t] for t in range(2)], axis=1)
    h = dot3(w_hi_ref[...], w_lo_ref[...], *split(taps))
    wide = h.shape[0]
    out_ref[0:wide, :] = h[:, :LANES]
    out_ref[wide : 2 * wide, :] = h[:, LANES:]
    low = jnp.transpose(dot3(l_hi_ref[...], l_lo_ref[...], *split(f_ref[2])))[0:32, :]
    edge = jnp.concatenate([edge_ref[...], jnp.zeros((ROWS, LANES), F32)], axis=0)
    out_ref[2 * wide : 2 * wide + 32, :] = jnp.where(band == 0, edge, low)


def select(place, both_ref, out_ref):
    band, _ = place()
    size = both_ref.shape[0] // 2
    tmpl = (size - 32) // 4
    for k in range(4):
        start = size * (k // 2) + 2 * tmpl * (k % 2) + band * tmpl
        out_ref[k * tmpl : (k + 1) * tmpl, :] = both_ref[pl.ds(pl.multiple_of(start, tmpl), tmpl), :]
    low = both_ref[size + 4 * tmpl :, :]
    low = jnp.where(band == 0, low, pltpu.roll(low, 64, 1))
    tail = both_ref[4 * tmpl : 4 * tmpl + 8, :]
    mid = both_ref[4 * tmpl + 8 : 4 * tmpl + 16, :]
    strain = jnp.concatenate([pltpu.roll(tail, 64, 1), tail, pltpu.roll(mid, 64, 1), mid], axis=0)
    out_ref[4 * tmpl : 4 * tmpl + 32, :] = jnp.where(lane_iota(32) < 64, low, strain)
    out_ref[4 * tmpl + 32 :, :] = both_ref[4 * tmpl + 16 : 4 * tmpl + 24, :]


class Toeplitz:
    def __init__(self, source, shift, hi_ref, lo_ref):
        self.source, self.shift, self.hi_ref, self.lo_ref = source, shift, hi_ref, lo_ref
        self.turned = {}
        self.lane = lane_iota(ROWS)
        self.sub = lax.broadcasted_iota(jnp.int32, (ROWS, LANES), 0)

    def turn(self, group, n):
        key = (group, n)
        if key not in self.turned:
            by = (ROWS * group + self.shift) % LANES
            self.turned[key] = pltpu.roll(self.source(n), by, 1, stride=1, stride_axis=0)
        return self.turned[key]

    def eight(self, group, n):
        by = ROWS * group + self.shift
        amount = self.sub + by
        value = jnp.where(self.lane >= amount, self.turn(group, n), self.turn(group, n - 1))
        if by + ROWS - 1 > LANES:
            value = jnp.where(self.lane >= amount - LANES, value, self.turn(group, n - 2))
        return value

    def build(self, n, column):
        for pair in range(LANES // 16):
            value = jnp.concatenate([self.eight(2 * pair, n), self.eight(2 * pair + 1, n)], axis=0)
            hi, lo = split(value)
            at = (pl.ds(16 * pair, 16), pl.ds(LANES * column, LANES))
            self.hi_ref[at] = hi
            self.lo_ref[at] = lo


def wide(hi_ref, lo_ref, start, width):
    def pair(ref):
        return [ref[:, start : start + width], ref[:, start - LANES : start - LANES + width]]

    return jnp.concatenate(pair(hi_ref) + pair(hi_ref) + pair(lo_ref), axis=0)


def filter_and_rebuild(
    place, own_ref, left_ref, right_ref, second_ref, strain_ref, up_hi_ref, up_lo_ref, result_ref,
    out_ref, sem_ref, xh_ref, ym_ref, yl_ref, th_hi, th_lo, tm_hi, tm_lo, tl_hi, tl_lo, hh_ref, hm_ref, sm_ref,
    hl_ref,
):
    _, slot, slots = place()
    tmpl = out_ref.shape[0]
    base = 4 * tmpl
    lane = lane_iota(ROWS)

    def edges(ref, keep):
        def wide(first):
            a, b = ref[first : first + 8, :], ref[first + 8 : first + 16, :]
            return jnp.where(keep, jnp.where(lane < 64, pltpu.roll(a, 64, 1), b), 0.0)

        return wide(base), wide(base + 16), jnp.where(keep, ref[base + 32 : base + 40, :], 0.0)

    here = edges(own_ref, slot >= 0)
    left = edges(left_ref, slot >= 1)
    second = edges(second_ref, slot >= 2)
    right = edges(right_ref, slot < slots - 1)
    xh_ref[0:8, :] = left[0]
    xh_ref[8:72, :] = strain_ref[...]
    for k, block in enumerate((second, left, here, right)):
        ym_ref[8 * k : 8 * k + 8, :] = block[1]
        yl_ref[k : k + 1, :] = block[2][0:1, :]

    for source, ahead in ((own_ref, 0), (right_ref, 1), (second_ref, 2), (left_ref, 3)):
        share = (slot + ahead) % SHARES
        rows = pl.ds(pl.multiple_of(share * tmpl, tmpl), tmpl)
        for k in range(4):
            hi, lo = split(source[k * tmpl : (k + 1) * tmpl, :])
            ref, at = (hh_ref, hm_ref)[k // 2], LANES * (k % 2)
            ref[rows, at : at + LANES] = hi
            ref[rows, 256 + at : 256 + at + LANES] = lo
            ref[rows, 512 + at : 512 + at + LANES] = hi
        hl_ref[pl.ds(pl.multiple_of(share * 32, 32), 32), :] = source[base : base + 32, :]
    h_low = jnp.transpose(hl_ref[...])[0:tmpl, :]

    def rows_of(ref):
        return lambda n: jnp.broadcast_to(ref[n : n + 1, :], (ROWS, LANES))

    low_t = Toeplitz(rows_of(yl_ref), 9, tl_hi, tl_lo)
    low_t.build(2, 0)
    low_t.build(3, 1)
    part_low = dot3(*split(h_low), tl_hi[...], tl_lo[...])
    low_count = LANES
    z = lax.broadcasted_iota(jnp.int32, part_low.shape, 1) - 9 + slot * low_count
    part_low = jnp.where((z >= 0) & (z < slots * low_count), part_low, 0.0)
    low_hi, low_lo = split(part_low)

    mid_t = Toeplitz(rows_of(ym_ref), 8, tm_hi, tm_lo)
    for n in range(1, 17):
        mid_t.build(n + 7 + 1, n)
    for r in range(4):
        sm_ref[:, 256 * r : 256 * r + 256] = rebuild(low_hi, low_lo, up_hi_ref, up_lo_ref, r)
    edge = dot3(low_hi[:, LANES:], low_lo[:, LANES:], up_hi_ref[0, 0:LANES, 0:LANES], up_lo_ref[0, 0:LANES, 0:LANES])
    for c in range(4):
        edge = edge + dot(hm_ref[c * tmpl : (c + 1) * tmpl, :], wide(tm_hi, tm_lo, 2048 - 256 * c, LANES))
    for m in range(-3, 4):
        first, last = max(0, -m), min(3, 3 - m)
        got = dot(hm_ref[first * tmpl : (last + 1) * tmpl, :], wide(tm_hi, tm_lo, 256 * m + 1024, 256))
        for c in range(first, last + 1):
            at = 256 * (m + c)
            sm_ref[:, at : at + 256] += got[(c - first) * tmpl : (c - first + 1) * tmpl, :]
    sm_ref[:, 1024:1152] = edge
    mid_count = 1024
    v = lax.broadcasted_iota(jnp.int32, sm_ref.shape, 1) - 8 + slot * mid_count
    part_mid = jnp.where((v >= 0) & (v < slots * mid_count), sm_ref[...], 0.0)
    mid_hi, mid_lo = split(part_mid)

    def stacked(x):
        return jnp.concatenate([x[:, LANES * g : LANES * g + 256] for g in range(8)], axis=0)

    stack_hi, stack_lo = stacked(mid_hi), stacked(mid_lo)
    for r in range(4):
        got = rebuild(stack_hi, stack_lo, up_hi_ref, up_lo_ref, r)
        for g in range(8):
            at = 1024 * g + 256 * r
            out_ref[:, at : at + 256] = got[g * tmpl : (g + 1) * tmpl, :]
    high_t = Toeplitz(rows_of(xh_ref), 0, th_hi, th_lo)
    blocks = out_ref.shape[1] // 256
    copies = []

    def chunk(k):
        where = (slice(None), pl.ds(1024 * k, 1024))
        return pltpu.make_async_copy(out_ref.at[where], result_ref.at[where], sem_ref.at[k])

    for n in (1, 2, 3):
        high_t.build(n, n)
    for m in range(-3, blocks):
        high_t.build(2 * m + 8, 2 * m + 8) if 2 * m + 8 > 3 else None
        high_t.build(2 * m + 9, 2 * m + 9) if 2 * m + 9 > 3 else None
        first, last = max(0, -m), min(3, blocks - 1 - m)
        got = dot(hh_ref[first * tmpl : (last + 1) * tmpl, :], wide(th_hi, th_lo, 256 * m + 1024, 256))
        for c in range(first, last + 1):
            at = 256 * (m + c)
            out_ref[:, at : at + 256] += got[(c - first) * tmpl : (c - first + 1) * tmpl, :]
        if m % 4 == 3 and m >= 0:
            done = chunk(m // 4)
            done.start()
            copies.append(done)
    for done in copies:
        done.wait()


VMEM = pl.BlockSpec(memory_space=pltpu.VMEM)
SMEM = pl.BlockSpec(memory_space=pltpu.SMEM)
ANY = pl.BlockSpec(memory_space=pl.ANY)


def near(x):
    return pltpu.with_memory_space_constraint(x, pltpu.VMEM)


def place():
    return lax.axis_index("band").astype(jnp.int32), lax.axis_index("tm").astype(jnp.int32)


def call_pack(count, filters, recons, strains, parts, place=place):
    wide, basis = recons[0].shape
    half = pltpu.VMEM((wide, basis), BF16)
    return pl.pallas_call(
        functools.partial(pack_filters, place),
        out_shape=(
            pltpu.VMEM((parts, 24, LANES), F32), half, half, half, half,
            pltpu.VMEM(strains[0].shape, F32), pltpu.VMEM((24, LANES), F32),
        ),
        in_specs=[SMEM] + [VMEM] * 9,
        out_specs=(VMEM,) * 7,
        scratch_shapes=[pltpu.VMEM((24, LANES), F32)],
        name="pack_filters",
    )(count, *filters, *recons, *strains)


def call_combine(got, weights, edge, place=place):
    wide, basis = weights[0].shape
    return pl.pallas_call(
        functools.partial(combine, place),
        out_shape=pltpu.VMEM((2 * wide + 32, LANES), F32),
        in_specs=[VMEM] * 6,
        out_specs=VMEM,
        scratch_shapes=[pltpu.VMEM((3, basis, LANES), F32)],
        name="combine",
    )(*[near(x) for x in (got, *weights, edge)])


def call_select(both, place=place):
    return pl.pallas_call(
        functools.partial(select, place),
        out_shape=pltpu.VMEM((both.shape[0] // 2 + 8, LANES), F32),
        in_specs=[VMEM],
        out_specs=VMEM,
        name="select",
    )(near(both))


def call_filter(own, left, right, second, strain, up_hi, up_lo, tmpl, count, slots, place=place):
    return pl.pallas_call(
        functools.partial(filter_and_rebuild, lambda: (*place(), slots)),
        out_shape=jax.ShapeDtypeStruct((tmpl, count), F32),
        in_specs=[VMEM] * 7,
        out_specs=ANY,
        scratch_shapes=[
            pltpu.VMEM((tmpl, count), F32),
            pltpu.SemaphoreType.DMA((count // 1024,)),
            pltpu.VMEM((72, LANES), F32),
            pltpu.VMEM((32, LANES), F32),
            pltpu.VMEM((8, LANES), F32),
            pltpu.VMEM((LANES, 9216), BF16),
            pltpu.VMEM((LANES, 9216), BF16),
            pltpu.VMEM((LANES, 2304), BF16),
            pltpu.VMEM((LANES, 2304), BF16),
            pltpu.VMEM((LANES, 256), BF16),
            pltpu.VMEM((LANES, 256), BF16),
            pltpu.VMEM((4 * tmpl, 768), BF16),
            pltpu.VMEM((4 * tmpl, 768), BF16),
            pltpu.VMEM((tmpl, 1152), F32),
            pltpu.VMEM((LANES, LANES), F32),
        ],
        name="filter_and_rebuild",
    )(*[near(x) for x in (own, left, right, second, strain, up_hi, up_lo)])


def interp_halves():
    exact = jnp.asarray(interp_blocks().astype(np.float32))
    return split(exact)


def local(
    strain_high, strain_mid, strain_low,
    filters_high, filters_mid, filters_low,
    recon_high, recon_mid, recon_low, basis_count,
):
    tmpl_count = lax.axis_size("tmpl")
    def turned(recon):
        basis, parts, count = recon.shape
        return jnp.transpose(recon, (1, 2, 0)).reshape(parts * count, basis)

    packed, *weights, strain, edge = call_pack(
        basis_count,
        (filters_high, filters_mid, filters_low),
        (turned(recon_high), turned(recon_mid), turned(recon_low)),
        (strain_high.reshape(-1, LANES), strain_mid.reshape(-1, LANES), strain_low.reshape(1, LANES)),
        tmpl_count,
    )
    slots = lax.axis_size("tm")
    got = lax.all_to_all(packed, "tmpl", 0, 0, tiled=True)
    both = lax.all_gather(call_combine(got, weights, edge), "band", axis=0, tiled=True)
    own = call_select(both)

    def moved(by):
        return lax.ppermute(own, "tm", [(i, (i + by) % slots) for i in range(slots)])

    second, left, right = moved(2), moved(1), moved(-1)
    up_hi, up_lo = interp_halves()
    out = call_filter(own, left, right, second, strain, up_hi, up_lo, recon_high.shape[2], strain_high.shape[0], slots)
    return out[None]


def solution(mesh):
    in_specs = (
        P("tm"), P("tm"), P("tm"),
        P("tmpl", None), P("tmpl", None), P("tmpl", None),
        P(None, None, "tmpl"), P(None, None, "tmpl"), P(None, None, "tmpl"),
        P(),
    )
    out_specs = P("band", "tmpl", "tm")
    return jax.shard_map(local, mesh=mesh, in_specs=in_specs, out_specs=out_specs, check_vma=False)
```

```python
import functools

import jax
import jax.numpy as jnp
import numpy as np
from jax import lax
from jax.experimental import pallas as pl
from jax.experimental.pallas import tpu as pltpu
from jax.sharding import PartitionSpec as P

RATIO = 8
HALF_TAPS = 8
LANES = 128
ROWS = 8
SHARES = 4
BF16 = jnp.bfloat16
F32 = jnp.float32


def interp_blocks():
    phase = np.arange(RATIO)[:, None] / RATIO
    lag = np.arange(2 * HALF_TAPS)[None, :]
    v = phase - (lag - HALF_TAPS)
    g = np.sinc(v) * (0.5 + 0.5 * np.cos(np.pi * v / (HALF_TAPS + 1)))
    blocks = np.zeros((4, 256, 256), np.float64)
    for r in range(4):
        for n in range(256):
            for q in range(2 * HALF_TAPS):
                blocks[r, 32 * r + n // RATIO + q, n] = g[n % RATIO, q]
    return blocks


def split(x):
    hi = x.astype(BF16)
    lo = (x - hi.astype(F32)).astype(BF16)
    return hi, lo


def dot(a, b):
    return lax.dot_general(a, b, (((1,), (0,)), ((), ())), preferred_element_type=F32)


def dot3(a_hi, a_lo, b_hi, b_lo):
    left = jnp.concatenate([a_hi, a_lo, a_hi], axis=1)
    right = jnp.concatenate([b_hi, b_hi, b_lo], axis=0)
    return dot(left, right)


def rebuild(hi, lo, up_hi_ref, up_lo_ref, r):
    if r == 3:
        return dot3(hi, lo, up_hi_ref[r], up_lo_ref[r])
    first_hi, first_lo = hi[:, :LANES], lo[:, :LANES]
    return dot3(first_hi, first_lo, up_hi_ref[r, :LANES, :], up_lo_ref[r, :LANES, :])


def lane_iota(rows):
    return lax.broadcasted_iota(jnp.int32, (rows, LANES), 1)


def pack_filters(place, high_ref, mid_ref, low_ref, out_ref, line_ref):
    band, slot = place()
    share = slot % SHARES
    rows = high_ref.shape[0]
    for t in range(2):
        start = pl.multiple_of(share * 256 + t * LANES, LANES)
        high = high_ref[:, pl.ds(start, LANES)]
        mid = mid_ref[:, pl.ds(start, LANES)]
        line_ref[rows * t : rows * (t + 1), :] = jnp.where(band == 0, high, mid)
    low = pltpu.roll(low_ref[...], (LANES - 32 * share) % LANES, 1)
    turned = [low] + [pltpu.roll(low, 32 * k, 1) for k in (1, 2, 3)]
    lane = lane_iota(1)
    for first in range(0, 12, 4):
        value = jnp.zeros((1, LANES), F32)
        for q in range(first, min(first + 4, rows)):
            at = 32 * (q - first)
            value = jnp.where((lane >= at) & (lane < at + 32), turned[q - first][q : q + 1, :], value)
        line_ref[2 * rows + first // 4 : 2 * rows + first // 4 + 1, :] = value
    line_ref[2 * rows + 3 : 24, :] = jnp.zeros((24 - 2 * rows - 3, LANES), F32)
    line = line_ref[...]
    for p in range(out_ref.shape[0]):
        out_ref[p] = line


def prepare(
    place, count_ref, rhigh_ref, rmid_ref, rlow_ref, shigh_ref, smid_ref, slow_ref,
    w_hi_ref, w_lo_ref, l_hi_ref, l_lo_ref, strain_ref, edge_ref,
):
    band, _ = place()
    strain_ref[...] = shigh_ref[...]
    edge_ref[0:8, :] = shigh_ref[56:64, :]
    edge_ref[8:16, :] = smid_ref[...]
    edge_ref[16:24, :] = jnp.broadcast_to(slow_ref[...], (ROWS, LANES))
    column = lax.broadcasted_iota(jnp.int32, rhigh_ref.shape, 1)
    limit = jnp.where(band == 0, count_ref[0], count_ref[1])
    weights = jnp.where(column < limit, jnp.where(band == 0, rhigh_ref[...], rmid_ref[...]), 0.0)
    w_hi_ref[...], w_lo_ref[...] = split(weights)
    l_hi_ref[...], l_lo_ref[...] = split(jnp.where(column < count_ref[2], rlow_ref[...], 0.0))


def combine(place, got_ref, w_hi_ref, w_lo_ref, l_hi_ref, l_lo_ref, edge_ref, _, out_ref, f_ref):
    band, _ = place()
    parts = got_ref.shape[0]
    basis = w_hi_ref.shape[1]
    rows = basis // parts
    for q in range(rows):
        at = pl.ds(q, parts, stride=rows)
        for t in range(2):
            f_ref[t, at, :] = got_ref[:, rows * t + q, :]
        low = got_ref[:, 2 * rows + q // 4, :]
        f_ref[2, at, :] = pltpu.roll(low, LANES - 32 * (q % 4), 1) if q % 4 else low
    taps = jnp.concatenate([f_ref[t] for t in range(2)], axis=1)
    h = dot3(w_hi_ref[...], w_lo_ref[...], *split(taps))
    wide = h.shape[0]
    out_ref[0:wide, :] = h[:, :LANES]
    out_ref[wide : 2 * wide, :] = h[:, LANES:]
    low = jnp.transpose(dot3(l_hi_ref[...], l_lo_ref[...], *split(f_ref[2])))[0:32, :]
    edge = jnp.concatenate([edge_ref[...], jnp.zeros((ROWS, LANES), F32)], axis=0)
    out_ref[2 * wide : 2 * wide + 32, :] = jnp.where(band == 0, edge, low)


def select(place, both_ref, out_ref):
    band, _ = place()
    size = both_ref.shape[0] // 2
    tmpl = (size - 32) // 4
    for k in range(4):
        start = size * (k // 2) + 2 * tmpl * (k % 2) + band * tmpl
        out_ref[k * tmpl : (k + 1) * tmpl, :] = both_ref[pl.ds(pl.multiple_of(start, tmpl), tmpl), :]
    low = both_ref[size + 4 * tmpl :, :]
    low = jnp.where(band == 0, low, pltpu.roll(low, 64, 1))
    tail = both_ref[4 * tmpl : 4 * tmpl + 8, :]
    mid = both_ref[4 * tmpl + 8 : 4 * tmpl + 16, :]
    strain = jnp.concatenate([pltpu.roll(tail, 64, 1), tail, pltpu.roll(mid, 64, 1), mid], axis=0)
    out_ref[4 * tmpl : 4 * tmpl + 32, :] = jnp.where(lane_iota(32) < 64, low, strain)
    out_ref[4 * tmpl + 32 :, :] = both_ref[4 * tmpl + 16 : 4 * tmpl + 24, :]


class Toeplitz:
    def __init__(self, source, shift, hi_ref, lo_ref):
        self.source, self.shift, self.hi_ref, self.lo_ref = source, shift, hi_ref, lo_ref
        self.turned = {}
        self.lane = lane_iota(ROWS)
        self.sub = lax.broadcasted_iota(jnp.int32, (ROWS, LANES), 0)

    def turn(self, group, n):
        key = (group, n)
        if key not in self.turned:
            by = (ROWS * group + self.shift) % LANES
            self.turned[key] = pltpu.roll(self.source(n), by, 1, stride=1, stride_axis=0)
        return self.turned[key]

    def eight(self, group, n):
        by = ROWS * group + self.shift
        amount = self.sub + by
        value = jnp.where(self.lane >= amount, self.turn(group, n), self.turn(group, n - 1))
        if by + ROWS - 1 > LANES:
            value = jnp.where(self.lane >= amount - LANES, value, self.turn(group, n - 2))
        return value

    def build(self, n, column):
        for pair in range(LANES // 16):
            value = jnp.concatenate([self.eight(2 * pair, n), self.eight(2 * pair + 1, n)], axis=0)
            hi, lo = split(value)
            at = (pl.ds(16 * pair, 16), pl.ds(LANES * column, LANES))
            self.hi_ref[at] = hi
            self.lo_ref[at] = lo


def wide(hi_ref, lo_ref, start, width):
    def pair(ref):
        return [ref[:, start : start + width], ref[:, start - LANES : start - LANES + width]]

    return jnp.concatenate(pair(hi_ref) + pair(hi_ref) + pair(lo_ref), axis=0)


def filter_and_rebuild(
    place, own_ref, left_ref, right_ref, across_ref, second_ref, strain_ref, up_hi_ref, up_lo_ref, result_ref,
    out_ref, sem_ref, xh_ref, ym_ref, yl_ref, th_hi, th_lo, tm_hi, tm_lo, tl_hi, tl_lo, hh_ref, hm_ref, sm_ref,
    hl_ref,
):
    _, slot, slots = place()
    tmpl = out_ref.shape[0]
    base = 4 * tmpl
    lane = lane_iota(ROWS)

    def edges(ref, keep):
        def wide(first):
            a, b = ref[first : first + 8, :], ref[first + 8 : first + 16, :]
            return jnp.where(keep, jnp.where(lane < 64, pltpu.roll(a, 64, 1), b), 0.0)

        return wide(base), wide(base + 16), jnp.where(keep, ref[base + 32 : base + 40, :], 0.0)

    here = edges(own_ref, slot >= 0)
    left = edges(left_ref, slot >= 1)
    second = [second_ref[8 * k : 8 * k + 8, :] for k in range(3)]
    right = edges(right_ref, slot < slots - 1)
    xh_ref[0:8, :] = left[0]
    xh_ref[8:72, :] = strain_ref[...]
    for k, block in enumerate((second, left, here, right)):
        ym_ref[8 * k : 8 * k + 8, :] = block[1]
        yl_ref[k : k + 1, :] = block[2][0:1, :]

    for source, ahead in ((own_ref, 0), (right_ref, 1), (across_ref, 2), (left_ref, 3)):
        share = (slot + ahead) % SHARES
        rows = pl.ds(pl.multiple_of(share * tmpl, tmpl), tmpl)
        for k in range(4):
            hi, lo = split(source[k * tmpl : (k + 1) * tmpl, :])
            ref, at = (hh_ref, hm_ref)[k // 2], LANES * (k % 2)
            ref[rows, at : at + LANES] = hi
            ref[rows, 256 + at : 256 + at + LANES] = lo
            ref[rows, 512 + at : 512 + at + LANES] = hi
        hl_ref[pl.ds(pl.multiple_of(share * 32, 32), 32), :] = source[base : base + 32, :]
    h_low = jnp.transpose(hl_ref[...])[0:tmpl, :]

    def rows_of(ref):
        return lambda n: jnp.broadcast_to(ref[n : n + 1, :], (ROWS, LANES))

    low_t = Toeplitz(rows_of(yl_ref), 9, tl_hi, tl_lo)
    low_t.build(2, 0)
    low_t.build(3, 1)
    part_low = dot3(*split(h_low), tl_hi[...], tl_lo[...])
    low_count = LANES
    z = lax.broadcasted_iota(jnp.int32, part_low.shape, 1) - 9 + slot * low_count
    part_low = jnp.where((z >= 0) & (z < slots * low_count), part_low, 0.0)
    low_hi, low_lo = split(part_low)

    mid_t = Toeplitz(rows_of(ym_ref), 8, tm_hi, tm_lo)
    for n in range(1, 17):
        mid_t.build(n + 7 + 1, n)
    for r in range(4):
        sm_ref[:, 256 * r : 256 * r + 256] = rebuild(low_hi, low_lo, up_hi_ref, up_lo_ref, r)
    edge = dot3(low_hi[:, LANES:], low_lo[:, LANES:], up_hi_ref[0, 0:LANES, 0:LANES], up_lo_ref[0, 0:LANES, 0:LANES])
    for c in range(4):
        edge = edge + dot(hm_ref[c * tmpl : (c + 1) * tmpl, :], wide(tm_hi, tm_lo, 2048 - 256 * c, LANES))
    for m in range(-3, 4):
        first, last = max(0, -m), min(3, 3 - m)
        got = dot(hm_ref[first * tmpl : (last + 1) * tmpl, :], wide(tm_hi, tm_lo, 256 * m + 1024, 256))
        for c in range(first, last + 1):
            at = 256 * (m + c)
            sm_ref[:, at : at + 256] += got[(c - first) * tmpl : (c - first + 1) * tmpl, :]
    sm_ref[:, 1024:1152] = edge
    mid_count = 1024
    v = lax.broadcasted_iota(jnp.int32, sm_ref.shape, 1) - 8 + slot * mid_count
    part_mid = jnp.where((v >= 0) & (v < slots * mid_count), sm_ref[...], 0.0)
    mid_hi, mid_lo = split(part_mid)

    def stacked(x):
        return jnp.concatenate([x[:, LANES * g : LANES * g + 256] for g in range(8)], axis=0)

    stack_hi, stack_lo = stacked(mid_hi), stacked(mid_lo)
    for r in range(4):
        got = rebuild(stack_hi, stack_lo, up_hi_ref, up_lo_ref, r)
        for g in range(8):
            at = 1024 * g + 256 * r
            out_ref[:, at : at + 256] = got[g * tmpl : (g + 1) * tmpl, :]
    high_t = Toeplitz(rows_of(xh_ref), 0, th_hi, th_lo)
    blocks = out_ref.shape[1] // 256
    copies, sent, ends = [], 0, [m for m in range(3, blocks, 4) if m < blocks - 1] + [blocks - 3, blocks - 2, blocks - 1]

    def chunk(k, first, last):
        where = (slice(None), pl.ds(256 * first, 256 * (last - first)))
        return pltpu.make_async_copy(out_ref.at[where], result_ref.at[where], sem_ref.at[k])

    for n in (1, 2, 3):
        high_t.build(n, n)
    for m in range(-3, blocks):
        high_t.build(2 * m + 8, 2 * m + 8) if 2 * m + 8 > 3 else None
        high_t.build(2 * m + 9, 2 * m + 9) if 2 * m + 9 > 3 else None
        first, last = max(0, -m), min(3, blocks - 1 - m)
        got = dot(hh_ref[first * tmpl : (last + 1) * tmpl, :], wide(th_hi, th_lo, 256 * m + 1024, 256))
        for c in range(first, last + 1):
            at = 256 * (m + c)
            out_ref[:, at : at + 256] += got[(c - first) * tmpl : (c - first + 1) * tmpl, :]
        if m in ends:
            done = chunk(len(copies), sent, m + 1)
            done.start()
            copies.append(done)
            sent = m + 1
    for done in copies:
        done.wait()


VMEM = pl.BlockSpec(memory_space=pltpu.VMEM)
SMEM = pl.BlockSpec(memory_space=pltpu.SMEM)
ANY = pl.BlockSpec(memory_space=pl.ANY)


def near(x):
    return pltpu.with_memory_space_constraint(x, pltpu.VMEM)


def place():
    return lax.axis_index("band").astype(jnp.int32), lax.axis_index("tm").astype(jnp.int32)


def call_pack(filters, parts, place=place):
    return pl.pallas_call(
        functools.partial(pack_filters, place),
        out_shape=pltpu.VMEM((parts, 24, LANES), F32),
        in_specs=[VMEM] * 3,
        out_specs=VMEM,
        scratch_shapes=[pltpu.VMEM((24, LANES), F32)],
        name="pack_filters",
    )(*filters)


def call_prepare(count, recons, strains, place=place):
    wide, basis = recons[0].shape
    half = pltpu.VMEM((wide, basis), BF16)
    return pl.pallas_call(
        functools.partial(prepare, place),
        out_shape=(half, half, half, half, pltpu.VMEM(strains[0].shape, F32), pltpu.VMEM((24, LANES), F32)),
        in_specs=[SMEM] + [VMEM] * 6,
        out_specs=(VMEM,) * 6,
        name="prepare",
    )(count, *recons, *strains)


def call_combine(got, weights, edge, second, place=place):
    wide, basis = weights[0].shape
    return pl.pallas_call(
        functools.partial(combine, place),
        out_shape=pltpu.VMEM((2 * wide + 32, LANES), F32),
        in_specs=[VMEM] * 7,
        out_specs=VMEM,
        scratch_shapes=[pltpu.VMEM((3, basis, LANES), F32)],
        name="combine",
    )(*[near(x) for x in (got, *weights, edge, second)])


def call_select(both, place=place):
    return pl.pallas_call(
        functools.partial(select, place),
        out_shape=pltpu.VMEM((both.shape[0] // 2 + 8, LANES), F32),
        in_specs=[VMEM],
        out_specs=VMEM,
        name="select",
    )(near(both))


def call_filter(own, left, right, across, second, strain, up_hi, up_lo, tmpl, count, slots, place=place):
    return pl.pallas_call(
        functools.partial(filter_and_rebuild, lambda: (*place(), slots)),
        out_shape=jax.ShapeDtypeStruct((tmpl, count), F32),
        in_specs=[VMEM] * 8,
        out_specs=ANY,
        scratch_shapes=[
            pltpu.VMEM((tmpl, count), F32),
            pltpu.SemaphoreType.DMA((count // 1024 + 2,)),
            pltpu.VMEM((72, LANES), F32),
            pltpu.VMEM((32, LANES), F32),
            pltpu.VMEM((8, LANES), F32),
            pltpu.VMEM((LANES, 9216), BF16),
            pltpu.VMEM((LANES, 9216), BF16),
            pltpu.VMEM((LANES, 2304), BF16),
            pltpu.VMEM((LANES, 2304), BF16),
            pltpu.VMEM((LANES, 256), BF16),
            pltpu.VMEM((LANES, 256), BF16),
            pltpu.VMEM((4 * tmpl, 768), BF16),
            pltpu.VMEM((4 * tmpl, 768), BF16),
            pltpu.VMEM((tmpl, 1152), F32),
            pltpu.VMEM((LANES, LANES), F32),
        ],
        name="filter_and_rebuild",
    )(*[near(x) for x in (own, left, right, across, second, strain, up_hi, up_lo)])


def interp_halves():
    exact = jnp.asarray(interp_blocks().astype(np.float32))
    return split(exact)


def local(
    strain_high, strain_mid, strain_low,
    filters_high, filters_mid, filters_low,
    recon_high, recon_mid, recon_low, basis_count,
):
    tmpl_count = lax.axis_size("tmpl")
    def turned(recon):
        basis, parts, count = recon.shape
        return jnp.transpose(recon, (1, 2, 0)).reshape(parts * count, basis)

    packed = call_pack((filters_high, filters_mid, filters_low), tmpl_count)
    *weights, strain, edge = call_prepare(
        basis_count,
        (turned(recon_high), turned(recon_mid), turned(recon_low)),
        (strain_high.reshape(-1, LANES), strain_mid.reshape(-1, LANES), strain_low.reshape(1, LANES)),
    )
    slots = lax.axis_size("tm")
    got = lax.all_to_all(packed, "tmpl", 0, 0, tiled=True)
    second = lax.ppermute(edge, "tm", [(i, i + 2) for i in range(slots - 2)])
    both = lax.all_gather(call_combine(got, weights, edge, second), "band", axis=0, tiled=True)
    own = call_select(both)

    def moved(by):
        return lax.ppermute(own, "tm", [(i, (i + by(i)) % slots) for i in range(slots)])

    across, left, right = moved(lambda i: 2 if i % 2 else -2), moved(lambda i: 1), moved(lambda i: -1)
    up_hi, up_lo = interp_halves()
    out = call_filter(
        own, left, right, across, second, strain, up_hi, up_lo, recon_high.shape[2], strain_high.shape[0], slots
    )
    return out[None]


def solution(mesh):
    in_specs = (
        P("tm"), P("tm"), P("tm"),
        P("tmpl", None), P("tmpl", None), P("tmpl", None),
        P(None, None, "tmpl"), P(None, None, "tmpl"), P(None, None, "tmpl"),
        P(),
    )
    out_specs = P("band", "tmpl", "tm")
    return jax.shard_map(local, mesh=mesh, in_specs=in_specs, out_specs=out_specs, check_vma=False)
```

```python
import functools

import jax
import jax.numpy as jnp
import numpy as np
from jax import lax
from jax.experimental import pallas as pl
from jax.experimental.pallas import tpu as pltpu
from jax.sharding import PartitionSpec as P


RATIO = 8
HALF_TAPS = 8
LANES = 128
ROWS = 8
SHARES = 4
BF16 = jnp.bfloat16
F32 = jnp.float32


def interp_blocks():
    phase = np.arange(RATIO)[:, None] / RATIO
    lag = np.arange(2 * HALF_TAPS)[None, :]
    v = phase - (lag - HALF_TAPS)
    g = np.sinc(v) * (0.5 + 0.5 * np.cos(np.pi * v / (HALF_TAPS + 1)))
    blocks = np.zeros((4, 256, 256), np.float64)
    for r in range(4):
        for n in range(256):
            for q in range(2 * HALF_TAPS):
                blocks[r, 32 * r + n // RATIO + q, n] = g[n % RATIO, q]
    return blocks


def split(x):
    hi = x.astype(BF16)
    lo = (x - hi.astype(F32)).astype(BF16)
    return hi, lo


def dot(a, b):
    return lax.dot_general(a, b, (((1,), (0,)), ((), ())), preferred_element_type=F32)


def dot3(a_hi, a_lo, b_hi, b_lo):
    left = jnp.concatenate([a_hi, a_lo, a_hi], axis=1)
    right = jnp.concatenate([b_hi, b_hi, b_lo], axis=0)
    return dot(left, right)


def rebuild(hi, lo, up_hi_ref, up_lo_ref, r):
    if r == 3:
        return dot3(hi, lo, up_hi_ref[r], up_lo_ref[r])
    first_hi, first_lo = hi[:, :LANES], lo[:, :LANES]
    return dot3(first_hi, first_lo, up_hi_ref[r, :LANES, :], up_lo_ref[r, :LANES, :])


def lane_iota(rows):
    return lax.broadcasted_iota(jnp.int32, (rows, LANES), 1)


def pack_filters(
    place, count_ref, high_ref, mid_ref, low_ref, rhigh_ref, rmid_ref, rlow_ref, shigh_ref, smid_ref, slow_ref,
    out_ref, w_hi_ref, w_lo_ref, l_hi_ref, l_lo_ref, strain_ref, edge_ref, line_ref,
):
    band, slot = place()
    share = slot % SHARES
    rows = high_ref.shape[0]
    for t in range(2):
        start = pl.multiple_of(share * 256 + t * LANES, LANES)
        high = high_ref[:, pl.ds(start, LANES)]
        mid = mid_ref[:, pl.ds(start, LANES)]
        line_ref[rows * t : rows * (t + 1), :] = jnp.where(band == 0, high, mid)
    low = pltpu.roll(low_ref[...], (LANES - 32 * share) % LANES, 1)
    turned = [low] + [pltpu.roll(low, 32 * k, 1) for k in (1, 2, 3)]
    lane = lane_iota(1)
    for first in range(0, 12, 4):
        value = jnp.zeros((1, LANES), F32)
        for q in range(first, min(first + 4, rows)):
            at = 32 * (q - first)
            value = jnp.where((lane >= at) & (lane < at + 32), turned[q - first][q : q + 1, :], value)
        line_ref[2 * rows + first // 4 : 2 * rows + first // 4 + 1, :] = value
    line_ref[2 * rows + 3 : 24, :] = jnp.zeros((24 - 2 * rows - 3, LANES), F32)
    line = line_ref[...]
    for p in range(out_ref.shape[0]):
        out_ref[p] = line
    strain_ref[0:64, :] = shigh_ref[...]
    edge_ref[0:8, :] = shigh_ref[56:64, :]
    edge_ref[8:16, :] = smid_ref[...]
    edge_ref[16:24, :] = jnp.broadcast_to(slow_ref[...], (ROWS, LANES))
    column = lax.broadcasted_iota(jnp.int32, rhigh_ref.shape, 1)
    limit = jnp.where(band == 0, count_ref[0], count_ref[1])
    weights = jnp.where(column < limit, jnp.where(band == 0, rhigh_ref[...], rmid_ref[...]), 0.0)
    w_hi_ref[...], w_lo_ref[...] = split(weights)
    l_hi_ref[...], l_lo_ref[...] = split(jnp.where(column < count_ref[2], rlow_ref[...], 0.0))


def combine(place, got_ref, w_hi_ref, w_lo_ref, l_hi_ref, l_lo_ref, edge_ref, out_ref, f_ref):
    band, _ = place()
    parts = got_ref.shape[0]
    basis = w_hi_ref.shape[1]
    rows = basis // parts
    for q in range(rows):
        at = pl.ds(q, parts, stride=rows)
        for t in range(2):
            f_ref[t, at, :] = got_ref[:, rows * t + q, :]
        low = got_ref[:, 2 * rows + q // 4, :]
        f_ref[2, at, :] = pltpu.roll(low, LANES - 32 * (q % 4), 1) if q % 4 else low
    taps = jnp.concatenate([f_ref[t] for t in range(2)], axis=1)
    h = dot3(w_hi_ref[...], w_lo_ref[...], *split(taps))
    wide = h.shape[0]
    out_ref[0:wide, :] = h[:, :LANES]
    out_ref[wide : 2 * wide, :] = h[:, LANES:]
    low = jnp.transpose(dot3(l_hi_ref[...], l_lo_ref[...], *split(f_ref[2])))[0:32, :]
    edge = jnp.concatenate([edge_ref[...], jnp.zeros((ROWS, LANES), F32)], axis=0)
    out_ref[2 * wide : 2 * wide + 32, :] = jnp.where(band == 0, edge, low)


def select(place, both_ref, out_ref):
    band, _ = place()
    size = both_ref.shape[0] // 2
    tmpl = (size - 32) // 4
    for k in range(4):
        start = size * (k // 2) + 2 * tmpl * (k % 2) + band * tmpl
        out_ref[k * tmpl : (k + 1) * tmpl, :] = both_ref[pl.ds(pl.multiple_of(start, tmpl), tmpl), :]
    low = both_ref[size + 4 * tmpl :, :]
    low = jnp.where(band == 0, low, pltpu.roll(low, 64, 1))
    tail = both_ref[4 * tmpl : 4 * tmpl + 8, :]
    mid = both_ref[4 * tmpl + 8 : 4 * tmpl + 16, :]
    strain = jnp.concatenate([pltpu.roll(tail, 64, 1), tail, pltpu.roll(mid, 64, 1), mid], axis=0)
    out_ref[4 * tmpl : 4 * tmpl + 32, :] = jnp.where(lane_iota(32) < 64, low, strain)
    out_ref[4 * tmpl + 32 :, :] = both_ref[4 * tmpl + 16 : 4 * tmpl + 24, :]


class Toeplitz:
    def __init__(self, source, shift, hi_ref, lo_ref):
        self.source, self.shift, self.hi_ref, self.lo_ref = source, shift, hi_ref, lo_ref
        self.turned = {}
        self.lane = lane_iota(ROWS)
        self.sub = lax.broadcasted_iota(jnp.int32, (ROWS, LANES), 0)

    def turn(self, group, n):
        key = (group, n)
        if key not in self.turned:
            by = (ROWS * group + self.shift) % LANES
            self.turned[key] = pltpu.roll(self.source(n), by, 1, stride=1, stride_axis=0)
        return self.turned[key]

    def eight(self, group, n):
        by = ROWS * group + self.shift
        amount = self.sub + by
        value = jnp.where(self.lane >= amount, self.turn(group, n), self.turn(group, n - 1))
        if by + ROWS - 1 > LANES:
            value = jnp.where(self.lane >= amount - LANES, value, self.turn(group, n - 2))
        return value

    def build(self, n, column):
        for pair in range(LANES // 16):
            value = jnp.concatenate([self.eight(2 * pair, n), self.eight(2 * pair + 1, n)], axis=0)
            hi, lo = split(value)
            at = (pl.ds(16 * pair, 16), pl.ds(LANES * column, LANES))
            self.hi_ref[at] = hi
            self.lo_ref[at] = lo


def wide(hi_ref, lo_ref, start, width):
    def pair(ref):
        return [ref[:, start : start + width], ref[:, start - LANES : start - LANES + width]]

    return jnp.concatenate(pair(hi_ref) + pair(hi_ref) + pair(lo_ref), axis=0)


def filter_and_rebuild(
    place, own_ref, left_ref, right_ref, across_ref, second_ref, strain_ref, up_hi_ref, up_lo_ref, result_ref,
    out_ref, sem_ref, xh_ref, ym_ref, yl_ref, th_hi, th_lo, tm_hi, tm_lo, tl_hi, tl_lo, hh_ref, hm_ref, sm_ref,
    hl_ref,
):
    _, slot, slots = place()
    tmpl = out_ref.shape[0]
    base = 4 * tmpl
    lane = lane_iota(ROWS)

    def edges(ref, keep):
        def wide(first):
            a, b = ref[first : first + 8, :], ref[first + 8 : first + 16, :]
            return jnp.where(keep, jnp.where(lane < 64, pltpu.roll(a, 64, 1), b), 0.0)

        return wide(base), wide(base + 16), jnp.where(keep, ref[base + 32 : base + 40, :], 0.0)

    here = edges(own_ref, slot >= 0)
    left = edges(left_ref, slot >= 1)
    second = [second_ref[8 * k : 8 * k + 8, :] for k in range(3)]
    right = edges(right_ref, slot < slots - 1)
    xh_ref[0:8, :] = left[0]
    xh_ref[8:72, :] = strain_ref[...]
    for k, block in enumerate((second, left, here, right)):
        ym_ref[8 * k : 8 * k + 8, :] = block[1]
        yl_ref[k : k + 1, :] = block[2][0:1, :]

    for source, ahead in ((own_ref, 0), (right_ref, 1), (across_ref, 2), (left_ref, 3)):
        share = (slot + ahead) % SHARES
        rows = pl.ds(pl.multiple_of(share * tmpl, tmpl), tmpl)
        for k in range(4):
            hi, lo = split(source[k * tmpl : (k + 1) * tmpl, :])
            ref, at = (hh_ref, hm_ref)[k // 2], LANES * (k % 2)
            ref[rows, at : at + LANES] = hi
            ref[rows, 256 + at : 256 + at + LANES] = lo
            ref[rows, 512 + at : 512 + at + LANES] = hi
        hl_ref[pl.ds(pl.multiple_of(share * 32, 32), 32), :] = source[base : base + 32, :]
    h_low = jnp.transpose(hl_ref[...])[0:tmpl, :]

    def rows_of(ref):
        return lambda n: jnp.broadcast_to(ref[n : n + 1, :], (ROWS, LANES))

    low_t = Toeplitz(rows_of(yl_ref), 9, tl_hi, tl_lo)
    low_t.build(2, 0)
    low_t.build(3, 1)
    part_low = dot3(*split(h_low), tl_hi[...], tl_lo[...])
    low_count = LANES
    z = lax.broadcasted_iota(jnp.int32, part_low.shape, 1) - 9 + slot * low_count
    part_low = jnp.where((z >= 0) & (z < slots * low_count), part_low, 0.0)
    low_hi, low_lo = split(part_low)

    mid_t = Toeplitz(rows_of(ym_ref), 8, tm_hi, tm_lo)
    for n in range(1, 17):
        mid_t.build(n + 7 + 1, n)
    for r in range(4):
        sm_ref[:, 256 * r : 256 * r + 256] = rebuild(low_hi, low_lo, up_hi_ref, up_lo_ref, r)
    edge = dot3(low_hi[:, LANES:], low_lo[:, LANES:], up_hi_ref[0, 0:LANES, 0:LANES], up_lo_ref[0, 0:LANES, 0:LANES])
    for c in range(4):
        edge = edge + dot(hm_ref[c * tmpl : (c + 1) * tmpl, :], wide(tm_hi, tm_lo, 2048 - 256 * c, LANES))
    for m in range(-3, 4):
        first, last = max(0, -m), min(3, 3 - m)
        got = dot(hm_ref[first * tmpl : (last + 1) * tmpl, :], wide(tm_hi, tm_lo, 256 * m + 1024, 256))
        for c in range(first, last + 1):
            at = 256 * (m + c)
            sm_ref[:, at : at + 256] += got[(c - first) * tmpl : (c - first + 1) * tmpl, :]
    sm_ref[:, 1024:1152] = edge
    mid_count = 1024
    v = lax.broadcasted_iota(jnp.int32, sm_ref.shape, 1) - 8 + slot * mid_count
    part_mid = jnp.where((v >= 0) & (v < slots * mid_count), sm_ref[...], 0.0)
    mid_hi, mid_lo = split(part_mid)

    def stacked(x):
        return jnp.concatenate([x[:, LANES * g : LANES * g + 256] for g in range(8)], axis=0)

    stack_hi, stack_lo = stacked(mid_hi), stacked(mid_lo)
    for r in range(4):
        got = rebuild(stack_hi, stack_lo, up_hi_ref, up_lo_ref, r)
        for g in range(8):
            at = 1024 * g + 256 * r
            out_ref[:, at : at + 256] = got[g * tmpl : (g + 1) * tmpl, :]
    high_t = Toeplitz(rows_of(xh_ref), 0, th_hi, th_lo)
    blocks = out_ref.shape[1] // 256
    copies = []

    def chunk(k):
        where = (slice(None), pl.ds(1024 * k, 1024))
        return pltpu.make_async_copy(out_ref.at[where], result_ref.at[where], sem_ref.at[k])

    for n in (1, 2, 3):
        high_t.build(n, n)
    for m in range(-3, blocks):
        high_t.build(2 * m + 8, 2 * m + 8) if 2 * m + 8 > 3 else None
        high_t.build(2 * m + 9, 2 * m + 9) if 2 * m + 9 > 3 else None
        first, last = max(0, -m), min(3, blocks - 1 - m)
        got = dot(hh_ref[first * tmpl : (last + 1) * tmpl, :], wide(th_hi, th_lo, 256 * m + 1024, 256))
        for c in range(first, last + 1):
            at = 256 * (m + c)
            out_ref[:, at : at + 256] += got[(c - first) * tmpl : (c - first + 1) * tmpl, :]
        if m % 4 == 3 and m >= 0:
            done = chunk(m // 4)
            done.start()
            copies.append(done)
    for done in copies:
        done.wait()


VMEM = pl.BlockSpec(memory_space=pltpu.VMEM)
SMEM = pl.BlockSpec(memory_space=pltpu.SMEM)
ANY = pl.BlockSpec(memory_space=pl.ANY)


def near(x):
    return pltpu.with_memory_space_constraint(x, pltpu.VMEM)


def place():
    return lax.axis_index("band").astype(jnp.int32), lax.axis_index("tm").astype(jnp.int32)


def call_pack(count, filters, recons, strains, parts, place=place):
    wide, basis = recons[0].shape
    half = pltpu.VMEM((wide, basis), BF16)
    return pl.pallas_call(
        functools.partial(pack_filters, place),
        out_shape=(
            pltpu.VMEM((parts, 24, LANES), F32), half, half, half, half,
            pltpu.VMEM(strains[0].shape, F32), pltpu.VMEM((24, LANES), F32),
        ),
        in_specs=[SMEM] + [VMEM] * 9,
        out_specs=(VMEM,) * 7,
        scratch_shapes=[pltpu.VMEM((24, LANES), F32)],
        name="pack_filters",
    )(count, *filters, *recons, *strains)


def call_combine(got, weights, edge, place=place):
    wide, basis = weights[0].shape
    return pl.pallas_call(
        functools.partial(combine, place),
        out_shape=pltpu.VMEM((2 * wide + 32, LANES), F32),
        in_specs=[VMEM] * 6,
        out_specs=VMEM,
        scratch_shapes=[pltpu.VMEM((3, basis, LANES), F32)],
        name="combine",
    )(*[near(x) for x in (got, *weights, edge)])


def call_select(both, place=place):
    return pl.pallas_call(
        functools.partial(select, place),
        out_shape=pltpu.VMEM((both.shape[0] // 2 + 8, LANES), F32),
        in_specs=[VMEM],
        out_specs=VMEM,
        name="select",
    )(near(both))


def call_filter(own, left, right, across, second, strain, up_hi, up_lo, tmpl, count, slots, place=place):
    return pl.pallas_call(
        functools.partial(filter_and_rebuild, lambda: (*place(), slots)),
        out_shape=jax.ShapeDtypeStruct((tmpl, count), F32),
        in_specs=[VMEM] * 8,
        out_specs=ANY,
        scratch_shapes=[
            pltpu.VMEM((tmpl, count), F32),
            pltpu.SemaphoreType.DMA((count // 1024,)),
            pltpu.VMEM((72, LANES), F32),
            pltpu.VMEM((32, LANES), F32),
            pltpu.VMEM((8, LANES), F32),
            pltpu.VMEM((LANES, 9216), BF16),
            pltpu.VMEM((LANES, 9216), BF16),
            pltpu.VMEM((LANES, 2304), BF16),
            pltpu.VMEM((LANES, 2304), BF16),
            pltpu.VMEM((LANES, 256), BF16),
            pltpu.VMEM((LANES, 256), BF16),
            pltpu.VMEM((4 * tmpl, 768), BF16),
            pltpu.VMEM((4 * tmpl, 768), BF16),
            pltpu.VMEM((tmpl, 1152), F32),
            pltpu.VMEM((LANES, LANES), F32),
        ],
        name="filter_and_rebuild",
    )(*[near(x) for x in (own, left, right, across, second, strain, up_hi, up_lo)])


def interp_halves():
    exact = jnp.asarray(interp_blocks().astype(np.float32))
    return split(exact)


def local(
    strain_high, strain_mid, strain_low,
    filters_high, filters_mid, filters_low,
    recon_high, recon_mid, recon_low, basis_count,
):
    tmpl_count = lax.axis_size("tmpl")

    def turned(recon):
        basis, parts, count = recon.shape
        return jnp.transpose(recon, (1, 2, 0)).reshape(parts * count, basis)

    packed, *weights, strain, edge = call_pack(
        basis_count,
        (filters_high, filters_mid, filters_low),
        (turned(recon_high), turned(recon_mid), turned(recon_low)),
        (strain_high.reshape(-1, LANES), strain_mid.reshape(-1, LANES), strain_low.reshape(1, LANES)),
        tmpl_count,
    )
    slots = lax.axis_size("tm")
    got = lax.all_to_all(packed, "tmpl", 0, 0, tiled=True)
    both = lax.all_gather(call_combine(got, weights, edge), "band", axis=0, tiled=True)
    own = call_select(both)

    def moved(pairs, value):
        return lax.ppermute(value, "tm", pairs)

    def ring(by):
        return [(i, (i + by(i)) % slots) for i in range(slots)]

    left = moved(ring(lambda i: 1), own)
    right = moved(ring(lambda i: -1), own)
    across = moved(ring(lambda i: 2 if i % 2 else -2), own)
    second = moved([(i, i + 2) for i in range(slots - 2)], edge)
    up_hi, up_lo = interp_halves()
    out = call_filter(
        own, left, right, across, second, strain, up_hi, up_lo, recon_high.shape[2], strain_high.shape[0], slots
    )
    return out[None]


def solution(mesh):
    in_specs = (
        P("tm"), P("tm"), P("tm"),
        P("tmpl", None), P("tmpl", None), P("tmpl", None),
        P(None, None, "tmpl"), P(None, None, "tmpl"), P(None, None, "tmpl"),
        P(),
    )
    out_specs = P("band", "tmpl", "tm")
    return jax.shard_map(local, mesh=mesh, in_specs=in_specs, out_specs=out_specs, check_vma=False)
```

```python
import functools

import jax
import jax.numpy as jnp
import numpy as np
from jax import lax
from jax.experimental import pallas as pl
from jax.experimental.pallas import tpu as pltpu
from jax.sharding import PartitionSpec as P

RATIO = 8
HALF_TAPS = 8
LANES = 128
ROWS = 8
SHARES = 4
BF16 = jnp.bfloat16
F32 = jnp.float32


def interp_blocks():
    phase = np.arange(RATIO)[:, None] / RATIO
    lag = np.arange(2 * HALF_TAPS)[None, :]
    v = phase - (lag - HALF_TAPS)
    g = np.sinc(v) * (0.5 + 0.5 * np.cos(np.pi * v / (HALF_TAPS + 1)))
    blocks = np.zeros((4, 256, 256), np.float64)
    for r in range(4):
        for n in range(256):
            for q in range(2 * HALF_TAPS):
                blocks[r, 32 * r + n // RATIO + q, n] = g[n % RATIO, q]
    return blocks


def split(x):
    hi = x.astype(BF16)
    lo = (x - hi.astype(F32)).astype(BF16)
    return hi, lo


def dot(a, b):
    return lax.dot_general(a, b, (((1,), (0,)), ((), ())), preferred_element_type=F32)


def dot3(a_hi, a_lo, b_hi, b_lo):
    left = jnp.concatenate([a_hi, a_lo, a_hi], axis=1)
    right = jnp.concatenate([b_hi, b_hi, b_lo], axis=0)
    return dot(left, right)


def rebuild(hi, lo, up_hi_ref, up_lo_ref, r):
    if r == 3:
        return dot3(hi, lo, up_hi_ref[r], up_lo_ref[r])
    first_hi, first_lo = hi[:, :LANES], lo[:, :LANES]
    return dot3(first_hi, first_lo, up_hi_ref[r, :LANES, :], up_lo_ref[r, :LANES, :])


def lane_iota(rows):
    return lax.broadcasted_iota(jnp.int32, (rows, LANES), 1)


def pack_filters(
    place, count_ref, high_ref, mid_ref, low_ref, rhigh_ref, rmid_ref, rlow_ref, shigh_ref, smid_ref, slow_ref,
    out_ref, w_hi_ref, w_lo_ref, l_hi_ref, l_lo_ref, strain_ref, edge_ref, line_ref,
):
    band, slot = place()
    share = slot % SHARES
    rows = high_ref.shape[0]
    for t in range(2):
        start = pl.multiple_of(share * 256 + t * LANES, LANES)
        high = high_ref[:, pl.ds(start, LANES)]
        mid = mid_ref[:, pl.ds(start, LANES)]
        line_ref[rows * t : rows * (t + 1), :] = jnp.where(band == 0, high, mid)
    low = pltpu.roll(low_ref[...], (LANES - 32 * share) % LANES, 1)
    turned = [low] + [pltpu.roll(low, 32 * k, 1) for k in (1, 2, 3)]
    lane = lane_iota(1)
    for first in range(0, 12, 4):
        value = jnp.zeros((1, LANES), F32)
        for q in range(first, min(first + 4, rows)):
            at = 32 * (q - first)
            value = jnp.where((lane >= at) & (lane < at + 32), turned[q - first][q : q + 1, :], value)
        line_ref[2 * rows + first // 4 : 2 * rows + first // 4 + 1, :] = value
    line_ref[2 * rows + 3 : 24, :] = jnp.zeros((24 - 2 * rows - 3, LANES), F32)
    line = line_ref[...]
    for p in range(out_ref.shape[0]):
        out_ref[p] = line
    strain_ref[0:64, :] = shigh_ref[...]
    edge_ref[0:8, :] = shigh_ref[56:64, :]
    edge_ref[8:16, :] = smid_ref[...]
    edge_ref[16:24, :] = jnp.broadcast_to(slow_ref[...], (ROWS, LANES))
    column = lax.broadcasted_iota(jnp.int32, rhigh_ref.shape, 1)
    limit = jnp.where(band == 0, count_ref[0], count_ref[1])
    weights = jnp.where(column < limit, jnp.where(band == 0, rhigh_ref[...], rmid_ref[...]), 0.0)
    w_hi_ref[...], w_lo_ref[...] = split(weights)
    l_hi_ref[...], l_lo_ref[...] = split(jnp.where(column < count_ref[2], rlow_ref[...], 0.0))


def combine(place, got_ref, w_hi_ref, w_lo_ref, l_hi_ref, l_lo_ref, edge_ref, out_ref, f_ref):
    band, _ = place()
    parts = got_ref.shape[0]
    basis = w_hi_ref.shape[1]
    rows = basis // parts
    for q in range(rows):
        at = pl.ds(q, parts, stride=rows)
        for t in range(2):
            f_ref[t, at, :] = got_ref[:, rows * t + q, :]
        low = got_ref[:, 2 * rows + q // 4, :]
        f_ref[2, at, :] = pltpu.roll(low, LANES - 32 * (q % 4), 1) if q % 4 else low
    taps = jnp.concatenate([f_ref[t] for t in range(2)], axis=1)
    h = dot3(w_hi_ref[...], w_lo_ref[...], *split(taps))
    wide = h.shape[0]
    out_ref[0:wide, :] = h[:, :LANES]
    out_ref[wide : 2 * wide, :] = h[:, LANES:]
    low = jnp.transpose(dot3(l_hi_ref[...], l_lo_ref[...], *split(f_ref[2])))[0:32, :]
    edge = jnp.concatenate([edge_ref[...], jnp.zeros((ROWS, LANES), F32)], axis=0)
    out_ref[2 * wide : 2 * wide + 32, :] = jnp.where(band == 0, edge, low)


def select(place, both_ref, out_ref):
    band, _ = place()
    size = both_ref.shape[0] // 2
    tmpl = (size - 32) // 4
    for k in range(4):
        start = size * (k // 2) + 2 * tmpl * (k % 2) + band * tmpl
        out_ref[k * tmpl : (k + 1) * tmpl, :] = both_ref[pl.ds(pl.multiple_of(start, tmpl), tmpl), :]
    low = both_ref[size + 4 * tmpl :, :]
    low = jnp.where(band == 0, low, pltpu.roll(low, 64, 1))
    tail = both_ref[4 * tmpl : 4 * tmpl + 8, :]
    mid = both_ref[4 * tmpl + 8 : 4 * tmpl + 16, :]
    strain = jnp.concatenate([pltpu.roll(tail, 64, 1), tail, pltpu.roll(mid, 64, 1), mid], axis=0)
    out_ref[4 * tmpl : 4 * tmpl + 32, :] = jnp.where(lane_iota(32) < 64, low, strain)
    out_ref[4 * tmpl + 32 :, :] = both_ref[4 * tmpl + 16 : 4 * tmpl + 24, :]


class Toeplitz:
    def __init__(self, source, shift, hi_ref, lo_ref):
        self.source, self.shift, self.hi_ref, self.lo_ref = source, shift, hi_ref, lo_ref
        self.turned = {}
        self.lane = lane_iota(ROWS)
        self.sub = lax.broadcasted_iota(jnp.int32, (ROWS, LANES), 0)

    def turn(self, group, n):
        key = (group, n)
        if key not in self.turned:
            by = (ROWS * group + self.shift) % LANES
            self.turned[key] = pltpu.roll(self.source(n), by, 1, stride=1, stride_axis=0)
        return self.turned[key]

    def eight(self, group, n):
        by = ROWS * group + self.shift
        amount = self.sub + by
        value = jnp.where(self.lane >= amount, self.turn(group, n), self.turn(group, n - 1))
        if by + ROWS - 1 > LANES:
            value = jnp.where(self.lane >= amount - LANES, value, self.turn(group, n - 2))
        return value

    def build(self, n, column):
        for pair in range(LANES // 16):
            value = jnp.concatenate([self.eight(2 * pair, n), self.eight(2 * pair + 1, n)], axis=0)
            hi, lo = split(value)
            at = (pl.ds(16 * pair, 16), pl.ds(LANES * column, LANES))
            self.hi_ref[at] = hi
            self.lo_ref[at] = lo


def wide(hi_ref, lo_ref, start, width):
    def pair(ref):
        return [ref[:, start : start + width], ref[:, start - LANES : start - LANES + width]]

    return jnp.concatenate(pair(hi_ref) + pair(hi_ref) + pair(lo_ref), axis=0)


def rows_of(ref):
    return lambda n: jnp.broadcast_to(ref[n : n + 1, :], (ROWS, LANES))


def filter_own(place, own_ref, strain_ref, t_hi, t_lo, out_ref):
    tmpl = out_ref.shape[0]
    blocks = out_ref.shape[1] // 256 - 3
    own = Toeplitz(lambda n: jnp.broadcast_to(strain_ref[n - 8 : n - 7, :], (ROWS, LANES)), 0, t_hi, t_lo)
    hi, lo = split(jnp.concatenate([own_ref[0:tmpl, :], own_ref[tmpl : 2 * tmpl, :]], axis=1))
    both = jnp.concatenate([hi, lo], axis=0)
    out_ref[:, 0 : 4 * 256] = jnp.zeros((tmpl, 4 * 256), F32)
    out_ref[:, blocks * 256 :] = jnp.zeros((tmpl, 3 * 256), F32)
    own.build(9, 9)
    for m in range(1, blocks - 3):
        own.build(2 * m + 8, 2 * m + 8)
        own.build(2 * m + 9, 2 * m + 9)
        start = 256 * m + 1024
        taps = [jnp.concatenate([r[:, start : start + 256], r[:, start - LANES : start + LANES]], axis=0) for r in (t_hi, t_lo)]
        first = dot(both, taps[0])
        out_ref[:, 256 * (m + 3) : 256 * (m + 4)] = first[:tmpl] + first[tmpl:] + dot(hi, taps[1])
    for n in range(2 * (blocks - 3) + 8, 2 * blocks + 8):
        own.build(n, n)


def filter_and_rebuild(
    place, own_ref, left_ref, right_ref, second_ref, strain_ref, t_hi, t_lo, done_ref, up_hi_ref, up_lo_ref, result_ref,
    out_ref, head_ref, last_ref, own_late_ref, b1_ref, b2_ref, b3_ref, sem_ref, xh_ref, ym_ref, yl_ref, th_hi, th_lo, tm_hi, tm_lo, tl_hi, tl_lo, hh_ref, hm_ref, sm_ref,
    hl_ref, hc_ref,
):
    _, slot, slots = place()
    tmpl = out_ref.shape[0]
    base = 4 * tmpl
    lane = lane_iota(ROWS)

    def edges(ref, keep):
        def wide(first):
            a, b = ref[first : first + 8, :], ref[first + 8 : first + 16, :]
            return jnp.where(keep, jnp.where(lane < 64, pltpu.roll(a, 64, 1), b), 0.0)

        return wide(base), wide(base + 16), jnp.where(keep, ref[base + 32 : base + 40, :], 0.0)

    here = edges(own_ref, slot >= 0)
    left = edges(left_ref, slot >= 1)
    second = edges(second_ref, slot >= 2)
    right = edges(right_ref, slot < slots - 1)
    xh_ref[0:8, :] = left[0]
    xh_ref[8:16, :] = strain_ref[0:8, :]
    for k, block in enumerate((second, left, here, right)):
        ym_ref[8 * k : 8 * k + 8, :] = block[1]
        yl_ref[k : k + 1, :] = block[2][0:1, :]

    for source, ahead in ((own_ref, 0), (right_ref, 1), (second_ref, 2), (left_ref, 3)):
        share = (slot + ahead) % SHARES
        for k in range(4):
            hi, lo = split(source[k * tmpl : (k + 1) * tmpl, :])
            ref, at = (hh_ref, hm_ref)[k // 2], LANES * (k % 2)
            rows = pl.ds(pl.multiple_of(share * tmpl, tmpl), tmpl) if k // 2 else slice(ahead * tmpl, (ahead + 1) * tmpl)
            places = [(ref, rows)]
            if k // 2 == 0:
                places.append((hc_ref, pl.ds(pl.multiple_of(share * tmpl, tmpl), tmpl)))
            for ref, rows in places:
                ref[rows, at : at + LANES] = hi
                ref[rows, 256 + at : 256 + at + LANES] = lo
                ref[rows, 512 + at : 512 + at + LANES] = hi
        hl_ref[pl.ds(pl.multiple_of(share * 32, 32), 32), :] = source[base : base + 32, :]
    h_low = jnp.transpose(hl_ref[...])[0:tmpl, :]

    blocks = out_ref.shape[1] // 256
    copies, sent = [], 0
    late = (own_late_ref, b1_ref, b2_ref, b3_ref)
    shares = [(slot + ahead) % SHARES for ahead in range(SHARES)]
    high_t = Toeplitz(rows_of(xh_ref), 0, th_hi, th_lo)
    mid_t = Toeplitz(rows_of(ym_ref), 8, tm_hi, tm_lo)
    low_t = Toeplitz(rows_of(yl_ref), 9, tl_hi, tl_lo)

    def column(block):
        return pl.ds(pl.multiple_of(256 * block, 256), 256)

    def columns(m):
        return slice(256 * m, 256 * m + 256)

    for ref in (head_ref, last_ref):
        ref[...] = jnp.zeros(ref.shape, F32)

    def inner(m):
        first = 0 if m == 0 else 1
        taps = wide(th_hi, th_lo, 1024, 256) if m == 0 else wide(t_hi, t_lo, 256 * m + 1024, 256)
        got = dot(hh_ref[first * tmpl :, :], taps)
        for ahead in range(first, SHARES):
            late[ahead][:, columns(m + 3)] = got[(ahead - first) * tmpl : (ahead - first + 1) * tmpl, :]

    def outer(m):
        if m < 0:
            got = dot(hc_ref[-m * tmpl :, :], wide(th_hi, th_lo, 256 * m + 1024, 256))
            for k in range(SHARES + m):
                head_ref[:, columns(k)] += got[k * tmpl : (k + 1) * tmpl, :]
        else:
            count = blocks - m
            got = dot(hc_ref[: count * tmpl, :], wide(t_hi, t_lo, 256 * m + 1024, 256))
            for k in range(count):
                last_ref[:, columns(m + k - blocks + 3)] += got[k * tmpl : (k + 1) * tmpl, :]

    def finish(a):
        value = out_ref[:, columns(a)] + done_ref[:, column(a + 3 - shares[0])]
        for ahead in range(0 if a < SHARES else 1, SHARES):
            value = value + late[ahead][:, column(a + 3 - shares[ahead])]
        if a < 3:
            value = value + head_ref[:, columns(a)]
        if a >= blocks - 3:
            value = value + last_ref[:, columns(a - blocks + 3)]
        out_ref[:, columns(a)] = value

    def send(first, last):
        where = (slice(None), pl.ds(256 * first, 256 * (last - first)))
        copy = pltpu.make_async_copy(out_ref.at[where], result_ref.at[where], sem_ref.at[len(copies)])
        copy.start()
        copies.append(copy)

    for n in range(1, 10):
        high_t.build(n, n)
    for m in (-3, -2, -1):
        outer(m)
    for m in range(0, 8):
        inner(m)
        mid_t.build(2 * m + 9, 2 * m + 1)
        mid_t.build(2 * m + 10, 2 * m + 2)

    low_t.build(2, 0)
    low_t.build(3, 1)
    part_low = dot3(*split(h_low), tl_hi[...], tl_lo[...])
    low_count = LANES
    z = lax.broadcasted_iota(jnp.int32, part_low.shape, 1) - 9 + slot * low_count
    part_low = jnp.where((z >= 0) & (z < slots * low_count), part_low, 0.0)
    low_hi, low_lo = split(part_low)

    edge = jnp.zeros((tmpl, LANES), F32)
    for c in range(4):
        edge = edge + dot(hm_ref[c * tmpl : (c + 1) * tmpl, :], wide(tm_hi, tm_lo, 2048 - 256 * c, LANES))
    for r in range(4):
        sm_ref[:, 256 * r : 256 * r + 256] = rebuild(low_hi, low_lo, up_hi_ref, up_lo_ref, r)
    sm_ref[:, 1024:1152] = edge + dot3(
        low_hi[:, LANES:], low_lo[:, LANES:], up_hi_ref[0, 0:LANES, 0:LANES], up_lo_ref[0, 0:LANES, 0:LANES]
    )
    for m in range(-3, 4):
        first, last = max(0, -m), min(3, 3 - m)
        got = dot(hm_ref[first * tmpl : (last + 1) * tmpl, :], wide(tm_hi, tm_lo, 256 * m + 1024, 256))
        for c in range(first, last + 1):
            at = 256 * (m + c)
            sm_ref[:, at : at + 256] += got[(c - first) * tmpl : (c - first + 1) * tmpl, :]
    own_late_ref[:, 0:768] = jnp.zeros((tmpl, 768), F32)
    own_late_ref[:, 1024:] = jnp.zeros((tmpl, 768), F32)
    for ref in late[1:]:
        ref[:, 0:768] = jnp.zeros((tmpl, 768), F32)
        ref[:, 256 * blocks :] = jnp.zeros((tmpl, 768), F32)
    inner(8)
    inner(9)
    mid_count = 1024
    v = lax.broadcasted_iota(jnp.int32, sm_ref.shape, 1) - 8 + slot * mid_count
    part_mid = jnp.where((v >= 0) & (v < slots * mid_count), sm_ref[...], 0.0)
    mid_hi, mid_lo = split(part_mid)

    def stacked(x):
        return jnp.concatenate([x[:, LANES * g : LANES * g + 256] for g in range(8)], axis=0)

    stack_hi, stack_lo = stacked(mid_hi), stacked(mid_lo)
    for r in range(4):
        got = rebuild(stack_hi, stack_lo, up_hi_ref, up_lo_ref, r)
        for g in range(8):
            out_ref[:, columns(4 * g + r)] = got[g * tmpl : (g + 1) * tmpl, :]
    ready = 10
    for m in range(ready, blocks):
        inner(m) if m < blocks - 3 else outer(m)
        if m == ready:
            for a in range(m + 1):
                finish(a)
        else:
            finish(m)
        if m % 4 == 3 or m >= blocks - 2:
            send(sent, m + 1)
            sent = m + 1
    for copy in copies:
        copy.wait()


VMEM = pl.BlockSpec(memory_space=pltpu.VMEM)
SMEM = pl.BlockSpec(memory_space=pltpu.SMEM)
ANY = pl.BlockSpec(memory_space=pl.ANY)


def near(x):
    return pltpu.with_memory_space_constraint(x, pltpu.VMEM)


def place():
    return lax.axis_index("band").astype(jnp.int32), lax.axis_index("tm").astype(jnp.int32)


def call_pack(count, filters, recons, strains, parts, place=place):
    wide, basis = recons[0].shape
    half = pltpu.VMEM((wide, basis), BF16)
    return pl.pallas_call(
        functools.partial(pack_filters, place),
        out_shape=(
            pltpu.VMEM((parts, 24, LANES), F32), half, half, half, half,
            pltpu.VMEM(strains[0].shape, F32), pltpu.VMEM((24, LANES), F32),
        ),
        in_specs=[SMEM] + [VMEM] * 9,
        out_specs=(VMEM,) * 7,
        scratch_shapes=[pltpu.VMEM((24, LANES), F32)],
        name="pack_filters",
    )(count, *filters, *recons, *strains)


def call_combine(got, weights, edge, place=place):
    wide, basis = weights[0].shape
    return pl.pallas_call(
        functools.partial(combine, place),
        out_shape=pltpu.VMEM((2 * wide + 32, LANES), F32),
        in_specs=[VMEM] * 6,
        out_specs=VMEM,
        scratch_shapes=[pltpu.VMEM((3, basis, LANES), F32)],
        name="combine",
    )(*[near(x) for x in (got, *weights, edge)])


def call_select(both, place=place):
    return pl.pallas_call(
        functools.partial(select, place),
        out_shape=pltpu.VMEM((both.shape[0] // 2 + 8, LANES), F32),
        in_specs=[VMEM],
        out_specs=VMEM,
        name="select",
    )(near(both))


def call_filter_own(own, strain, tmpl, count, place=place):
    half = pltpu.VMEM((LANES, count + 1024), BF16)
    return pl.pallas_call(
        functools.partial(filter_own, place),
        out_shape=(half, half, pltpu.VMEM((tmpl, count + 768), F32)),
        in_specs=[VMEM] * 2,
        out_specs=(VMEM,) * 3,
        name="filter_own",
        compiler_params=pltpu.CompilerParams(vmem_limit_bytes=24 << 20),
    )(near(own), near(strain))


def call_filter(own, left, right, second, strain, t_hi, t_lo, done, up_hi, up_lo, tmpl, count, slots, place=place):
    return pl.pallas_call(
        functools.partial(filter_and_rebuild, lambda: (*place(), slots)),
        out_shape=jax.ShapeDtypeStruct((tmpl, count), F32),
        in_specs=[VMEM] * 10,
        out_specs=ANY,
        scratch_shapes=[
            pltpu.VMEM((tmpl, count), F32),
            pltpu.VMEM((tmpl, 768), F32),
            pltpu.VMEM((tmpl, 768), F32),
            pltpu.VMEM((tmpl, 7 * 256), F32),
            pltpu.VMEM((tmpl, count + 768), F32),
            pltpu.VMEM((tmpl, count + 768), F32),
            pltpu.VMEM((tmpl, count + 768), F32),
            pltpu.SemaphoreType.DMA((count // 1024 + 1,)),
            pltpu.VMEM((16, LANES), F32),
            pltpu.VMEM((32, LANES), F32),
            pltpu.VMEM((8, LANES), F32),
            pltpu.VMEM((LANES, 1280), BF16),
            pltpu.VMEM((LANES, 1280), BF16),
            pltpu.VMEM((LANES, 2304), BF16),
            pltpu.VMEM((LANES, 2304), BF16),
            pltpu.VMEM((LANES, 256), BF16),
            pltpu.VMEM((LANES, 256), BF16),
            pltpu.VMEM((4 * tmpl, 768), BF16),
            pltpu.VMEM((4 * tmpl, 768), BF16),
            pltpu.VMEM((tmpl, 1152), F32),
            pltpu.VMEM((LANES, LANES), F32),
            pltpu.VMEM((4 * tmpl, 768), BF16),
        ],
        name="filter_and_rebuild",
        compiler_params=pltpu.CompilerParams(vmem_limit_bytes=40 << 20),
    )(*[near(x) for x in (own, left, right, second, strain, t_hi, t_lo, done, up_hi, up_lo)])


def interp_halves():
    exact = jnp.asarray(interp_blocks().astype(np.float32))
    return split(exact)


def local(
    strain_high, strain_mid, strain_low,
    filters_high, filters_mid, filters_low,
    recon_high, recon_mid, recon_low, basis_count,
):
    tmpl_count = lax.axis_size("tmpl")
    def turned(recon):
        basis, parts, count = recon.shape
        return jnp.transpose(recon, (1, 2, 0)).reshape(parts * count, basis)

    packed, *weights, strain, edge = call_pack(
        basis_count,
        (filters_high, filters_mid, filters_low),
        (turned(recon_high), turned(recon_mid), turned(recon_low)),
        (strain_high.reshape(-1, LANES), strain_mid.reshape(-1, LANES), strain_low.reshape(1, LANES)),
        tmpl_count,
    )
    slots = lax.axis_size("tm")
    got = lax.all_to_all(packed, "tmpl", 0, 0, tiled=True)
    both = lax.all_gather(call_combine(got, weights, edge), "band", axis=0, tiled=True)
    own = call_select(both)

    def moved(by):
        return lax.ppermute(own, "tm", [(i, (i + by) % slots) for i in range(slots)])

    second, left, right = moved(2), moved(1), moved(-1)
    tmpl, count = recon_high.shape[2], strain_high.shape[0]
    begun = call_filter_own(own, strain, tmpl, count)
    up_hi, up_lo = interp_halves()
    out = call_filter(own, left, right, second, strain, *begun, up_hi, up_lo, tmpl, count, slots)
    return out[None]


def solution(mesh):
    in_specs = (
        P("tm"), P("tm"), P("tm"),
        P("tmpl", None), P("tmpl", None), P("tmpl", None),
        P(None, None, "tmpl"), P(None, None, "tmpl"), P(None, None, "tmpl"),
        P(),
    )
    out_specs = P("band", "tmpl", "tm")
    return jax.shard_map(local, mesh=mesh, in_specs=in_specs, out_specs=out_specs, check_vma=False)
```

```python
import functools

import jax
import jax.numpy as jnp
import numpy as np
from jax import lax
from jax.experimental import pallas as pl
from jax.experimental.pallas import tpu as pltpu
from jax.sharding import PartitionSpec as P

RATIO = 8
HALF_TAPS = 8
LANES = 128
ROWS = 8
SHARES = 4
BF16 = jnp.bfloat16
F32 = jnp.float32


def interp_blocks():
    phase = np.arange(RATIO)[:, None] / RATIO
    lag = np.arange(2 * HALF_TAPS)[None, :]
    v = phase - (lag - HALF_TAPS)
    g = np.sinc(v) * (0.5 + 0.5 * np.cos(np.pi * v / (HALF_TAPS + 1)))
    blocks = np.zeros((4, 256, 256), np.float64)
    for r in range(4):
        for n in range(256):
            for q in range(2 * HALF_TAPS):
                blocks[r, 32 * r + n // RATIO + q, n] = g[n % RATIO, q]
    return blocks


def split(x):
    hi = x.astype(BF16)
    lo = (x - hi.astype(F32)).astype(BF16)
    return hi, lo


def dot(a, b):
    return lax.dot_general(a, b, (((1,), (0,)), ((), ())), preferred_element_type=F32)


def dot3(a_hi, a_lo, b_hi, b_lo):
    left = jnp.concatenate([a_hi, a_lo, a_hi], axis=1)
    right = jnp.concatenate([b_hi, b_hi, b_lo], axis=0)
    return dot(left, right)


def rebuild(hi, lo, up_hi_ref, up_lo_ref, r):
    if r == 3:
        return dot3(hi, lo, up_hi_ref[r], up_lo_ref[r])
    first_hi, first_lo = hi[:, :LANES], lo[:, :LANES]
    return dot3(first_hi, first_lo, up_hi_ref[r, :LANES, :], up_lo_ref[r, :LANES, :])


def lane_iota(rows):
    return lax.broadcasted_iota(jnp.int32, (rows, LANES), 1)


def pack_filters(
    place, count_ref, high_ref, mid_ref, low_ref, rhigh_ref, rmid_ref, rlow_ref, shigh_ref, smid_ref, slow_ref,
    out_ref, w_hi_ref, w_lo_ref, l_hi_ref, l_lo_ref, strain_ref, edge_ref, line_ref,
):
    band, slot = place()
    share = slot % SHARES
    rows = high_ref.shape[0]
    for t in range(2):
        start = pl.multiple_of(share * 256 + t * LANES, LANES)
        high = high_ref[:, pl.ds(start, LANES)]
        mid = mid_ref[:, pl.ds(start, LANES)]
        line_ref[rows * t : rows * (t + 1), :] = jnp.where(band == 0, high, mid)
    low = pltpu.roll(low_ref[...], (LANES - 32 * share) % LANES, 1)
    turned = [low] + [pltpu.roll(low, 32 * k, 1) for k in (1, 2, 3)]
    lane = lane_iota(1)
    for first in range(0, 12, 4):
        value = jnp.zeros((1, LANES), F32)
        for q in range(first, min(first + 4, rows)):
            at = 32 * (q - first)
            value = jnp.where((lane >= at) & (lane < at + 32), turned[q - first][q : q + 1, :], value)
        line_ref[2 * rows + first // 4 : 2 * rows + first // 4 + 1, :] = value
    line_ref[2 * rows + 3 : 24, :] = jnp.zeros((24 - 2 * rows - 3, LANES), F32)
    line = line_ref[...]
    for p in range(out_ref.shape[0]):
        out_ref[p] = line
    strain_ref[0:64, :] = shigh_ref[...]
    edge_ref[0:8, :] = shigh_ref[56:64, :]
    edge_ref[8:16, :] = smid_ref[...]
    edge_ref[16:24, :] = jnp.broadcast_to(slow_ref[...], (ROWS, LANES))
    column = lax.broadcasted_iota(jnp.int32, rhigh_ref.shape, 1)
    limit = jnp.where(band == 0, count_ref[0], count_ref[1])
    weights = jnp.where(column < limit, jnp.where(band == 0, rhigh_ref[...], rmid_ref[...]), 0.0)
    w_hi_ref[...], w_lo_ref[...] = split(weights)
    l_hi_ref[...], l_lo_ref[...] = split(jnp.where(column < count_ref[2], rlow_ref[...], 0.0))


def combine(place, got_ref, w_hi_ref, w_lo_ref, l_hi_ref, l_lo_ref, edge_ref, out_ref, f_ref):
    band, _ = place()
    parts = got_ref.shape[0]
    basis = w_hi_ref.shape[1]
    rows = basis // parts
    for q in range(rows):
        at = pl.ds(q, parts, stride=rows)
        for t in range(2):
            f_ref[t, at, :] = got_ref[:, rows * t + q, :]
        low = got_ref[:, 2 * rows + q // 4, :]
        f_ref[2, at, :] = pltpu.roll(low, LANES - 32 * (q % 4), 1) if q % 4 else low
    taps = jnp.concatenate([f_ref[t] for t in range(2)], axis=1)
    h = dot3(w_hi_ref[...], w_lo_ref[...], *split(taps))
    wide = h.shape[0]
    out_ref[0:wide, :] = h[:, :LANES]
    out_ref[wide : 2 * wide, :] = h[:, LANES:]
    low = jnp.transpose(dot3(l_hi_ref[...], l_lo_ref[...], *split(f_ref[2])))[0:32, :]
    edge = jnp.concatenate([edge_ref[...], jnp.zeros((ROWS, LANES), F32)], axis=0)
    out_ref[2 * wide : 2 * wide + 32, :] = jnp.where(band == 0, edge, low)


def select(place, both_ref, out_ref):
    band, _ = place()
    size = both_ref.shape[0] // 2
    tmpl = (size - 32) // 4
    for k in range(4):
        start = size * (k // 2) + 2 * tmpl * (k % 2) + band * tmpl
        out_ref[k * tmpl : (k + 1) * tmpl, :] = both_ref[pl.ds(pl.multiple_of(start, tmpl), tmpl), :]
    low = both_ref[size + 4 * tmpl :, :]
    low = jnp.where(band == 0, low, pltpu.roll(low, 64, 1))
    tail = both_ref[4 * tmpl : 4 * tmpl + 8, :]
    mid = both_ref[4 * tmpl + 8 : 4 * tmpl + 16, :]
    strain = jnp.concatenate([pltpu.roll(tail, 64, 1), tail, pltpu.roll(mid, 64, 1), mid], axis=0)
    out_ref[4 * tmpl : 4 * tmpl + 32, :] = jnp.where(lane_iota(32) < 64, low, strain)
    out_ref[4 * tmpl + 32 :, :] = both_ref[4 * tmpl + 16 : 4 * tmpl + 24, :]


class Toeplitz:
    def __init__(self, source, shift, hi_ref, lo_ref):
        self.source, self.shift, self.hi_ref, self.lo_ref = source, shift, hi_ref, lo_ref
        self.turned = {}
        self.lane = lane_iota(ROWS)
        self.sub = lax.broadcasted_iota(jnp.int32, (ROWS, LANES), 0)

    def turn(self, group, n):
        key = (group, n)
        if key not in self.turned:
            by = (ROWS * group + self.shift) % LANES
            self.turned[key] = pltpu.roll(self.source(n), by, 1, stride=1, stride_axis=0)
        return self.turned[key]

    def eight(self, group, n):
        by = ROWS * group + self.shift
        amount = self.sub + by
        value = jnp.where(self.lane >= amount, self.turn(group, n), self.turn(group, n - 1))
        if by + ROWS - 1 > LANES:
            value = jnp.where(self.lane >= amount - LANES, value, self.turn(group, n - 2))
        return value

    def build(self, n, column):
        for pair in range(LANES // 16):
            value = jnp.concatenate([self.eight(2 * pair, n), self.eight(2 * pair + 1, n)], axis=0)
            hi, lo = split(value)
            at = (pl.ds(16 * pair, 16), pl.ds(LANES * column, LANES))
            self.hi_ref[at] = hi
            self.lo_ref[at] = lo


def wide(hi_ref, lo_ref, start, width):
    def pair(ref):
        return [ref[:, start : start + width], ref[:, start - LANES : start - LANES + width]]

    return jnp.concatenate(pair(hi_ref) + pair(hi_ref) + pair(lo_ref), axis=0)


def narrow(hi, lo, t_hi, t_lo, start):
    two = [jnp.concatenate([r[:, start : start + 256], r[:, start - LANES : start + LANES]], axis=0) for r in (t_hi, t_lo)]
    count = hi.shape[0]
    first = dot(jnp.concatenate([hi, lo], axis=0), two[0])
    return first[:count] + first[count:] + dot(hi, two[1])


def rows_of(ref):
    return lambda n: jnp.broadcast_to(ref[n : n + 1, :], (ROWS, LANES))


def filter_own(place, own_ref, strain_ref, t_hi, t_lo, out_ref):
    tmpl = out_ref.shape[0]
    blocks = out_ref.shape[1] // 256 - 3
    own = Toeplitz(lambda n: jnp.broadcast_to(strain_ref[n - 8 : n - 7, :], (ROWS, LANES)), 0, t_hi, t_lo)
    hi, lo = split(jnp.concatenate([own_ref[0:tmpl, :], own_ref[tmpl : 2 * tmpl, :]], axis=1))
    both = jnp.concatenate([hi, lo], axis=0)
    out_ref[:, 0 : 4 * 256] = jnp.zeros((tmpl, 4 * 256), F32)
    out_ref[:, blocks * 256 :] = jnp.zeros((tmpl, 3 * 256), F32)
    own.build(9, 9)
    for m in range(1, blocks - 3):
        own.build(2 * m + 8, 2 * m + 8)
        own.build(2 * m + 9, 2 * m + 9)
        start = 256 * m + 1024
        taps = [jnp.concatenate([r[:, start : start + 256], r[:, start - LANES : start + LANES]], axis=0) for r in (t_hi, t_lo)]
        first = dot(both, taps[0])
        out_ref[:, 256 * (m + 3) : 256 * (m + 4)] = first[:tmpl] + first[tmpl:] + dot(hi, taps[1])
    for n in range(2 * (blocks - 3) + 8, 2 * blocks + 8):
        own.build(n, n)


def filter_two(right_ref, second_ref, t_hi, t_lo, b1_ref, b2_ref):
    tmpl = b1_ref.shape[0]
    blocks = b1_ref.shape[1] // 256 - 3
    taps = [jnp.concatenate([r[0:tmpl, :], r[tmpl : 2 * tmpl, :]], axis=1) for r in (right_ref, second_ref)]
    hi, lo = split(jnp.concatenate(taps, axis=0))
    for ref in (b1_ref, b2_ref):
        ref[:, 0 : 4 * 256] = jnp.zeros((tmpl, 4 * 256), F32)
        ref[:, blocks * 256 :] = jnp.zeros((tmpl, 3 * 256), F32)
    for m in range(1, blocks - 3):
        got = narrow(hi, lo, t_hi, t_lo, 256 * m + 1024)
        b1_ref[:, 256 * (m + 3) : 256 * (m + 4)] = got[:tmpl]
        b2_ref[:, 256 * (m + 3) : 256 * (m + 4)] = got[tmpl:]


def filter_and_rebuild(
    place, own_ref, left_ref, right_ref, second_ref, strain_ref, t_hi, t_lo, done_ref, b1_ref, b2_ref, up_hi_ref, up_lo_ref, result_ref,
    out_ref, head_ref, last_ref, z0_ref, z1_ref, z2_ref, b3_ref, sem_ref, xh_ref, ym_ref, yl_ref, th_hi, th_lo, tm_hi, tm_lo, tl_hi, tl_lo, hh_ref, hm_ref, sm_ref,
    hl_ref, hc_ref,
):
    _, slot, slots = place()
    tmpl = out_ref.shape[0]
    base = 4 * tmpl
    lane = lane_iota(ROWS)

    def edges(ref, keep):
        def wide(first):
            a, b = ref[first : first + 8, :], ref[first + 8 : first + 16, :]
            return jnp.where(keep, jnp.where(lane < 64, pltpu.roll(a, 64, 1), b), 0.0)

        return wide(base), wide(base + 16), jnp.where(keep, ref[base + 32 : base + 40, :], 0.0)

    here = edges(own_ref, slot >= 0)
    left = edges(left_ref, slot >= 1)
    second = edges(second_ref, slot >= 2)
    right = edges(right_ref, slot < slots - 1)
    xh_ref[0:8, :] = left[0]
    xh_ref[8:16, :] = strain_ref[0:8, :]
    for k, block in enumerate((second, left, here, right)):
        ym_ref[8 * k : 8 * k + 8, :] = block[1]
        yl_ref[k : k + 1, :] = block[2][0:1, :]

    for source, ahead in ((own_ref, 0), (right_ref, 1), (second_ref, 2), (left_ref, 3)):
        share = (slot + ahead) % SHARES
        for k in range(4):
            hi, lo = split(source[k * tmpl : (k + 1) * tmpl, :])
            ref, at = (hh_ref, hm_ref)[k // 2], LANES * (k % 2)
            rows = pl.ds(pl.multiple_of(share * tmpl, tmpl), tmpl) if k // 2 else slice(ahead * tmpl, (ahead + 1) * tmpl)
            places = [(ref, rows)]
            if k // 2 == 0:
                places.append((hc_ref, pl.ds(pl.multiple_of(share * tmpl, tmpl), tmpl)))
            for ref, rows in places:
                ref[rows, at : at + LANES] = hi
                ref[rows, 256 + at : 256 + at + LANES] = lo
                ref[rows, 512 + at : 512 + at + LANES] = hi
        hl_ref[pl.ds(pl.multiple_of(share * 32, 32), 32), :] = source[base : base + 32, :]
    h_low = jnp.transpose(hl_ref[...])[0:tmpl, :]

    blocks = out_ref.shape[1] // 256
    copies, sent = [], 0
    zero_block = (z0_ref, z1_ref, z2_ref, b3_ref)
    late = (done_ref, b1_ref, b2_ref, b3_ref)
    shares = [(slot + ahead) % SHARES for ahead in range(SHARES)]
    high_t = Toeplitz(rows_of(xh_ref), 0, th_hi, th_lo)
    mid_t = Toeplitz(rows_of(ym_ref), 8, tm_hi, tm_lo)
    low_t = Toeplitz(rows_of(yl_ref), 9, tl_hi, tl_lo)

    def column(block):
        return pl.ds(pl.multiple_of(256 * block, 256), 256)

    def columns(m):
        return slice(256 * m, 256 * m + 256)

    for ref in (head_ref, last_ref):
        ref[...] = jnp.zeros(ref.shape, F32)

    def inner(m):
        if m == 0:
            got = dot(hh_ref[...], wide(th_hi, th_lo, 1024, 256))
            for ahead, ref in enumerate(zero_block):
                ref[:, columns(3)] = got[ahead * tmpl : (ahead + 1) * tmpl, :]
            return
        hi, lo = hh_ref[3 * tmpl :, 0:256], hh_ref[3 * tmpl :, 256:512]
        b3_ref[:, columns(m + 3)] = narrow(hi, lo, t_hi, t_lo, 256 * m + 1024)

    def outer(m):
        if m < 0:
            got = dot(hc_ref[-m * tmpl :, :], wide(th_hi, th_lo, 256 * m + 1024, 256))
            for k in range(SHARES + m):
                head_ref[:, columns(k)] += got[k * tmpl : (k + 1) * tmpl, :]
        else:
            count = blocks - m
            got = dot(hc_ref[: count * tmpl, :], wide(t_hi, t_lo, 256 * m + 1024, 256))
            for k in range(count):
                last_ref[:, columns(m + k - blocks + 3)] += got[k * tmpl : (k + 1) * tmpl, :]

    def finish(a):
        value = out_ref[:, columns(a)]
        for ahead in range(SHARES):
            value = value + late[ahead][:, column(a + 3 - shares[ahead])]
            if a < SHARES and ahead < 3:
                value = value + zero_block[ahead][:, column(a + 3 - shares[ahead])]
        if a < 3:
            value = value + head_ref[:, columns(a)]
        if a >= blocks - 3:
            value = value + last_ref[:, columns(a - blocks + 3)]
        out_ref[:, columns(a)] = value

    def send(first, last):
        where = (slice(None), pl.ds(256 * first, 256 * (last - first)))
        copy = pltpu.make_async_copy(out_ref.at[where], result_ref.at[where], sem_ref.at[len(copies)])
        copy.start()
        copies.append(copy)

    for n in range(1, 10):
        high_t.build(n, n)
    for m in (-3, -2, -1):
        outer(m)
    for m in range(0, 8):
        inner(m)
        mid_t.build(2 * m + 9, 2 * m + 1)
        mid_t.build(2 * m + 10, 2 * m + 2)

    low_t.build(2, 0)
    low_t.build(3, 1)
    part_low = dot3(*split(h_low), tl_hi[...], tl_lo[...])
    low_count = LANES
    z = lax.broadcasted_iota(jnp.int32, part_low.shape, 1) - 9 + slot * low_count
    part_low = jnp.where((z >= 0) & (z < slots * low_count), part_low, 0.0)
    low_hi, low_lo = split(part_low)

    edge = jnp.zeros((tmpl, LANES), F32)
    for c in range(4):
        edge = edge + dot(hm_ref[c * tmpl : (c + 1) * tmpl, :], wide(tm_hi, tm_lo, 2048 - 256 * c, LANES))
    for r in range(4):
        sm_ref[:, 256 * r : 256 * r + 256] = rebuild(low_hi, low_lo, up_hi_ref, up_lo_ref, r)
    sm_ref[:, 1024:1152] = edge + dot3(
        low_hi[:, LANES:], low_lo[:, LANES:], up_hi_ref[0, 0:LANES, 0:LANES], up_lo_ref[0, 0:LANES, 0:LANES]
    )
    for m in range(-3, 4):
        first, last = max(0, -m), min(3, 3 - m)
        got = dot(hm_ref[first * tmpl : (last + 1) * tmpl, :], wide(tm_hi, tm_lo, 256 * m + 1024, 256))
        for c in range(first, last + 1):
            at = 256 * (m + c)
            sm_ref[:, at : at + 256] += got[(c - first) * tmpl : (c - first + 1) * tmpl, :]
    for ref in zero_block[:3]:
        ref[:, 0:768] = jnp.zeros((tmpl, 768), F32)
        ref[:, 1024:] = jnp.zeros((tmpl, 768), F32)
    b3_ref[:, 0:768] = jnp.zeros((tmpl, 768), F32)
    b3_ref[:, 256 * blocks :] = jnp.zeros((tmpl, 768), F32)
    inner(8)
    inner(9)
    mid_count = 1024
    v = lax.broadcasted_iota(jnp.int32, sm_ref.shape, 1) - 8 + slot * mid_count
    part_mid = jnp.where((v >= 0) & (v < slots * mid_count), sm_ref[...], 0.0)
    mid_hi, mid_lo = split(part_mid)

    def stacked(x):
        return jnp.concatenate([x[:, LANES * g : LANES * g + 256] for g in range(8)], axis=0)

    stack_hi, stack_lo = stacked(mid_hi), stacked(mid_lo)
    for r in range(4):
        got = rebuild(stack_hi, stack_lo, up_hi_ref, up_lo_ref, r)
        for g in range(8):
            out_ref[:, columns(4 * g + r)] = got[g * tmpl : (g + 1) * tmpl, :]
    ready = 10
    for m in range(ready, blocks):
        inner(m) if m < blocks - 3 else outer(m)
        if m == ready:
            for a in range(m + 1):
                finish(a)
        else:
            finish(m)
        if m % 4 == 3 or m >= blocks - 2:
            send(sent, m + 1)
            sent = m + 1
    for copy in copies:
        copy.wait()


VMEM = pl.BlockSpec(memory_space=pltpu.VMEM)
SMEM = pl.BlockSpec(memory_space=pltpu.SMEM)
ANY = pl.BlockSpec(memory_space=pl.ANY)


def near(x):
    return pltpu.with_memory_space_constraint(x, pltpu.VMEM)


def place():
    return lax.axis_index("band").astype(jnp.int32), lax.axis_index("tm").astype(jnp.int32)


def call_pack(count, filters, recons, strains, parts, place=place):
    wide, basis = recons[0].shape
    half = pltpu.VMEM((wide, basis), BF16)
    return pl.pallas_call(
        functools.partial(pack_filters, place),
        out_shape=(
            pltpu.VMEM((parts, 24, LANES), F32), half, half, half, half,
            pltpu.VMEM(strains[0].shape, F32), pltpu.VMEM((24, LANES), F32),
        ),
        in_specs=[SMEM] + [VMEM] * 9,
        out_specs=(VMEM,) * 7,
        scratch_shapes=[pltpu.VMEM((24, LANES), F32)],
        name="pack_filters",
    )(count, *filters, *recons, *strains)


def call_combine(got, weights, edge, place=place):
    wide, basis = weights[0].shape
    return pl.pallas_call(
        functools.partial(combine, place),
        out_shape=pltpu.VMEM((2 * wide + 32, LANES), F32),
        in_specs=[VMEM] * 6,
        out_specs=VMEM,
        scratch_shapes=[pltpu.VMEM((3, basis, LANES), F32)],
        name="combine",
    )(*[near(x) for x in (got, *weights, edge)])


def call_select(both, place=place):
    return pl.pallas_call(
        functools.partial(select, place),
        out_shape=pltpu.VMEM((both.shape[0] // 2 + 8, LANES), F32),
        in_specs=[VMEM],
        out_specs=VMEM,
        name="select",
    )(near(both))


def call_filter_own(own, strain, tmpl, count, place=place):
    half = pltpu.VMEM((LANES, count + 1024), BF16)
    return pl.pallas_call(
        functools.partial(filter_own, place),
        out_shape=(half, half, pltpu.VMEM((tmpl, count + 768), F32)),
        in_specs=[VMEM] * 2,
        out_specs=(VMEM,) * 3,
        name="filter_own",
        compiler_params=pltpu.CompilerParams(vmem_limit_bytes=24 << 20),
    )(near(own), near(strain))


def call_filter_two(right, second, t_hi, t_lo, tmpl, count):
    part = pltpu.VMEM((tmpl, count + 768), F32)
    return pl.pallas_call(
        filter_two,
        out_shape=(part, part),
        in_specs=[VMEM] * 4,
        out_specs=(VMEM,) * 2,
        name="filter_two",
        compiler_params=pltpu.CompilerParams(vmem_limit_bytes=24 << 20),
    )(*[near(x) for x in (right, second, t_hi, t_lo)])


def call_filter(own, left, right, second, strain, t_hi, t_lo, done, b1, b2, up_hi, up_lo, tmpl, count, slots, place=place):
    return pl.pallas_call(
        functools.partial(filter_and_rebuild, lambda: (*place(), slots)),
        out_shape=jax.ShapeDtypeStruct((tmpl, count), F32),
        in_specs=[VMEM] * 12,
        out_specs=ANY,
        scratch_shapes=[
            pltpu.VMEM((tmpl, count), F32),
            pltpu.VMEM((tmpl, 768), F32),
            pltpu.VMEM((tmpl, 768), F32),
            pltpu.VMEM((tmpl, 7 * 256), F32),
            pltpu.VMEM((tmpl, 7 * 256), F32),
            pltpu.VMEM((tmpl, 7 * 256), F32),
            pltpu.VMEM((tmpl, count + 768), F32),
            pltpu.SemaphoreType.DMA((count // 1024 + 1,)),
            pltpu.VMEM((16, LANES), F32),
            pltpu.VMEM((32, LANES), F32),
            pltpu.VMEM((8, LANES), F32),
            pltpu.VMEM((LANES, 1280), BF16),
            pltpu.VMEM((LANES, 1280), BF16),
            pltpu.VMEM((LANES, 2304), BF16),
            pltpu.VMEM((LANES, 2304), BF16),
            pltpu.VMEM((LANES, 256), BF16),
            pltpu.VMEM((LANES, 256), BF16),
            pltpu.VMEM((4 * tmpl, 768), BF16),
            pltpu.VMEM((4 * tmpl, 768), BF16),
            pltpu.VMEM((tmpl, 1152), F32),
            pltpu.VMEM((LANES, LANES), F32),
            pltpu.VMEM((4 * tmpl, 768), BF16),
        ],
        name="filter_and_rebuild",
        compiler_params=pltpu.CompilerParams(vmem_limit_bytes=36 << 20),
    )(*[near(x) for x in (own, left, right, second, strain, t_hi, t_lo, done, b1, b2, up_hi, up_lo)])


def interp_halves():
    exact = jnp.asarray(interp_blocks().astype(np.float32))
    return split(exact)


def local(
    strain_high, strain_mid, strain_low,
    filters_high, filters_mid, filters_low,
    recon_high, recon_mid, recon_low, basis_count,
):
    tmpl_count = lax.axis_size("tmpl")
    def turned(recon):
        basis, parts, count = recon.shape
        return jnp.transpose(recon, (1, 2, 0)).reshape(parts * count, basis)

    packed, *weights, strain, edge = call_pack(
        basis_count,
        (filters_high, filters_mid, filters_low),
        (turned(recon_high), turned(recon_mid), turned(recon_low)),
        (strain_high.reshape(-1, LANES), strain_mid.reshape(-1, LANES), strain_low.reshape(1, LANES)),
        tmpl_count,
    )
    slots = lax.axis_size("tm")
    got = lax.all_to_all(packed, "tmpl", 0, 0, tiled=True)
    both = lax.all_gather(call_combine(got, weights, edge), "band", axis=0, tiled=True)
    own = call_select(both)

    def moved(by):
        return lax.ppermute(own, "tm", [(i, (i + by) % slots) for i in range(slots)])

    second, left, right = moved(2), moved(1), moved(-1)
    tmpl, count = recon_high.shape[2], strain_high.shape[0]
    begun = call_filter_own(own, strain, tmpl, count)
    begun = (*begun, *call_filter_two(right, second, begun[0], begun[1], tmpl, count))
    up_hi, up_lo = interp_halves()
    out = call_filter(own, left, right, second, strain, *begun, up_hi, up_lo, tmpl, count, slots)
    return out[None]


def solution(mesh):
    in_specs = (
        P("tm"), P("tm"), P("tm"),
        P("tmpl", None), P("tmpl", None), P("tmpl", None),
        P(None, None, "tmpl"), P(None, None, "tmpl"), P(None, None, "tmpl"),
        P(),
    )
    out_specs = P("band", "tmpl", "tm")
    return jax.shard_map(local, mesh=mesh, in_specs=in_specs, out_specs=out_specs, check_vma=False)
```

```python
import functools

import jax
import jax.numpy as jnp
import numpy as np
from jax import lax
from jax.experimental import pallas as pl
from jax.experimental.pallas import tpu as pltpu
from jax.sharding import PartitionSpec as P

RATIO = 8
HALF_TAPS = 8
LANES = 128
ROWS = 8
SHARES = 4
BF16 = jnp.bfloat16
F32 = jnp.float32


def interp_blocks():
    phase = np.arange(RATIO)[:, None] / RATIO
    lag = np.arange(2 * HALF_TAPS)[None, :]
    v = phase - (lag - HALF_TAPS)
    g = np.sinc(v) * (0.5 + 0.5 * np.cos(np.pi * v / (HALF_TAPS + 1)))
    blocks = np.zeros((4, 256, 256), np.float64)
    for r in range(4):
        for n in range(256):
            for q in range(2 * HALF_TAPS):
                blocks[r, 32 * r + n // RATIO + q, n] = g[n % RATIO, q]
    return blocks


def split(x):
    hi = x.astype(BF16)
    lo = (x - hi.astype(F32)).astype(BF16)
    return hi, lo


def dot(a, b):
    return lax.dot_general(a, b, (((1,), (0,)), ((), ())), preferred_element_type=F32)


def dot3(a_hi, a_lo, b_hi, b_lo):
    left = jnp.concatenate([a_hi, a_lo, a_hi], axis=1)
    right = jnp.concatenate([b_hi, b_hi, b_lo], axis=0)
    return dot(left, right)


def rebuild(hi, lo, up_hi_ref, up_lo_ref, r):
    if r == 3:
        return dot3(hi, lo, up_hi_ref[r], up_lo_ref[r])
    first_hi, first_lo = hi[:, :LANES], lo[:, :LANES]
    return dot3(first_hi, first_lo, up_hi_ref[r, :LANES, :], up_lo_ref[r, :LANES, :])


def lane_iota(rows):
    return lax.broadcasted_iota(jnp.int32, (rows, LANES), 1)


def pack_filters(
    place, count_ref, high_ref, mid_ref, low_ref, rhigh_ref, rmid_ref, rlow_ref, shigh_ref, smid_ref, slow_ref,
    out_ref, w_hi_ref, w_lo_ref, l_hi_ref, l_lo_ref, strain_ref, edge_ref, line_ref,
):
    band, slot = place()
    share = slot % SHARES
    rows = high_ref.shape[0]
    for t in range(2):
        start = pl.multiple_of(share * 256 + t * LANES, LANES)
        high = high_ref[:, pl.ds(start, LANES)]
        mid = mid_ref[:, pl.ds(start, LANES)]
        line_ref[rows * t : rows * (t + 1), :] = jnp.where(band == 0, high, mid)
    low = pltpu.roll(low_ref[...], (LANES - 32 * share) % LANES, 1)
    turned = [low] + [pltpu.roll(low, 32 * k, 1) for k in (1, 2, 3)]
    lane = lane_iota(1)
    for first in range(0, 12, 4):
        value = jnp.zeros((1, LANES), F32)
        for q in range(first, min(first + 4, rows)):
            at = 32 * (q - first)
            value = jnp.where((lane >= at) & (lane < at + 32), turned[q - first][q : q + 1, :], value)
        line_ref[2 * rows + first // 4 : 2 * rows + first // 4 + 1, :] = value
    line_ref[2 * rows + 3 : 24, :] = jnp.zeros((24 - 2 * rows - 3, LANES), F32)
    line = line_ref[...]
    for p in range(out_ref.shape[0]):
        out_ref[p] = line
    strain_ref[0:64, :] = shigh_ref[...]
    edge_ref[0:8, :] = shigh_ref[56:64, :]
    edge_ref[8:16, :] = smid_ref[...]
    edge_ref[16:24, :] = jnp.broadcast_to(slow_ref[...], (ROWS, LANES))
    column = lax.broadcasted_iota(jnp.int32, rhigh_ref.shape, 1)
    limit = jnp.where(band == 0, count_ref[0], count_ref[1])
    weights = jnp.where(column < limit, jnp.where(band == 0, rhigh_ref[...], rmid_ref[...]), 0.0)
    w_hi_ref[...], w_lo_ref[...] = split(weights)
    l_hi_ref[...], l_lo_ref[...] = split(jnp.where(column < count_ref[2], rlow_ref[...], 0.0))


def combine(place, got_ref, w_hi_ref, w_lo_ref, l_hi_ref, l_lo_ref, edge_ref, out_ref, f_ref):
    band, _ = place()
    parts = got_ref.shape[0]
    basis = w_hi_ref.shape[1]
    rows = basis // parts
    for q in range(rows):
        at = pl.ds(q, parts, stride=rows)
        for t in range(2):
            f_ref[t, at, :] = got_ref[:, rows * t + q, :]
        low = got_ref[:, 2 * rows + q // 4, :]
        f_ref[2, at, :] = pltpu.roll(low, LANES - 32 * (q % 4), 1) if q % 4 else low
    taps = jnp.concatenate([f_ref[t] for t in range(2)], axis=1)
    h = dot3(w_hi_ref[...], w_lo_ref[...], *split(taps))
    wide = h.shape[0]
    out_ref[0:wide, :] = h[:, :LANES]
    out_ref[wide : 2 * wide, :] = h[:, LANES:]
    low = jnp.transpose(dot3(l_hi_ref[...], l_lo_ref[...], *split(f_ref[2])))[0:32, :]
    edge = jnp.concatenate([edge_ref[...], jnp.zeros((ROWS, LANES), F32)], axis=0)
    out_ref[2 * wide : 2 * wide + 32, :] = jnp.where(band == 0, edge, low)


def select(place, both_ref, out_ref):
    band, _ = place()
    size = both_ref.shape[0] // 2
    tmpl = (size - 32) // 4
    for k in range(4):
        start = size * (k // 2) + 2 * tmpl * (k % 2) + band * tmpl
        out_ref[k * tmpl : (k + 1) * tmpl, :] = both_ref[pl.ds(pl.multiple_of(start, tmpl), tmpl), :]
    low = both_ref[size + 4 * tmpl :, :]
    low = jnp.where(band == 0, low, pltpu.roll(low, 64, 1))
    tail = both_ref[4 * tmpl : 4 * tmpl + 8, :]
    mid = both_ref[4 * tmpl + 8 : 4 * tmpl + 16, :]
    strain = jnp.concatenate([pltpu.roll(tail, 64, 1), tail, pltpu.roll(mid, 64, 1), mid], axis=0)
    out_ref[4 * tmpl : 4 * tmpl + 32, :] = jnp.where(lane_iota(32) < 64, low, strain)
    out_ref[4 * tmpl + 32 :, :] = both_ref[4 * tmpl + 16 : 4 * tmpl + 24, :]


class Toeplitz:
    def __init__(self, source, shift, hi_ref, lo_ref):
        self.source, self.shift, self.hi_ref, self.lo_ref = source, shift, hi_ref, lo_ref
        self.turned = {}
        self.lane = lane_iota(ROWS)
        self.sub = lax.broadcasted_iota(jnp.int32, (ROWS, LANES), 0)

    def turn(self, group, n):
        key = (group, n)
        if key not in self.turned:
            by = (ROWS * group + self.shift) % LANES
            self.turned[key] = pltpu.roll(self.source(n), by, 1, stride=1, stride_axis=0)
        return self.turned[key]

    def eight(self, group, n):
        by = ROWS * group + self.shift
        amount = self.sub + by
        value = jnp.where(self.lane >= amount, self.turn(group, n), self.turn(group, n - 1))
        if by + ROWS - 1 > LANES:
            value = jnp.where(self.lane >= amount - LANES, value, self.turn(group, n - 2))
        return value

    def build(self, n, column):
        for pair in range(LANES // 16):
            value = jnp.concatenate([self.eight(2 * pair, n), self.eight(2 * pair + 1, n)], axis=0)
            hi, lo = split(value)
            at = (pl.ds(16 * pair, 16), pl.ds(LANES * column, LANES))
            self.hi_ref[at] = hi
            self.lo_ref[at] = lo


def wide(hi_ref, lo_ref, start, width):
    def pair(ref):
        return [ref[:, start : start + width], ref[:, start - LANES : start - LANES + width]]

    return jnp.concatenate(pair(hi_ref) + pair(hi_ref) + pair(lo_ref), axis=0)


def narrow(hi, lo, t_hi, t_lo, start):
    two = [jnp.concatenate([r[:, start : start + 256], r[:, start - LANES : start + LANES]], axis=0) for r in (t_hi, t_lo)]
    count = hi.shape[0]
    first = dot(jnp.concatenate([hi, lo], axis=0), two[0])
    return first[:count] + first[count:] + dot(hi, two[1])


def rows_of(ref):
    return lambda n: jnp.broadcast_to(ref[n : n + 1, :], (ROWS, LANES))


def filter_own(place, own_ref, strain_ref, t_hi, t_lo, out_ref):
    tmpl = out_ref.shape[0]
    blocks = out_ref.shape[1] // 256 - 3
    own = Toeplitz(lambda n: jnp.broadcast_to(strain_ref[n - 8 : n - 7, :], (ROWS, LANES)), 0, t_hi, t_lo)
    hi, lo = split(jnp.concatenate([own_ref[0:tmpl, :], own_ref[tmpl : 2 * tmpl, :]], axis=1))
    both = jnp.concatenate([hi, lo], axis=0)
    out_ref[:, 0 : 4 * 256] = jnp.zeros((tmpl, 4 * 256), F32)
    own.build(9, 9)
    for m in range(1, blocks):
        own.build(2 * m + 8, 2 * m + 8)
        own.build(2 * m + 9, 2 * m + 9)
        start = 256 * m + 1024
        taps = [jnp.concatenate([r[:, start : start + 256], r[:, start - LANES : start + LANES]], axis=0) for r in (t_hi, t_lo)]
        first = dot(both, taps[0])
        out_ref[:, 256 * (m + 3) : 256 * (m + 4)] = first[:tmpl] + first[tmpl:] + dot(hi, taps[1])


def column(block):
    return pl.ds(pl.multiple_of(256 * block, 256), 256)


def filter_two(place, right_ref, second_ref, t_hi, t_lo, done_ref, out_ref, b1_ref, b2_ref):
    _, slot = place()
    tmpl = out_ref.shape[0]
    blocks = out_ref.shape[1] // 256
    taps = [jnp.concatenate([r[0:tmpl, :], r[tmpl : 2 * tmpl, :]], axis=1) for r in (right_ref, second_ref)]
    hi, lo = split(jnp.concatenate(taps, axis=0))
    for ref in (b1_ref, b2_ref):
        ref[:, 0 : 4 * 256] = jnp.zeros((tmpl, 4 * 256), F32)
    for m in range(1, blocks):
        got = narrow(hi, lo, t_hi, t_lo, 256 * m + 1024)
        b1_ref[:, 256 * (m + 3) : 256 * (m + 4)] = got[:tmpl]
        b2_ref[:, 256 * (m + 3) : 256 * (m + 4)] = got[tmpl:]
        at = [column(m + 3 - (slot + ahead) % SHARES) for ahead in range(3)]
        out_ref[:, 256 * m : 256 * m + 256] = done_ref[:, at[0]] + b1_ref[:, at[1]] + b2_ref[:, at[2]]


def filter_and_rebuild(
    place, own_ref, left_ref, right_ref, second_ref, strain_ref, t_hi, t_lo, part_ref, up_hi_ref, up_lo_ref, result_ref,
    out_ref, head_ref, z0_ref, z1_ref, z2_ref, b3_ref, sem_ref, xh_ref, ym_ref, yl_ref, th_hi, th_lo, tm_hi, tm_lo, tl_hi, tl_lo, hh_ref, hm_ref, sm_ref,
    hl_ref, hc_ref,
):
    _, slot, slots = place()
    tmpl = out_ref.shape[0]
    base = 4 * tmpl
    lane = lane_iota(ROWS)

    def edges(ref, keep):
        def wide(first):
            a, b = ref[first : first + 8, :], ref[first + 8 : first + 16, :]
            return jnp.where(keep, jnp.where(lane < 64, pltpu.roll(a, 64, 1), b), 0.0)

        return wide(base), wide(base + 16), jnp.where(keep, ref[base + 32 : base + 40, :], 0.0)

    here = edges(own_ref, slot >= 0)
    left = edges(left_ref, slot >= 1)
    second = edges(second_ref, slot >= 2)
    right = edges(right_ref, slot < slots - 1)
    xh_ref[0:8, :] = left[0]
    xh_ref[8:16, :] = strain_ref[0:8, :]
    for k, block in enumerate((second, left, here, right)):
        ym_ref[8 * k : 8 * k + 8, :] = block[1]
        yl_ref[k : k + 1, :] = block[2][0:1, :]

    for source, ahead in ((own_ref, 0), (right_ref, 1), (second_ref, 2), (left_ref, 3)):
        share = (slot + ahead) % SHARES
        for k in range(4):
            hi, lo = split(source[k * tmpl : (k + 1) * tmpl, :])
            ref, at = (hh_ref, hm_ref)[k // 2], LANES * (k % 2)
            rows = pl.ds(pl.multiple_of(share * tmpl, tmpl), tmpl) if k // 2 else slice(ahead * tmpl, (ahead + 1) * tmpl)
            places = [(ref, rows)]
            if k // 2 == 0:
                places.append((hc_ref, pl.ds(pl.multiple_of(share * tmpl, tmpl), tmpl)))
            for ref, rows in places:
                ref[rows, at : at + LANES] = hi
                ref[rows, 256 + at : 256 + at + LANES] = lo
                ref[rows, 512 + at : 512 + at + LANES] = hi
        hl_ref[pl.ds(pl.multiple_of(share * 32, 32), 32), :] = source[base : base + 32, :]
    h_low = jnp.transpose(hl_ref[...])[0:tmpl, :]

    blocks = out_ref.shape[1] // 256
    copies, sent = [], 0
    zero_block = (z0_ref, z1_ref, z2_ref, b3_ref)
    shares = [(slot + ahead) % SHARES for ahead in range(SHARES)]
    high_t = Toeplitz(rows_of(xh_ref), 0, th_hi, th_lo)
    mid_t = Toeplitz(rows_of(ym_ref), 8, tm_hi, tm_lo)
    low_t = Toeplitz(rows_of(yl_ref), 9, tl_hi, tl_lo)

    def columns(m):
        return slice(256 * m, 256 * m + 256)

    head_ref[...] = jnp.zeros(head_ref.shape, F32)

    def inner(m):
        if m == 0:
            got = dot(hh_ref[...], wide(th_hi, th_lo, 1024, 256))
            for ahead, ref in enumerate(zero_block):
                ref[:, columns(3)] = got[ahead * tmpl : (ahead + 1) * tmpl, :]
            return
        hi, lo = hh_ref[3 * tmpl :, 0:256], hh_ref[3 * tmpl :, 256:512]
        b3_ref[:, columns(m + 3)] = narrow(hi, lo, t_hi, t_lo, 256 * m + 1024)

    def outer(m):
        got = dot(hc_ref[-m * tmpl :, :], wide(th_hi, th_lo, 256 * m + 1024, 256))
        for k in range(SHARES + m):
            head_ref[:, columns(k)] += got[k * tmpl : (k + 1) * tmpl, :]

    def finish(a):
        value = out_ref[:, columns(a)] + b3_ref[:, column(a + 3 - shares[3])]
        if a > 0:
            value = value + part_ref[:, columns(a)]
        if a < SHARES:
            for ahead in range(3):
                value = value + zero_block[ahead][:, column(a + 3 - shares[ahead])]
        if a < 3:
            value = value + head_ref[:, columns(a)]
        out_ref[:, columns(a)] = value

    def send(first, last):
        where = (slice(None), pl.ds(256 * first, 256 * (last - first)))
        copy = pltpu.make_async_copy(out_ref.at[where], result_ref.at[where], sem_ref.at[len(copies)])
        copy.start()
        copies.append(copy)

    for n in range(1, 10):
        high_t.build(n, n)
    for m in (-3, -2, -1):
        outer(m)
    for m in range(0, 8):
        inner(m)
        mid_t.build(2 * m + 9, 2 * m + 1)
        mid_t.build(2 * m + 10, 2 * m + 2)

    low_t.build(2, 0)
    low_t.build(3, 1)
    part_low = dot3(*split(h_low), tl_hi[...], tl_lo[...])
    low_count = LANES
    z = lax.broadcasted_iota(jnp.int32, part_low.shape, 1) - 9 + slot * low_count
    part_low = jnp.where((z >= 0) & (z < slots * low_count), part_low, 0.0)
    low_hi, low_lo = split(part_low)

    edge = jnp.zeros((tmpl, LANES), F32)
    for c in range(4):
        edge = edge + dot(hm_ref[c * tmpl : (c + 1) * tmpl, :], wide(tm_hi, tm_lo, 2048 - 256 * c, LANES))
    for r in range(4):
        sm_ref[:, 256 * r : 256 * r + 256] = rebuild(low_hi, low_lo, up_hi_ref, up_lo_ref, r)
    sm_ref[:, 1024:1152] = edge + dot3(
        low_hi[:, LANES:], low_lo[:, LANES:], up_hi_ref[0, 0:LANES, 0:LANES], up_lo_ref[0, 0:LANES, 0:LANES]
    )
    for m in range(-3, 4):
        first, last = max(0, -m), min(3, 3 - m)
        got = dot(hm_ref[first * tmpl : (last + 1) * tmpl, :], wide(tm_hi, tm_lo, 256 * m + 1024, 256))
        for c in range(first, last + 1):
            at = 256 * (m + c)
            sm_ref[:, at : at + 256] += got[(c - first) * tmpl : (c - first + 1) * tmpl, :]
    for ref in zero_block[:3]:
        ref[:, 0:768] = jnp.zeros((tmpl, 768), F32)
        ref[:, 1024:] = jnp.zeros((tmpl, 768), F32)
    b3_ref[:, 0:768] = jnp.zeros((tmpl, 768), F32)
    inner(8)
    inner(9)
    mid_count = 1024
    v = lax.broadcasted_iota(jnp.int32, sm_ref.shape, 1) - 8 + slot * mid_count
    part_mid = jnp.where((v >= 0) & (v < slots * mid_count), sm_ref[...], 0.0)
    mid_hi, mid_lo = split(part_mid)

    def stacked(x):
        return jnp.concatenate([x[:, LANES * g : LANES * g + 256] for g in range(8)], axis=0)

    stack_hi, stack_lo = stacked(mid_hi), stacked(mid_lo)
    for r in range(4):
        got = rebuild(stack_hi, stack_lo, up_hi_ref, up_lo_ref, r)
        for g in range(8):
            out_ref[:, columns(4 * g + r)] = got[g * tmpl : (g + 1) * tmpl, :]
    ready = 10
    for m in range(ready, blocks):
        inner(m)
        if m == ready:
            for a in range(m + 1):
                finish(a)
        else:
            finish(m)
        if m % 4 == 3 or m >= blocks - 2:
            send(sent, m + 1)
            sent = m + 1
    for copy in copies:
        copy.wait()


VMEM = pl.BlockSpec(memory_space=pltpu.VMEM)
SMEM = pl.BlockSpec(memory_space=pltpu.SMEM)
ANY = pl.BlockSpec(memory_space=pl.ANY)


def near(x):
    return pltpu.with_memory_space_constraint(x, pltpu.VMEM)


def place():
    return lax.axis_index("band").astype(jnp.int32), lax.axis_index("tm").astype(jnp.int32)


def call_pack(count, filters, recons, strains, parts, place=place):
    wide, basis = recons[0].shape
    half = pltpu.VMEM((wide, basis), BF16)
    return pl.pallas_call(
        functools.partial(pack_filters, place),
        out_shape=(
            pltpu.VMEM((parts, 24, LANES), F32), half, half, half, half,
            pltpu.VMEM(strains[0].shape, F32), pltpu.VMEM((24, LANES), F32),
        ),
        in_specs=[SMEM] + [VMEM] * 9,
        out_specs=(VMEM,) * 7,
        scratch_shapes=[pltpu.VMEM((24, LANES), F32)],
        name="pack_filters",
    )(count, *filters, *recons, *strains)


def call_combine(got, weights, edge, place=place):
    wide, basis = weights[0].shape
    return pl.pallas_call(
        functools.partial(combine, place),
        out_shape=pltpu.VMEM((2 * wide + 32, LANES), F32),
        in_specs=[VMEM] * 6,
        out_specs=VMEM,
        scratch_shapes=[pltpu.VMEM((3, basis, LANES), F32)],
        name="combine",
    )(*[near(x) for x in (got, *weights, edge)])


def call_select(both, place=place):
    return pl.pallas_call(
        functools.partial(select, place),
        out_shape=pltpu.VMEM((both.shape[0] // 2 + 8, LANES), F32),
        in_specs=[VMEM],
        out_specs=VMEM,
        name="select",
    )(near(both))


def call_filter_own(own, strain, tmpl, count, place=place):
    half = pltpu.VMEM((LANES, count + 1024), BF16)
    return pl.pallas_call(
        functools.partial(filter_own, place),
        out_shape=(half, half, pltpu.VMEM((tmpl, count + 768), F32)),
        in_specs=[VMEM] * 2,
        out_specs=(VMEM,) * 3,
        name="filter_own",
        compiler_params=pltpu.CompilerParams(vmem_limit_bytes=24 << 20),
    )(near(own), near(strain))


def call_filter_two(right, second, t_hi, t_lo, done, tmpl, count, place=place):
    return pl.pallas_call(
        functools.partial(filter_two, place),
        out_shape=pltpu.VMEM((tmpl, count), F32),
        in_specs=[VMEM] * 5,
        out_specs=VMEM,
        scratch_shapes=[pltpu.VMEM((tmpl, count + 768), F32)] * 2,
        name="filter_two",
        compiler_params=pltpu.CompilerParams(vmem_limit_bytes=24 << 20),
    )(*[near(x) for x in (right, second, t_hi, t_lo, done)])


def call_filter(own, left, right, second, strain, t_hi, t_lo, part, up_hi, up_lo, tmpl, count, slots, place=place):
    return pl.pallas_call(
        functools.partial(filter_and_rebuild, lambda: (*place(), slots)),
        out_shape=jax.ShapeDtypeStruct((tmpl, count), F32),
        in_specs=[VMEM] * 10,
        out_specs=ANY,
        scratch_shapes=[
            pltpu.VMEM((tmpl, count), F32),
            pltpu.VMEM((tmpl, 768), F32),
            pltpu.VMEM((tmpl, 7 * 256), F32),
            pltpu.VMEM((tmpl, 7 * 256), F32),
            pltpu.VMEM((tmpl, 7 * 256), F32),
            pltpu.VMEM((tmpl, count + 768), F32),
            pltpu.SemaphoreType.DMA((count // 1024 + 1,)),
            pltpu.VMEM((16, LANES), F32),
            pltpu.VMEM((32, LANES), F32),
            pltpu.VMEM((8, LANES), F32),
            pltpu.VMEM((LANES, 1280), BF16),
            pltpu.VMEM((LANES, 1280), BF16),
            pltpu.VMEM((LANES, 2304), BF16),
            pltpu.VMEM((LANES, 2304), BF16),
            pltpu.VMEM((LANES, 256), BF16),
            pltpu.VMEM((LANES, 256), BF16),
            pltpu.VMEM((4 * tmpl, 768), BF16),
            pltpu.VMEM((4 * tmpl, 768), BF16),
            pltpu.VMEM((tmpl, 1152), F32),
            pltpu.VMEM((LANES, LANES), F32),
            pltpu.VMEM((4 * tmpl, 768), BF16),
        ],
        name="filter_and_rebuild",
        compiler_params=pltpu.CompilerParams(vmem_limit_bytes=36 << 20),
    )(*[near(x) for x in (own, left, right, second, strain, t_hi, t_lo, part, up_hi, up_lo)])


def interp_halves():
    exact = jnp.asarray(interp_blocks().astype(np.float32))
    return split(exact)


def local(
    strain_high, strain_mid, strain_low,
    filters_high, filters_mid, filters_low,
    recon_high, recon_mid, recon_low, basis_count,
):
    tmpl_count = lax.axis_size("tmpl")
    def turned(recon):
        basis, parts, count = recon.shape
        return jnp.transpose(recon, (1, 2, 0)).reshape(parts * count, basis)

    packed, *weights, strain, edge = call_pack(
        basis_count,
        (filters_high, filters_mid, filters_low),
        (turned(recon_high), turned(recon_mid), turned(recon_low)),
        (strain_high.reshape(-1, LANES), strain_mid.reshape(-1, LANES), strain_low.reshape(1, LANES)),
        tmpl_count,
    )
    slots = lax.axis_size("tm")
    got = lax.all_to_all(packed, "tmpl", 0, 0, tiled=True)
    both = lax.all_gather(call_combine(got, weights, edge), "band", axis=0, tiled=True)
    own = call_select(both)

    def moved(by):
        return lax.ppermute(own, "tm", [(i, (i + by) % slots) for i in range(slots)])

    second, left, right = moved(2), moved(1), moved(-1)
    tmpl, count = recon_high.shape[2], strain_high.shape[0]
    t_hi, t_lo, done = call_filter_own(own, strain, tmpl, count)
    begun = (t_hi, t_lo, call_filter_two(right, second, t_hi, t_lo, done, tmpl, count))
    up_hi, up_lo = interp_halves()
    out = call_filter(own, left, right, second, strain, *begun, up_hi, up_lo, tmpl, count, slots)
    return out[None]


def solution(mesh):
    in_specs = (
        P("tm"), P("tm"), P("tm"),
        P("tmpl", None), P("tmpl", None), P("tmpl", None),
        P(None, None, "tmpl"), P(None, None, "tmpl"), P(None, None, "tmpl"),
        P(),
    )
    out_specs = P("band", "tmpl", "tm")
    return jax.shard_map(local, mesh=mesh, in_specs=in_specs, out_specs=out_specs, check_vma=False)
```

```python
import functools

import jax
import jax.numpy as jnp
import numpy as np
from jax import lax
from jax.experimental import pallas as pl
from jax.experimental.pallas import tpu as pltpu
from jax.sharding import PartitionSpec as P


RATIO = 8
HALF_TAPS = 8
LANES = 128
ROWS = 8
SHARES = 4
BF16 = jnp.bfloat16
F32 = jnp.float32


def interp_blocks():
    phase = np.arange(RATIO)[:, None] / RATIO
    lag = np.arange(2 * HALF_TAPS)[None, :]
    v = phase - (lag - HALF_TAPS)
    g = np.sinc(v) * (0.5 + 0.5 * np.cos(np.pi * v / (HALF_TAPS + 1)))
    blocks = np.zeros((4, 256, 256), np.float64)
    for r in range(4):
        for n in range(256):
            for q in range(2 * HALF_TAPS):
                blocks[r, 32 * r + n // RATIO + q, n] = g[n % RATIO, q]
    return blocks


def split(x):
    hi = x.astype(BF16)
    lo = (x - hi.astype(F32)).astype(BF16)
    return hi, lo


def dot(a, b):
    return lax.dot_general(a, b, (((1,), (0,)), ((), ())), preferred_element_type=F32)


def dot3(a_hi, a_lo, b_hi, b_lo):
    left = jnp.concatenate([a_hi, a_lo, a_hi], axis=1)
    right = jnp.concatenate([b_hi, b_hi, b_lo], axis=0)
    return dot(left, right)


def rebuild(hi, lo, up_hi_ref, up_lo_ref, r):
    if r == 3:
        return dot3(hi, lo, up_hi_ref[r], up_lo_ref[r])
    first_hi, first_lo = hi[:, :LANES], lo[:, :LANES]
    return dot3(first_hi, first_lo, up_hi_ref[r, :LANES, :], up_lo_ref[r, :LANES, :])


def lane_iota(rows):
    return lax.broadcasted_iota(jnp.int32, (rows, LANES), 1)


def pack_filters(
    place, count_ref, high_ref, mid_ref, low_ref, rhigh_ref, rmid_ref, rlow_ref, shigh_ref, smid_ref, slow_ref,
    out_ref, w_hi_ref, w_lo_ref, l_hi_ref, l_lo_ref, strain_ref, edge_ref, line_ref,
):
    band, slot = place()
    share = slot % SHARES
    rows = high_ref.shape[0]
    for t in range(2):
        start = pl.multiple_of(share * 256 + t * LANES, LANES)
        high = high_ref[:, pl.ds(start, LANES)]
        mid = mid_ref[:, pl.ds(start, LANES)]
        line_ref[rows * t : rows * (t + 1), :] = jnp.where(band == 0, high, mid)
    low = pltpu.roll(low_ref[...], (LANES - 32 * share) % LANES, 1)
    turned = [low] + [pltpu.roll(low, 32 * k, 1) for k in (1, 2, 3)]
    lane = lane_iota(1)
    for first in range(0, 12, 4):
        value = jnp.zeros((1, LANES), F32)
        for q in range(first, min(first + 4, rows)):
            at = 32 * (q - first)
            value = jnp.where((lane >= at) & (lane < at + 32), turned[q - first][q : q + 1, :], value)
        line_ref[2 * rows + first // 4 : 2 * rows + first // 4 + 1, :] = value
    line_ref[2 * rows + 3 : 24, :] = jnp.zeros((24 - 2 * rows - 3, LANES), F32)
    line = line_ref[...]
    for p in range(out_ref.shape[0]):
        out_ref[p] = line
    strain_ref[0:64, :] = shigh_ref[...]
    edge_ref[0:8, :] = shigh_ref[56:64, :]
    edge_ref[8:16, :] = smid_ref[...]
    edge_ref[16:24, :] = jnp.broadcast_to(slow_ref[...], (ROWS, LANES))
    column = lax.broadcasted_iota(jnp.int32, rhigh_ref.shape, 1)
    limit = jnp.where(band == 0, count_ref[0], count_ref[1])
    weights = jnp.where(column < limit, jnp.where(band == 0, rhigh_ref[...], rmid_ref[...]), 0.0)
    w_hi_ref[...], w_lo_ref[...] = split(weights)
    l_hi_ref[...], l_lo_ref[...] = split(jnp.where(column < count_ref[2], rlow_ref[...], 0.0))


def combine(place, got_ref, w_hi_ref, w_lo_ref, l_hi_ref, l_lo_ref, edge_ref, out_ref, f_ref):
    band, _ = place()
    parts = got_ref.shape[0]
    basis = w_hi_ref.shape[1]
    rows = basis // parts
    for q in range(rows):
        at = pl.ds(q, parts, stride=rows)
        for t in range(2):
            f_ref[t, at, :] = got_ref[:, rows * t + q, :]
        low = got_ref[:, 2 * rows + q // 4, :]
        f_ref[2, at, :] = pltpu.roll(low, LANES - 32 * (q % 4), 1) if q % 4 else low
    taps = jnp.concatenate([f_ref[t] for t in range(2)], axis=1)
    h = dot3(w_hi_ref[...], w_lo_ref[...], *split(taps))
    wide = h.shape[0]
    out_ref[0:wide, :] = h[:, :LANES]
    out_ref[wide : 2 * wide, :] = h[:, LANES:]
    low = jnp.transpose(dot3(l_hi_ref[...], l_lo_ref[...], *split(f_ref[2])))[0:32, :]
    edge = jnp.concatenate([edge_ref[...], jnp.zeros((ROWS, LANES), F32)], axis=0)
    out_ref[2 * wide : 2 * wide + 32, :] = jnp.where(band == 0, edge, low)


def select(place, both_ref, out_ref):
    band, _ = place()
    size = both_ref.shape[0] // 2
    tmpl = (size - 32) // 4
    for k in range(4):
        start = size * (k // 2) + 2 * tmpl * (k % 2) + band * tmpl
        out_ref[k * tmpl : (k + 1) * tmpl, :] = both_ref[pl.ds(pl.multiple_of(start, tmpl), tmpl), :]
    low = both_ref[size + 4 * tmpl :, :]
    low = jnp.where(band == 0, low, pltpu.roll(low, 64, 1))
    tail = both_ref[4 * tmpl : 4 * tmpl + 8, :]
    mid = both_ref[4 * tmpl + 8 : 4 * tmpl + 16, :]
    strain = jnp.concatenate([pltpu.roll(tail, 64, 1), tail, pltpu.roll(mid, 64, 1), mid], axis=0)
    out_ref[4 * tmpl : 4 * tmpl + 32, :] = jnp.where(lane_iota(32) < 64, low, strain)
    out_ref[4 * tmpl + 32 :, :] = both_ref[4 * tmpl + 16 : 4 * tmpl + 24, :]


class Toeplitz:
    def __init__(self, source, shift, hi_ref, lo_ref):
        self.source, self.shift, self.hi_ref, self.lo_ref = source, shift, hi_ref, lo_ref
        self.turned = {}
        self.lane = lane_iota(ROWS)
        self.sub = lax.broadcasted_iota(jnp.int32, (ROWS, LANES), 0)

    def turn(self, group, n):
        key = (group, n)
        if key not in self.turned:
            by = (ROWS * group + self.shift) % LANES
            self.turned[key] = pltpu.roll(self.source(n), by, 1, stride=1, stride_axis=0)
        return self.turned[key]

    def eight(self, group, n):
        by = ROWS * group + self.shift
        amount = self.sub + by
        value = jnp.where(self.lane >= amount, self.turn(group, n), self.turn(group, n - 1))
        if by + ROWS - 1 > LANES:
            value = jnp.where(self.lane >= amount - LANES, value, self.turn(group, n - 2))
        return value

    def build(self, n, column):
        for pair in range(LANES // 16):
            value = jnp.concatenate([self.eight(2 * pair, n), self.eight(2 * pair + 1, n)], axis=0)
            hi, lo = split(value)
            at = (pl.ds(16 * pair, 16), pl.ds(LANES * column, LANES))
            self.hi_ref[at] = hi
            self.lo_ref[at] = lo


def wide(hi_ref, lo_ref, start, width):
    def pair(ref):
        return [ref[:, start : start + width], ref[:, start - LANES : start - LANES + width]]

    return jnp.concatenate(pair(hi_ref) + pair(hi_ref) + pair(lo_ref), axis=0)


def narrow(hi, lo, t_hi, t_lo, start):
    two = [jnp.concatenate([r[:, start : start + 256], r[:, start - LANES : start + LANES]], axis=0) for r in (t_hi, t_lo)]
    count = hi.shape[0]
    first = dot(jnp.concatenate([hi, lo], axis=0), two[0])
    return first[:count] + first[count:] + dot(hi, two[1])


def rows_of(ref):
    return lambda n: jnp.broadcast_to(ref[n : n + 1, :], (ROWS, LANES))


def filter_own(own_ref, strain_ref, t_hi, t_lo, out_ref):
    tmpl = out_ref.shape[0]
    blocks = out_ref.shape[1] // 256 - 3
    own = Toeplitz(lambda n: jnp.broadcast_to(strain_ref[n - 8 : n - 7, :], (ROWS, LANES)), 0, t_hi, t_lo)
    hi, lo = split(jnp.concatenate([own_ref[0:tmpl, :], own_ref[tmpl : 2 * tmpl, :]], axis=1))
    both = jnp.concatenate([hi, lo], axis=0)
    out_ref[:, 0 : 4 * 256] = jnp.zeros((tmpl, 4 * 256), F32)
    own.build(9, 9)
    for m in range(1, blocks):
        own.build(2 * m + 8, 2 * m + 8)
        own.build(2 * m + 9, 2 * m + 9)
        start = 256 * m + 1024
        taps = [jnp.concatenate([r[:, start : start + 256], r[:, start - LANES : start + LANES]], axis=0) for r in (t_hi, t_lo)]
        first = dot(both, taps[0])
        out_ref[:, 256 * (m + 3) : 256 * (m + 4)] = first[:tmpl] + first[tmpl:] + dot(hi, taps[1])


def column(block):
    return pl.ds(pl.multiple_of(256 * block, 256), 256)


def filter_two(place, right_ref, second_ref, t_hi, t_lo, done_ref, out_ref, b1_ref, b2_ref):
    _, slot = place()
    tmpl = out_ref.shape[0]
    blocks = out_ref.shape[1] // 256
    taps = [jnp.concatenate([r[0:tmpl, :], r[tmpl : 2 * tmpl, :]], axis=1) for r in (right_ref, second_ref)]
    hi, lo = split(jnp.concatenate(taps, axis=0))
    for ref in (b1_ref, b2_ref):
        ref[:, 0 : 4 * 256] = jnp.zeros((tmpl, 4 * 256), F32)
    for m in range(1, blocks):
        got = narrow(hi, lo, t_hi, t_lo, 256 * m + 1024)
        b1_ref[:, 256 * (m + 3) : 256 * (m + 4)] = got[:tmpl]
        b2_ref[:, 256 * (m + 3) : 256 * (m + 4)] = got[tmpl:]
        at = [column(m + 3 - (slot + ahead) % SHARES) for ahead in range(3)]
        out_ref[:, 256 * m : 256 * m + 256] = done_ref[:, at[0]] + b1_ref[:, at[1]] + b2_ref[:, at[2]]


def filter_and_rebuild(
    place, own_ref, left_ref, right_ref, second_ref, strain_ref, t_hi, t_lo, part_ref, up_hi_ref, up_lo_ref, result_ref,
    out_ref, head_ref, z0_ref, z1_ref, z2_ref, b3_ref, sem_ref, xh_ref, ym_ref, yl_ref, th_hi, th_lo, tm_hi, tm_lo, tl_hi, tl_lo, hh_ref, hm_ref, sm_ref,
    hl_ref, hc_ref,
):
    _, slot, slots = place()
    tmpl = out_ref.shape[0]
    base = 4 * tmpl
    lane = lane_iota(ROWS)

    def edges(ref, keep):
        def wide(first):
            a, b = ref[first : first + 8, :], ref[first + 8 : first + 16, :]
            return jnp.where(keep, jnp.where(lane < 64, pltpu.roll(a, 64, 1), b), 0.0)

        return wide(base), wide(base + 16), jnp.where(keep, ref[base + 32 : base + 40, :], 0.0)

    here = edges(own_ref, slot >= 0)
    left = edges(left_ref, slot >= 1)
    second = edges(second_ref, slot >= 2)
    right = edges(right_ref, slot < slots - 1)
    xh_ref[0:8, :] = left[0]
    xh_ref[8:16, :] = strain_ref[0:8, :]
    for k, block in enumerate((second, left, here, right)):
        ym_ref[8 * k : 8 * k + 8, :] = block[1]
        yl_ref[k : k + 1, :] = block[2][0:1, :]

    for source, ahead in ((own_ref, 0), (right_ref, 1), (second_ref, 2), (left_ref, 3)):
        share = (slot + ahead) % SHARES
        for k in range(4):
            hi, lo = split(source[k * tmpl : (k + 1) * tmpl, :])
            ref, at = (hh_ref, hm_ref)[k // 2], LANES * (k % 2)
            rows = pl.ds(pl.multiple_of(share * tmpl, tmpl), tmpl) if k // 2 else slice(ahead * tmpl, (ahead + 1) * tmpl)
            places = [(ref, rows)]
            if k // 2 == 0:
                places.append((hc_ref, pl.ds(pl.multiple_of(share * tmpl, tmpl), tmpl)))
            for ref, rows in places:
                ref[rows, at : at + LANES] = hi
                ref[rows, 256 + at : 256 + at + LANES] = lo
                ref[rows, 512 + at : 512 + at + LANES] = hi
        hl_ref[pl.ds(pl.multiple_of(share * 32, 32), 32), :] = source[base : base + 32, :]
    h_low = jnp.transpose(hl_ref[...])[0:tmpl, :]

    blocks = out_ref.shape[1] // 256
    copies, sent = [], 0
    zero_block = (z0_ref, z1_ref, z2_ref, b3_ref)
    shares = [(slot + ahead) % SHARES for ahead in range(SHARES)]
    high_t = Toeplitz(rows_of(xh_ref), 0, th_hi, th_lo)
    mid_t = Toeplitz(rows_of(ym_ref), 8, tm_hi, tm_lo)
    low_t = Toeplitz(rows_of(yl_ref), 9, tl_hi, tl_lo)

    def columns(m):
        return slice(256 * m, 256 * m + 256)

    head_ref[...] = jnp.zeros(head_ref.shape, F32)

    def inner(m):
        if m == 0:
            got = dot(hh_ref[...], wide(th_hi, th_lo, 1024, 256))
            for ahead, ref in enumerate(zero_block):
                ref[:, columns(3)] = got[ahead * tmpl : (ahead + 1) * tmpl, :]
            return
        hi, lo = hh_ref[3 * tmpl :, 0:256], hh_ref[3 * tmpl :, 256:512]
        b3_ref[:, columns(m + 3)] = narrow(hi, lo, t_hi, t_lo, 256 * m + 1024)

    def outer(m):
        got = dot(hc_ref[-m * tmpl :, :], wide(th_hi, th_lo, 256 * m + 1024, 256))
        for k in range(SHARES + m):
            head_ref[:, columns(k)] += got[k * tmpl : (k + 1) * tmpl, :]

    def finish(a):
        value = out_ref[:, columns(a)] + b3_ref[:, column(a + 3 - shares[3])]
        if a > 0:
            value = value + part_ref[:, columns(a)]
        if a < SHARES:
            for ahead in range(3):
                value = value + zero_block[ahead][:, column(a + 3 - shares[ahead])]
        if a < 3:
            value = value + head_ref[:, columns(a)]
        out_ref[:, columns(a)] = value

    def send(first, last):
        where = (slice(None), pl.ds(256 * first, 256 * (last - first)))
        copy = pltpu.make_async_copy(out_ref.at[where], result_ref.at[where], sem_ref.at[len(copies)])
        copy.start()
        copies.append(copy)

    for n in range(1, 10):
        high_t.build(n, n)
    for m in (-3, -2, -1):
        outer(m)
    for m in range(0, 8):
        inner(m)
        mid_t.build(2 * m + 9, 2 * m + 1)
        mid_t.build(2 * m + 10, 2 * m + 2)

    low_t.build(2, 0)
    low_t.build(3, 1)
    part_low = dot3(*split(h_low), tl_hi[...], tl_lo[...])
    low_count = LANES
    z = lax.broadcasted_iota(jnp.int32, part_low.shape, 1) - 9 + slot * low_count
    part_low = jnp.where((z >= 0) & (z < slots * low_count), part_low, 0.0)
    low_hi, low_lo = split(part_low)

    edge = jnp.zeros((tmpl, LANES), F32)
    for c in range(4):
        edge = edge + dot(hm_ref[c * tmpl : (c + 1) * tmpl, :], wide(tm_hi, tm_lo, 2048 - 256 * c, LANES))
    for r in range(4):
        sm_ref[:, 256 * r : 256 * r + 256] = rebuild(low_hi, low_lo, up_hi_ref, up_lo_ref, r)
    sm_ref[:, 1024:1152] = edge + dot3(
        low_hi[:, LANES:], low_lo[:, LANES:], up_hi_ref[0, 0:LANES, 0:LANES], up_lo_ref[0, 0:LANES, 0:LANES]
    )
    for m in range(-3, 4):
        first, last = max(0, -m), min(3, 3 - m)
        got = dot(hm_ref[first * tmpl : (last + 1) * tmpl, :], wide(tm_hi, tm_lo, 256 * m + 1024, 256))
        for c in range(first, last + 1):
            at = 256 * (m + c)
            sm_ref[:, at : at + 256] += got[(c - first) * tmpl : (c - first + 1) * tmpl, :]
    for ref in zero_block[:3]:
        ref[:, 0:768] = jnp.zeros((tmpl, 768), F32)
        ref[:, 1024:] = jnp.zeros((tmpl, 768), F32)
    b3_ref[:, 0:768] = jnp.zeros((tmpl, 768), F32)
    inner(8)
    inner(9)
    mid_count = 1024
    v = lax.broadcasted_iota(jnp.int32, sm_ref.shape, 1) - 8 + slot * mid_count
    part_mid = jnp.where((v >= 0) & (v < slots * mid_count), sm_ref[...], 0.0)
    mid_hi, mid_lo = split(part_mid)

    def stacked(x):
        return jnp.concatenate([x[:, LANES * g : LANES * g + 256] for g in range(8)], axis=0)

    stack_hi, stack_lo = stacked(mid_hi), stacked(mid_lo)
    for r in range(4):
        got = rebuild(stack_hi, stack_lo, up_hi_ref, up_lo_ref, r)
        for g in range(8):
            out_ref[:, columns(4 * g + r)] = got[g * tmpl : (g + 1) * tmpl, :]
    ready = 10
    for m in range(ready, blocks):
        inner(m)
        if m == ready:
            for a in range(m + 1):
                finish(a)
        else:
            finish(m)
        if m % 4 == 3 or m >= blocks - 2:
            send(sent, m + 1)
            sent = m + 1
    for copy in copies:
        copy.wait()


VMEM = pl.BlockSpec(memory_space=pltpu.VMEM)
SMEM = pl.BlockSpec(memory_space=pltpu.SMEM)
ANY = pl.BlockSpec(memory_space=pl.ANY)


def near(x):
    return pltpu.with_memory_space_constraint(x, pltpu.VMEM)


def place():
    return lax.axis_index("band").astype(jnp.int32), lax.axis_index("tm").astype(jnp.int32)


def call_pack(count, filters, recons, strains, parts, place=place):
    wide, basis = recons[0].shape
    half = pltpu.VMEM((wide, basis), BF16)
    return pl.pallas_call(
        functools.partial(pack_filters, place),
        out_shape=(
            pltpu.VMEM((parts, 24, LANES), F32), half, half, half, half,
            pltpu.VMEM(strains[0].shape, F32), pltpu.VMEM((24, LANES), F32),
        ),
        in_specs=[SMEM] + [VMEM] * 9,
        out_specs=(VMEM,) * 7,
        scratch_shapes=[pltpu.VMEM((24, LANES), F32)],
        name="pack_filters",
    )(count, *filters, *recons, *strains)


def call_combine(got, weights, edge, place=place):
    wide, basis = weights[0].shape
    return pl.pallas_call(
        functools.partial(combine, place),
        out_shape=pltpu.VMEM((2 * wide + 32, LANES), F32),
        in_specs=[VMEM] * 6,
        out_specs=VMEM,
        scratch_shapes=[pltpu.VMEM((3, basis, LANES), F32)],
        name="combine",
    )(*[near(x) for x in (got, *weights, edge)])


def call_select(both, place=place):
    return pl.pallas_call(
        functools.partial(select, place),
        out_shape=pltpu.VMEM((both.shape[0] // 2 + 8, LANES), F32),
        in_specs=[VMEM],
        out_specs=VMEM,
        name="select",
    )(near(both))


def call_filter_own(own, strain, tmpl, count):
    half = pltpu.VMEM((LANES, count + 1024), BF16)
    return pl.pallas_call(
        filter_own,
        out_shape=(half, half, pltpu.VMEM((tmpl, count + 768), F32)),
        in_specs=[VMEM] * 2,
        out_specs=(VMEM,) * 3,
        name="filter_own",
        compiler_params=pltpu.CompilerParams(vmem_limit_bytes=24 << 20),
    )(near(own), near(strain))


def call_filter_two(right, second, t_hi, t_lo, done, tmpl, count, place=place):
    return pl.pallas_call(
        functools.partial(filter_two, place),
        out_shape=pltpu.VMEM((tmpl, count), F32),
        in_specs=[VMEM] * 5,
        out_specs=VMEM,
        scratch_shapes=[pltpu.VMEM((tmpl, count + 768), F32)] * 2,
        name="filter_two",
        compiler_params=pltpu.CompilerParams(vmem_limit_bytes=24 << 20),
    )(*[near(x) for x in (right, second, t_hi, t_lo, done)])


def call_filter(own, left, right, second, strain, t_hi, t_lo, part, up_hi, up_lo, tmpl, count, slots, place=place):
    return pl.pallas_call(
        functools.partial(filter_and_rebuild, lambda: (*place(), slots)),
        out_shape=jax.ShapeDtypeStruct((tmpl, count), F32),
        in_specs=[VMEM] * 10,
        out_specs=ANY,
        scratch_shapes=[
            pltpu.VMEM((tmpl, count), F32),
            pltpu.VMEM((tmpl, 768), F32),
            pltpu.VMEM((tmpl, 7 * 256), F32),
            pltpu.VMEM((tmpl, 7 * 256), F32),
            pltpu.VMEM((tmpl, 7 * 256), F32),
            pltpu.VMEM((tmpl, count + 768), F32),
            pltpu.SemaphoreType.DMA((count // 1024 + 1,)),
            pltpu.VMEM((16, LANES), F32),
            pltpu.VMEM((32, LANES), F32),
            pltpu.VMEM((8, LANES), F32),
            pltpu.VMEM((LANES, 1280), BF16),
            pltpu.VMEM((LANES, 1280), BF16),
            pltpu.VMEM((LANES, 2304), BF16),
            pltpu.VMEM((LANES, 2304), BF16),
            pltpu.VMEM((LANES, 256), BF16),
            pltpu.VMEM((LANES, 256), BF16),
            pltpu.VMEM((4 * tmpl, 768), BF16),
            pltpu.VMEM((4 * tmpl, 768), BF16),
            pltpu.VMEM((tmpl, 1152), F32),
            pltpu.VMEM((LANES, LANES), F32),
            pltpu.VMEM((4 * tmpl, 768), BF16),
        ],
        name="filter_and_rebuild",
        compiler_params=pltpu.CompilerParams(vmem_limit_bytes=36 << 20),
    )(*[near(x) for x in (own, left, right, second, strain, t_hi, t_lo, part, up_hi, up_lo)])


def interp_halves():
    exact = jnp.asarray(interp_blocks().astype(np.float32))
    return split(exact)


def local(
    strain_high, strain_mid, strain_low,
    filters_high, filters_mid, filters_low,
    recon_high, recon_mid, recon_low, basis_count,
):
    tmpl_count = lax.axis_size("tmpl")

    def turned(recon):
        basis, parts, count = recon.shape
        return jnp.transpose(recon, (1, 2, 0)).reshape(parts * count, basis)

    packed, *weights, strain, edge = call_pack(
        basis_count,
        (filters_high, filters_mid, filters_low),
        (turned(recon_high), turned(recon_mid), turned(recon_low)),
        (strain_high.reshape(-1, LANES), strain_mid.reshape(-1, LANES), strain_low.reshape(1, LANES)),
        tmpl_count,
    )
    slots = lax.axis_size("tm")
    got = lax.all_to_all(packed, "tmpl", 0, 0, tiled=True)
    both = lax.all_gather(call_combine(got, weights, edge), "band", axis=0, tiled=True)
    own = call_select(both)

    def moved(by):
        return lax.ppermute(own, "tm", [(i, (i + by) % slots) for i in range(slots)])

    second, right, left = moved(2), moved(-1), moved(1)
    tmpl, count = recon_high.shape[2], strain_high.shape[0]
    t_hi, t_lo, done = call_filter_own(own, strain, tmpl, count)
    begun = (t_hi, t_lo, call_filter_two(right, second, t_hi, t_lo, done, tmpl, count))
    up_hi, up_lo = interp_halves()
    out = call_filter(own, left, right, second, strain, *begun, up_hi, up_lo, tmpl, count, slots)
    return out[None]


def solution(mesh):
    in_specs = (
        P("tm"), P("tm"), P("tm"),
        P("tmpl", None), P("tmpl", None), P("tmpl", None),
        P(None, None, "tmpl"), P(None, None, "tmpl"), P(None, None, "tmpl"),
        P(),
    )
    out_specs = P("band", "tmpl", "tm")
    return jax.shard_map(local, mesh=mesh, in_specs=in_specs, out_specs=out_specs, check_vma=False)
```

```python
import functools

import jax
import jax.numpy as jnp
import numpy as np
from jax import lax
from jax.experimental import pallas as pl
from jax.experimental.pallas import tpu as pltpu
from jax.sharding import PartitionSpec as P


RATIO = 8
HALF_TAPS = 8
LANES = 128
ROWS = 8
SHARES = 4
BF16 = jnp.bfloat16
F32 = jnp.float32


def interp_blocks():
    phase = np.arange(RATIO)[:, None] / RATIO
    lag = np.arange(2 * HALF_TAPS)[None, :]
    v = phase - (lag - HALF_TAPS)
    g = np.sinc(v) * (0.5 + 0.5 * np.cos(np.pi * v / (HALF_TAPS + 1)))
    blocks = np.zeros((4, 256, 256), np.float64)
    for r in range(4):
        for n in range(256):
            for q in range(2 * HALF_TAPS):
                blocks[r, 32 * r + n // RATIO + q, n] = g[n % RATIO, q]
    return blocks


def split(x):
    hi = x.astype(BF16)
    lo = (x - hi.astype(F32)).astype(BF16)
    return hi, lo


def dot(a, b):
    return lax.dot_general(a, b, (((1,), (0,)), ((), ())), preferred_element_type=F32)


def dot3(a_hi, a_lo, b_hi, b_lo):
    left = jnp.concatenate([a_hi, a_lo, a_hi], axis=1)
    right = jnp.concatenate([b_hi, b_hi, b_lo], axis=0)
    return dot(left, right)


def rebuild(hi, lo, up_hi_ref, up_lo_ref, r):
    if r == 3:
        return dot3(hi, lo, up_hi_ref[r], up_lo_ref[r])
    first_hi, first_lo = hi[:, :LANES], lo[:, :LANES]
    return dot3(first_hi, first_lo, up_hi_ref[r, :LANES, :], up_lo_ref[r, :LANES, :])


def lane_iota(rows):
    return lax.broadcasted_iota(jnp.int32, (rows, LANES), 1)


def pack_filters(
    place, count_ref, high_ref, mid_ref, low_ref, rhigh_ref, rmid_ref, rlow_ref, shigh_ref, smid_ref, slow_ref,
    out_ref, w_hi_ref, w_lo_ref, l_hi_ref, l_lo_ref, strain_ref, edge_ref, line_ref,
):
    band, slot = place()
    share = slot % SHARES
    rows = high_ref.shape[0]
    for t in range(2):
        start = pl.multiple_of(share * 256 + t * LANES, LANES)
        high = high_ref[:, pl.ds(start, LANES)]
        mid = mid_ref[:, pl.ds(start, LANES)]
        line_ref[rows * t : rows * (t + 1), :] = jnp.where(band == 0, high, mid)
    low = pltpu.roll(low_ref[...], (LANES - 32 * share) % LANES, 1)
    turned = [low] + [pltpu.roll(low, 32 * k, 1) for k in (1, 2, 3)]
    lane = lane_iota(1)
    for first in range(0, 12, 4):
        value = jnp.zeros((1, LANES), F32)
        for q in range(first, min(first + 4, rows)):
            at = 32 * (q - first)
            value = jnp.where((lane >= at) & (lane < at + 32), turned[q - first][q : q + 1, :], value)
        line_ref[2 * rows + first // 4 : 2 * rows + first // 4 + 1, :] = value
    line_ref[2 * rows + 3 : 24, :] = jnp.zeros((24 - 2 * rows - 3, LANES), F32)
    line = jnp.concatenate([line_ref[8 * k : 8 * k + 8, :] for k in range(3)], axis=1)
    for p in range(out_ref.shape[0]):
        out_ref[p] = line
    strain_ref[0:64, :] = shigh_ref[...]
    edge_ref[0:8, :] = shigh_ref[56:64, :]
    edge_ref[8:16, :] = smid_ref[...]
    edge_ref[16:24, :] = jnp.broadcast_to(slow_ref[...], (ROWS, LANES))
    column = lax.broadcasted_iota(jnp.int32, rhigh_ref.shape, 1)
    limit = jnp.where(band == 0, count_ref[0], count_ref[1])
    weights = jnp.where(column < limit, jnp.where(band == 0, rhigh_ref[...], rmid_ref[...]), 0.0)
    w_hi_ref[...], w_lo_ref[...] = split(weights)
    l_hi_ref[...], l_lo_ref[...] = split(jnp.where(column < count_ref[2], rlow_ref[...], 0.0))


def combine(place, got_ref, w_hi_ref, w_lo_ref, l_hi_ref, l_lo_ref, edge_ref, out_ref, f_ref):
    band, _ = place()
    parts = got_ref.shape[0]
    basis = w_hi_ref.shape[1]
    rows = basis // parts

    def row(k):
        return got_ref[:, k % 8, LANES * (k // 8) : LANES * (k // 8 + 1)]

    for q in range(rows):
        at = pl.ds(q, parts, stride=rows)
        for t in range(2):
            f_ref[t, at, :] = row(rows * t + q)
        low = row(2 * rows + q // 4)
        f_ref[2, at, :] = pltpu.roll(low, LANES - 32 * (q % 4), 1) if q % 4 else low
    taps = jnp.concatenate([f_ref[t] for t in range(2)], axis=1)
    h = dot3(w_hi_ref[...], w_lo_ref[...], *split(taps))
    wide = h.shape[0]
    out_ref[0:wide, :] = h[:, :LANES]
    out_ref[wide : 2 * wide, :] = h[:, LANES:]
    low = jnp.transpose(dot3(l_hi_ref[...], l_lo_ref[...], *split(f_ref[2])))[0:32, :]
    edge = jnp.concatenate([edge_ref[...], jnp.zeros((ROWS, LANES), F32)], axis=0)
    out_ref[2 * wide : 2 * wide + 32, :] = jnp.where(band == 0, edge, low)


def select(place, both_ref, out_ref):
    band, _ = place()
    size = both_ref.shape[0] // 2
    tmpl = (size - 32) // 4
    for k in range(4):
        start = size * (k // 2) + 2 * tmpl * (k % 2) + band * tmpl
        out_ref[k * tmpl : (k + 1) * tmpl, :] = both_ref[pl.ds(pl.multiple_of(start, tmpl), tmpl), :]
    low = both_ref[size + 4 * tmpl :, :]
    low = jnp.where(band == 0, low, pltpu.roll(low, 64, 1))
    tail = both_ref[4 * tmpl : 4 * tmpl + 8, :]
    mid = both_ref[4 * tmpl + 8 : 4 * tmpl + 16, :]
    strain = jnp.concatenate([pltpu.roll(tail, 64, 1), tail, pltpu.roll(mid, 64, 1), mid], axis=0)
    out_ref[4 * tmpl : 4 * tmpl + 32, :] = jnp.where(lane_iota(32) < 64, low, strain)
    out_ref[4 * tmpl + 32 :, :] = both_ref[4 * tmpl + 16 : 4 * tmpl + 24, :]


class Toeplitz:
    def __init__(self, source, shift, hi_ref, lo_ref):
        self.source, self.shift, self.hi_ref, self.lo_ref = source, shift, hi_ref, lo_ref
        self.turned = {}
        self.lane = lane_iota(ROWS)
        self.sub = lax.broadcasted_iota(jnp.int32, (ROWS, LANES), 0)

    def turn(self, group, n):
        key = (group, n)
        if key not in self.turned:
            by = (ROWS * group + self.shift) % LANES
            self.turned[key] = pltpu.roll(self.source(n), by, 1, stride=1, stride_axis=0)
        return self.turned[key]

    def eight(self, group, n):
        by = ROWS * group + self.shift
        amount = self.sub + by
        value = jnp.where(self.lane >= amount, self.turn(group, n), self.turn(group, n - 1))
        if by + ROWS - 1 > LANES:
            value = jnp.where(self.lane >= amount - LANES, value, self.turn(group, n - 2))
        return value

    def build(self, n, column):
        for pair in range(LANES // 16):
            value = jnp.concatenate([self.eight(2 * pair, n), self.eight(2 * pair + 1, n)], axis=0)
            hi, lo = split(value)
            at = (pl.ds(16 * pair, 16), pl.ds(LANES * column, LANES))
            self.hi_ref[at] = hi
            self.lo_ref[at] = lo


def wide(hi_ref, lo_ref, start, width):
    def pair(ref):
        return [ref[:, start : start + width], ref[:, start - LANES : start - LANES + width]]

    return jnp.concatenate(pair(hi_ref) + pair(hi_ref) + pair(lo_ref), axis=0)


def narrow(hi, lo, t_hi, t_lo, start):
    two = [jnp.concatenate([r[:, start : start + 256], r[:, start - LANES : start + LANES]], axis=0) for r in (t_hi, t_lo)]
    count = hi.shape[0]
    first = dot(jnp.concatenate([hi, lo], axis=0), two[0])
    return first[:count] + first[count:] + dot(hi, two[1])


def rows_of(ref):
    return lambda n: jnp.broadcast_to(ref[n : n + 1, :], (ROWS, LANES))


def filter_own(own_ref, strain_ref, t_hi, t_lo, out_ref):
    tmpl = out_ref.shape[0]
    blocks = out_ref.shape[1] // 256 - 3
    own = Toeplitz(lambda n: jnp.broadcast_to(strain_ref[n - 8 : n - 7, :], (ROWS, LANES)), 0, t_hi, t_lo)
    hi, lo = split(jnp.concatenate([own_ref[0:tmpl, :], own_ref[tmpl : 2 * tmpl, :]], axis=1))
    both = jnp.concatenate([hi, lo], axis=0)
    out_ref[:, 0 : 4 * 256] = jnp.zeros((tmpl, 4 * 256), F32)
    own.build(9, 9)
    for m in range(1, blocks):
        own.build(2 * m + 8, 2 * m + 8)
        own.build(2 * m + 9, 2 * m + 9)
        start = 256 * m + 1024
        taps = [jnp.concatenate([r[:, start : start + 256], r[:, start - LANES : start + LANES]], axis=0) for r in (t_hi, t_lo)]
        first = dot(both, taps[0])
        out_ref[:, 256 * (m + 3) : 256 * (m + 4)] = first[:tmpl] + first[tmpl:] + dot(hi, taps[1])


def column(block):
    return pl.ds(pl.multiple_of(256 * block, 256), 256)


def filter_two(place, right_ref, second_ref, t_hi, t_lo, done_ref, out_ref, b1_ref, b2_ref):
    _, slot = place()
    tmpl = out_ref.shape[0]
    blocks = out_ref.shape[1] // 256
    taps = [jnp.concatenate([r[0:tmpl, :], r[tmpl : 2 * tmpl, :]], axis=1) for r in (right_ref, second_ref)]
    hi, lo = split(jnp.concatenate(taps, axis=0))
    for ref in (b1_ref, b2_ref):
        ref[:, 0 : 4 * 256] = jnp.zeros((tmpl, 4 * 256), F32)
    for m in range(1, blocks):
        got = narrow(hi, lo, t_hi, t_lo, 256 * m + 1024)
        b1_ref[:, 256 * (m + 3) : 256 * (m + 4)] = got[:tmpl]
        b2_ref[:, 256 * (m + 3) : 256 * (m + 4)] = got[tmpl:]
        at = [column(m + 3 - (slot + ahead) % SHARES) for ahead in range(3)]
        out_ref[:, 256 * m : 256 * m + 256] = done_ref[:, at[0]] + b1_ref[:, at[1]] + b2_ref[:, at[2]]


def filter_and_rebuild(
    place, own_ref, left_ref, right_ref, second_ref, strain_ref, t_hi, t_lo, part_ref, up_hi_ref, up_lo_ref, result_ref,
    out_ref, head_ref, z0_ref, z1_ref, z2_ref, b3_ref, sem_ref, xh_ref, ym_ref, yl_ref, th_hi, th_lo, tm_hi, tm_lo, tl_hi, tl_lo, hh_ref, hm_ref, sm_ref,
    hl_ref, hc_ref,
):
    _, slot, slots = place()
    tmpl = out_ref.shape[0]
    base = 4 * tmpl
    lane = lane_iota(ROWS)

    def edges(ref, keep):
        def wide(first):
            a, b = ref[first : first + 8, :], ref[first + 8 : first + 16, :]
            return jnp.where(keep, jnp.where(lane < 64, pltpu.roll(a, 64, 1), b), 0.0)

        return wide(base), wide(base + 16), jnp.where(keep, ref[base + 32 : base + 40, :], 0.0)

    here = edges(own_ref, slot >= 0)
    left = edges(left_ref, slot >= 1)
    second = edges(second_ref, slot >= 2)
    right = edges(right_ref, slot < slots - 1)
    xh_ref[0:8, :] = left[0]
    xh_ref[8:16, :] = strain_ref[0:8, :]
    for k, block in enumerate((second, left, here, right)):
        ym_ref[8 * k : 8 * k + 8, :] = block[1]
        yl_ref[k : k + 1, :] = block[2][0:1, :]

    for source, ahead in ((own_ref, 0), (right_ref, 1), (second_ref, 2), (left_ref, 3)):
        share = (slot + ahead) % SHARES
        for k in range(4):
            hi, lo = split(source[k * tmpl : (k + 1) * tmpl, :])
            ref, at = (hh_ref, hm_ref)[k // 2], LANES * (k % 2)
            rows = pl.ds(pl.multiple_of(share * tmpl, tmpl), tmpl) if k // 2 else slice(ahead * tmpl, (ahead + 1) * tmpl)
            places = [(ref, rows)]
            if k // 2 == 0:
                places.append((hc_ref, pl.ds(pl.multiple_of(share * tmpl, tmpl), tmpl)))
            for ref, rows in places:
                ref[rows, at : at + LANES] = hi
                ref[rows, 256 + at : 256 + at + LANES] = lo
                ref[rows, 512 + at : 512 + at + LANES] = hi
        hl_ref[pl.ds(pl.multiple_of(share * 32, 32), 32), :] = source[base : base + 32, :]
    h_low = jnp.transpose(hl_ref[...])[0:tmpl, :]

    blocks = out_ref.shape[1] // 256
    copies, sent = [], 0
    zero_block = (z0_ref, z1_ref, z2_ref, b3_ref)
    shares = [(slot + ahead) % SHARES for ahead in range(SHARES)]
    high_t = Toeplitz(rows_of(xh_ref), 0, th_hi, th_lo)
    mid_t = Toeplitz(rows_of(ym_ref), 8, tm_hi, tm_lo)
    low_t = Toeplitz(rows_of(yl_ref), 9, tl_hi, tl_lo)

    def columns(m):
        return slice(256 * m, 256 * m + 256)

    head_ref[...] = jnp.zeros(head_ref.shape, F32)

    def inner(m):
        if m == 0:
            got = dot(hh_ref[...], wide(th_hi, th_lo, 1024, 256))
            for ahead, ref in enumerate(zero_block):
                ref[:, columns(3)] = got[ahead * tmpl : (ahead + 1) * tmpl, :]
            return
        hi, lo = hh_ref[3 * tmpl :, 0:256], hh_ref[3 * tmpl :, 256:512]
        b3_ref[:, columns(m + 3)] = narrow(hi, lo, t_hi, t_lo, 256 * m + 1024)

    def outer(m):
        got = dot(hc_ref[-m * tmpl :, :], wide(th_hi, th_lo, 256 * m + 1024, 256))
        for k in range(SHARES + m):
            head_ref[:, columns(k)] += got[k * tmpl : (k + 1) * tmpl, :]

    def finish(a):
        value = out_ref[:, columns(a)] + b3_ref[:, column(a + 3 - shares[3])]
        if a > 0:
            value = value + part_ref[:, columns(a)]
        if a < SHARES:
            for ahead in range(3):
                value = value + zero_block[ahead][:, column(a + 3 - shares[ahead])]
        if a < 3:
            value = value + head_ref[:, columns(a)]
        out_ref[:, columns(a)] = value

    def send(first, last):
        where = (slice(None), pl.ds(256 * first, 256 * (last - first)))
        copy = pltpu.make_async_copy(out_ref.at[where], result_ref.at[where], sem_ref.at[len(copies)])
        copy.start()
        copies.append(copy)

    for n in range(1, 10):
        high_t.build(n, n)
    for m in (-3, -2, -1):
        outer(m)
    for m in range(0, 8):
        inner(m)
        mid_t.build(2 * m + 9, 2 * m + 1)
        mid_t.build(2 * m + 10, 2 * m + 2)

    low_t.build(2, 0)
    low_t.build(3, 1)
    part_low = dot3(*split(h_low), tl_hi[...], tl_lo[...])
    low_count = LANES
    z = lax.broadcasted_iota(jnp.int32, part_low.shape, 1) - 9 + slot * low_count
    part_low = jnp.where((z >= 0) & (z < slots * low_count), part_low, 0.0)
    low_hi, low_lo = split(part_low)

    edge = jnp.zeros((tmpl, LANES), F32)
    for c in range(4):
        edge = edge + dot(hm_ref[c * tmpl : (c + 1) * tmpl, :], wide(tm_hi, tm_lo, 2048 - 256 * c, LANES))
    for r in range(4):
        sm_ref[:, 256 * r : 256 * r + 256] = rebuild(low_hi, low_lo, up_hi_ref, up_lo_ref, r)
    sm_ref[:, 1024:1152] = edge + dot3(
        low_hi[:, LANES:], low_lo[:, LANES:], up_hi_ref[0, 0:LANES, 0:LANES], up_lo_ref[0, 0:LANES, 0:LANES]
    )
    for m in range(-3, 4):
        first, last = max(0, -m), min(3, 3 - m)
        got = dot(hm_ref[first * tmpl : (last + 1) * tmpl, :], wide(tm_hi, tm_lo, 256 * m + 1024, 256))
        for c in range(first, last + 1):
            at = 256 * (m + c)
            sm_ref[:, at : at + 256] += got[(c - first) * tmpl : (c - first + 1) * tmpl, :]
    for ref in zero_block[:3]:
        ref[:, 0:768] = jnp.zeros((tmpl, 768), F32)
        ref[:, 1024:] = jnp.zeros((tmpl, 768), F32)
    b3_ref[:, 0:768] = jnp.zeros((tmpl, 768), F32)
    inner(8)
    inner(9)
    mid_count = 1024
    v = lax.broadcasted_iota(jnp.int32, sm_ref.shape, 1) - 8 + slot * mid_count
    part_mid = jnp.where((v >= 0) & (v < slots * mid_count), sm_ref[...], 0.0)
    mid_hi, mid_lo = split(part_mid)

    def stacked(x):
        return jnp.concatenate([x[:, LANES * g : LANES * g + 256] for g in range(8)], axis=0)

    stack_hi, stack_lo = stacked(mid_hi), stacked(mid_lo)
    for r in range(4):
        got = rebuild(stack_hi, stack_lo, up_hi_ref, up_lo_ref, r)
        for g in range(8):
            out_ref[:, columns(4 * g + r)] = got[g * tmpl : (g + 1) * tmpl, :]
    ready = 10
    for m in range(ready, blocks):
        inner(m)
        if m == ready:
            for a in range(m + 1):
                finish(a)
        else:
            finish(m)
        if m % 4 == 3 or m >= blocks - 2:
            send(sent, m + 1)
            sent = m + 1
    for copy in copies:
        copy.wait()


VMEM = pl.BlockSpec(memory_space=pltpu.VMEM)
SMEM = pl.BlockSpec(memory_space=pltpu.SMEM)
ANY = pl.BlockSpec(memory_space=pl.ANY)


def near(x):
    return pltpu.with_memory_space_constraint(x, pltpu.VMEM)


def place():
    return lax.axis_index("band").astype(jnp.int32), lax.axis_index("tm").astype(jnp.int32)


def call_pack(count, filters, recons, strains, parts, place=place):
    wide, basis = recons[0].shape
    half = pltpu.VMEM((wide, basis), BF16)
    return pl.pallas_call(
        functools.partial(pack_filters, place),
        out_shape=(
            pltpu.VMEM((parts, 8, 3 * LANES), F32), half, half, half, half,
            pltpu.VMEM(strains[0].shape, F32), pltpu.VMEM((24, LANES), F32),
        ),
        in_specs=[SMEM] + [VMEM] * 9,
        out_specs=(VMEM,) * 7,
        scratch_shapes=[pltpu.VMEM((24, LANES), F32)],
        name="pack_filters",
    )(count, *filters, *recons, *strains)


def call_combine(got, weights, edge, place=place):
    wide, basis = weights[0].shape
    return pl.pallas_call(
        functools.partial(combine, place),
        out_shape=pltpu.VMEM((2 * wide + 32, LANES), F32),
        in_specs=[VMEM] * 6,
        out_specs=VMEM,
        scratch_shapes=[pltpu.VMEM((3, basis, LANES), F32)],
        name="combine",
    )(*[near(x) for x in (got, *weights, edge)])


def call_select(both, place=place):
    return pl.pallas_call(
        functools.partial(select, place),
        out_shape=pltpu.VMEM((both.shape[0] // 2 + 8, LANES), F32),
        in_specs=[VMEM],
        out_specs=VMEM,
        name="select",
    )(near(both))


def call_filter_own(own, strain, tmpl, count):
    half = pltpu.VMEM((LANES, count + 1024), BF16)
    return pl.pallas_call(
        filter_own,
        out_shape=(half, half, pltpu.VMEM((tmpl, count + 768), F32)),
        in_specs=[VMEM] * 2,
        out_specs=(VMEM,) * 3,
        name="filter_own",
        compiler_params=pltpu.CompilerParams(vmem_limit_bytes=24 << 20),
    )(near(own), near(strain))


def call_filter_two(right, second, t_hi, t_lo, done, tmpl, count, place=place):
    return pl.pallas_call(
        functools.partial(filter_two, place),
        out_shape=pltpu.VMEM((tmpl, count), F32),
        in_specs=[VMEM] * 5,
        out_specs=VMEM,
        scratch_shapes=[pltpu.VMEM((tmpl, count + 768), F32)] * 2,
        name="filter_two",
        compiler_params=pltpu.CompilerParams(vmem_limit_bytes=24 << 20),
    )(*[near(x) for x in (right, second, t_hi, t_lo, done)])


def call_filter(own, left, right, second, strain, t_hi, t_lo, part, up_hi, up_lo, tmpl, count, slots, place=place):
    return pl.pallas_call(
        functools.partial(filter_and_rebuild, lambda: (*place(), slots)),
        out_shape=jax.ShapeDtypeStruct((tmpl, count), F32),
        in_specs=[VMEM] * 10,
        out_specs=ANY,
        scratch_shapes=[
            pltpu.VMEM((tmpl, count), F32),
            pltpu.VMEM((tmpl, 768), F32),
            pltpu.VMEM((tmpl, 7 * 256), F32),
            pltpu.VMEM((tmpl, 7 * 256), F32),
            pltpu.VMEM((tmpl, 7 * 256), F32),
            pltpu.VMEM((tmpl, count + 768), F32),
            pltpu.SemaphoreType.DMA((count // 1024 + 1,)),
            pltpu.VMEM((16, LANES), F32),
            pltpu.VMEM((32, LANES), F32),
            pltpu.VMEM((8, LANES), F32),
            pltpu.VMEM((LANES, 1280), BF16),
            pltpu.VMEM((LANES, 1280), BF16),
            pltpu.VMEM((LANES, 2304), BF16),
            pltpu.VMEM((LANES, 2304), BF16),
            pltpu.VMEM((LANES, 256), BF16),
            pltpu.VMEM((LANES, 256), BF16),
            pltpu.VMEM((4 * tmpl, 768), BF16),
            pltpu.VMEM((4 * tmpl, 768), BF16),
            pltpu.VMEM((tmpl, 1152), F32),
            pltpu.VMEM((LANES, LANES), F32),
            pltpu.VMEM((4 * tmpl, 768), BF16),
        ],
        name="filter_and_rebuild",
        compiler_params=pltpu.CompilerParams(vmem_limit_bytes=36 << 20),
    )(*[near(x) for x in (own, left, right, second, strain, t_hi, t_lo, part, up_hi, up_lo)])


def interp_halves():
    exact = jnp.asarray(interp_blocks().astype(np.float32))
    return split(exact)


def local(
    strain_high, strain_mid, strain_low,
    filters_high, filters_mid, filters_low,
    recon_high, recon_mid, recon_low, basis_count,
):
    tmpl_count = lax.axis_size("tmpl")

    def turned(recon):
        basis, parts, count = recon.shape
        return jnp.transpose(recon, (1, 2, 0)).reshape(parts * count, basis)

    packed, *weights, strain, edge = call_pack(
        basis_count,
        (filters_high, filters_mid, filters_low),
        (turned(recon_high), turned(recon_mid), turned(recon_low)),
        (strain_high.reshape(-1, LANES), strain_mid.reshape(-1, LANES), strain_low.reshape(1, LANES)),
        tmpl_count,
    )
    slots = lax.axis_size("tm")
    got = lax.all_to_all(packed, "tmpl", 0, 0, tiled=True)
    both = lax.all_gather(call_combine(got, weights, edge), "band", axis=0, tiled=True)
    own = call_select(both)

    def moved(by):
        return lax.ppermute(own, "tm", [(i, (i + by) % slots) for i in range(slots)])

    second, right, left = moved(2), moved(-1), moved(1)
    tmpl, count = recon_high.shape[2], strain_high.shape[0]
    t_hi, t_lo, done = call_filter_own(own, strain, tmpl, count)
    begun = (t_hi, t_lo, call_filter_two(right, second, t_hi, t_lo, done, tmpl, count))
    up_hi, up_lo = interp_halves()
    out = call_filter(own, left, right, second, strain, *begun, up_hi, up_lo, tmpl, count, slots)
    return out[None]


def solution(mesh):
    in_specs = (
        P("tm"), P("tm"), P("tm"),
        P("tmpl", None), P("tmpl", None), P("tmpl", None),
        P(None, None, "tmpl"), P(None, None, "tmpl"), P(None, None, "tmpl"),
        P(),
    )
    out_specs = P("band", "tmpl", "tm")
    return jax.shard_map(local, mesh=mesh, in_specs=in_specs, out_specs=out_specs, check_vma=False)
```
